32 devices in a mesh: gx: 2 (over x), gy: 4 (over y, core), gz: 4 (over z).
Axes of the slice: x: 2, y: 2, z: 4, core: 2. Of those that a mesh axis runs over, the one named last changes fastest.
Arguments:
- right_side: float32 [24, 64, 512], P('gx', 'gy', 'gz'), may hold values from -8 to 8
- coefficient: float32 [24, 64, 512], P('gx', 'gy', 'gz'), may hold values from 0.02 to 1
Outputs:
- solution: float32 [24, 64, 512], P('gx', 'gy', 'gz')
- residual: float32 [24, 64, 512], P('gx', 'gy', 'gz')
- precond: float32 [24, 64, 512], P('gx', 'gy', 'gz')
- image: float32 [24, 64, 512], P('gx', 'gy', 'gz')
The draws below stay inside these ranges and needn't reach their ends.
All inputs are finite; a program needn't handle non-finite values.
Results may differ from the reference program's by a relative error of at most 0.00021.
Values sent between devices are 32-bit elements; how exact they have to be, the bound alone decides.
A program may use at most 64 MiB of HBM per device.

```python
import math
import jax
import jax.numpy as jnp

SWEEPS = 4
ITERS = 1
NX = 24
NY = 64
NZ = 512


def block_levels(own_key, shape, shards, smallest, largest):
    loudness, own = 1.0, jax.random.fold_in(own_key, 6)
    for position, parts in shards:
        steps = jnp.exp(jax.random.uniform(jax.random.fold_in(own, position), (parts,), jnp.float32, smallest / len(shards), largest / len(shards)))
        loudness = loudness * jnp.repeat(steps, shape[position] // parts).reshape([-1 if axis == position else 1 for axis in range(len(shape))])
    return loudness


def noise(own_key, shape, scale, reach, pieces=(), kind=jnp.bfloat16):
    values = jax.random.normal(own_key, shape, jnp.float32) * scale
    if len(pieces) > 0:
        values = block_levels(own_key, shape, pieces, -0.22, 0.18) * values
    return jnp.clip(values, min=-reach, max=reach).astype(kind)


def setup_inputs(seed: int = 0) -> dict:
    arg_keys = jax.random.split(jax.random.key(seed), 3)
    return {
        "right_side": noise(arg_keys[0], (NX, NY, NZ), 1.0, 8.0, ((0, 2), (1, 4), (2, 4)), jnp.float32),
        "coefficient": jnp.clip(jnp.exp(math.log(1.0) - 3.912023 * jax.random.uniform(arg_keys[1], (NX, NY, NZ), jnp.float32) ** block_levels(arg_keys[1], (NX, NY, NZ), ((0, 2), (1, 4), (2, 4)), -0.2, 0.2)), 0.02, 1.0),
    }


relaxation = 0.6


def block_sum(padded):
    summed = padded[:-2] + padded[1:-1] + padded[2:]
    summed = summed[:, :-2] + summed[:, 1:-1] + summed[:, 2:]
    return summed[:, :, :-2] + summed[:, :, 1:-1] + summed[:, :, 2:]


def operate(values, reaction):
    return (27.0 + reaction) * values - block_sum(jnp.pad(values, 1))


def restrict(values):
    extent = values.shape
    grouped = values.reshape(extent[0] // 2, 2, extent[1] // 2, 2, extent[2] // 2, 2)
    return 0.5 * grouped.sum(axis=(1, 3, 5))


def prolong(values):
    return jnp.repeat(jnp.repeat(jnp.repeat(values, 2, axis=0), 2, axis=1), 2, axis=2)


def coarsest(source, reaction):
    correction = relaxation * source / (26.0 + reaction)
    for sweep in range(SWEEPS - 1):
        correction = correction + relaxation * (source - operate(correction, reaction)) / (26.0 + reaction)
    return correction


def multigrid(source, reactions, level_index):
    if level_index == 2:
        return coarsest(source, reactions[2])
    reaction = reactions[level_index]
    correction = relaxation * source / (26.0 + reaction)
    remainder = source - operate(correction, reaction)
    correction = correction + prolong(multigrid(restrict(remainder), reactions, level_index + 1))
    return correction + relaxation * (source - operate(correction, reaction)) / (26.0 + reaction)


def reference(right_side, coefficient):
    middle = restrict(coefficient)
    reactions = (coefficient, middle, restrict(middle))
    solution = jnp.zeros_like(right_side)
    residual = right_side
    precond = multigrid(residual, reactions, 0)
    image = operate(precond, coefficient)
    direction = precond
    dir_image = image
    dir_precond = precond
    dir_twice = image
    gamma_prev = jnp.float32(1.0)
    alpha_prev = jnp.float32(1.0)
    for step in range(ITERS):
        gamma_now = jnp.sum(residual * precond)
        delta_now = jnp.sum(image * precond)
        precond_image = multigrid(image, reactions, 0)
        image_twice = operate(precond_image, coefficient)
        if step == 0:
            alpha_now = gamma_now / delta_now
            direction = precond
            dir_image = image
            dir_precond = precond_image
            dir_twice = image_twice
        else:
            beta_now = gamma_now / gamma_prev
            alpha_now = gamma_now / (delta_now - beta_now * gamma_now / alpha_prev)
            dir_twice = image_twice + beta_now * dir_twice
            dir_precond = precond_image + beta_now * dir_precond
            dir_image = image + beta_now * dir_image
            direction = precond + beta_now * direction
        solution = solution + alpha_now * direction
        residual = residual - alpha_now * dir_image
        precond = precond - alpha_now * dir_precond
        image = image - alpha_now * dir_twice
        gamma_prev = gamma_now
        alpha_prev = alpha_now
    return (solution, residual, precond, image)
```

```python
import functools

import jax
import jax.numpy as jnp
from jax import lax
from jax.experimental import pallas as pl
from jax.experimental.pallas import tpu as pltpu
from jax.sharding import PartitionSpec as P

SWEEPS = 4
relaxation = 0.6

AXES = ("gx", "gy", "gz")
MESH = pl.DeviceIdType.MESH
WIDTH = 5
EDGE = 8
SPAN = 2 * WIDTH
PART = SWEEPS


def dot(a, b):
    high = a.astype(jnp.bfloat16)
    low = (a - high.astype(jnp.float32)).astype(jnp.bfloat16)
    both = jnp.concatenate([high, low], 1)
    b = b.astype(jnp.bfloat16)
    return jnp.dot(both, jnp.concatenate([b, b], 0), preferred_element_type=jnp.float32)


def iota(shape, dim):
    return lax.broadcasted_iota(jnp.int32, shape, dim)


def kernel(counts, block, reach, g_hbm, c_hbm, pre_ref, img_ref, twice_ref, image_twice_ref, alpha_ref, g_ref,
           c_ref, insem, gc0, im0, pk1, pk2, zr1, zr2, t1, d0, d1, xr0, xr1, pf0, pf1, xm, um,
           cs1, cs2, cr1, cr2, kept, mid, red_s, red_r, ssem, rsem, lssem, lrsem):
    bx, by, bz = block
    kx = reach
    me = [lax.axis_index(a) for a in AXES]
    ex, ey = bx + SPAN, by + 2 * EDGE
    mx, my = bx // 2 + 4, ey // 2
    qx = bx // 4
    lane = iota((ey, bz), 1)
    row = iota((ey, bz), 0)

    def valid(offset):
        ok = None
        for axis, step in enumerate(offset):
            if step == 0:
                continue
            place = me[axis] + step
            term = place >= 0 if step < 0 else place < counts[axis]
            ok = term if ok is None else jnp.logical_and(ok, term)
        return ok

    def target(offset):
        return tuple(m + s for m, s in zip(me, offset))

    near = [(dx, dy, dz) for dx in range(-kx, kx + 1) for dy in (-1, 0, 1) for dz in (-1, 0, 1)]
    near = [o for o in near if o != (0, 0, 0) and all(counts[a] > abs(o[a]) for a in range(3))]
    near.sort(key=lambda o: (-abs(o[0]), abs(o[1]) + abs(o[2])))
    close = [o for o in near if abs(o[0]) <= 1]

    barrier = pltpu.get_barrier_semaphore()
    lines = []
    for axis in range(3):
        for step in range(1, counts[axis]):
            to = list(me)
            to[axis] = lax.rem(me[axis] + step, counts[axis])
            lines.append((axis, step, tuple(to)))

    copies = [pltpu.make_async_copy(src, dst, insem.at[n])
              for n, (src, dst) in enumerate(((g_hbm, g_ref), (c_hbm, c_ref)))]
    for copy in copies:
        copy.start()
    zr1[...] = jnp.zeros_like(zr1)
    gc0[...] = jnp.zeros_like(gc0)
    cr1[...] = jnp.zeros_like(cr1)

    for offset in near:
        @pl.when(valid(offset))
        def _(offset=offset):
            pl.semaphore_signal(barrier, inc=1, device_id=target(offset), device_id_type=MESH)
    for axis, step, to in lines:
        pl.semaphore_signal(barrier, inc=1, device_id=to, device_id_type=MESH)

    def options(axis, far):
        total = 1
        for step in range(1, far + 1):
            if counts[axis] > step:
                total = total + (me[axis] >= step).astype(jnp.int32)
                total = total + (me[axis] + step < counts[axis]).astype(jnp.int32)
        return total

    greeted = options(0, kx) * options(1, 1) * options(2, 1) - 1 + len(lines)

    strip = (lane[:by] < WIDTH) | (lane[:by] >= bz - WIDTH)

    def packed(planes):
        total = None
        for i, plane in enumerate(planes):
            piece = jnp.where(strip, plane, 0.0)
            if i > 0:
                piece = pltpu.roll(piece, SPAN * i, 1)
            total = piece if total is None else total + piece
        return total

    def fill(buf, pk, s, planes):
        for i, plane in enumerate(planes):
            buf[s, WIDTH + i, EDGE:EDGE + by, :] = plane
        pk[s] = packed(planes)

    def row_ends(dy):
        if dy == 0:
            return 0, by, EDGE
        if dy > 0:
            return by - EDGE, EDGE, 0
        return 0, EDGE, EDGE + by

    def fine_copy(phase, n, offset, buf, pk, zr):
        dx, dy, dz = offset
        start, size, goes = row_ends(dy)
        if dz == 0:
            if dx == 0:
                px, nx, tx = WIDTH, bx, WIDTH
            elif dx > 0:
                px, nx, tx = bx, WIDTH, 0
            else:
                px, nx, tx = WIDTH, WIDTH, WIDTH + bx
            src = buf.at[:, pl.ds(px, nx), pl.ds(EDGE + start, size), :]
            dst = buf.at[:, pl.ds(tx, nx), pl.ds(goes, size), :]
        else:
            side = 0 if dz > 0 else 1
            src = pk.at[:, pl.ds(start, size), :]
            dst = zr.at[side, 1 - dx, :, pl.ds(goes, size), :]
        return pltpu.make_async_remote_copy(
            src_ref=src, dst_ref=dst, send_sem=ssem.at[phase, n], recv_sem=rsem.at[phase, n],
            device_id=target(offset), device_id_type=MESH)

    def coarse_copy(phase, n, offset, cs, cr):
        dx, dy, dz = offset
        return pltpu.make_async_remote_copy(
            src_ref=cs, dst_ref=cr.at[kx - dx, 1 - dy, 1 - dz],
            send_sem=ssem.at[phase, n], recv_sem=rsem.at[phase, n],
            device_id=target(offset), device_id_type=MESH)

    def begin(make, offsets):
        for n, offset in enumerate(offsets):
            @pl.when(valid(offset))
            def _(n=n, offset=offset):
                make(n, offset).start()

    def arrive(make, offsets):
        for n, offset in enumerate(offsets):
            @pl.when(valid(tuple(-s for s in offset)))
            def _(n=n, offset=offset):
                make(n, offset).wait_recv()

    def leave(make, offsets):
        for n, offset in enumerate(offsets):
            @pl.when(valid(offset))
            def _(n=n, offset=offset):
                make(n, offset).wait_send()

    def line_copy(axis, step, to):
        n = sum(counts[:axis]) + step
        return pltpu.make_async_remote_copy(
            src_ref=red_s.at[axis], dst_ref=red_r.at[n], send_sem=lssem.at[n],
            recv_sem=lrsem.at[n], device_id=to, device_id_type=MESH)

    def line_begin(axis, value):
        red_s[axis] = value
        for a, step, to in lines:
            if a == axis:
                line_copy(a, step, to).start()

    def line_end(axis):
        value = red_s[axis]
        for a, step, to in lines:
            if a == axis:
                line_copy(a, step, to).wait_recv()
                value = value + red_r[sum(counts[:a]) + step]
        return value

    place = lax.rem(lane + WIDTH, bz)
    low = lax.rem(place, SPAN) < WIDTH
    band = (lane < WIDTH) | (lane >= bz - WIDTH)

    def spread(zr, s, t):
        for side in range(3):
            merged = jnp.where(low, zr[0, side, s], zr[1, side, s])
            if side == 0:
                todo = [(bx - WIDTH + i, i) for i in range(WIDTH)]
            elif side == 1:
                todo = [(i, WIDTH + i) for i in range(bx)]
            else:
                todo = [(i, WIDTH + bx + i) for i in range(WIDTH)]
            for i, e in todo:
                piece = merged if i == 0 else pltpu.roll(merged, (bz - SPAN * i) % bz, 1)
                t1[t, e] = jnp.where(band, piece, 0.0)

    first, last = lane == 0, lane == bz - 1

    def yz(a, b):
        sa = a + jnp.where(first, pltpu.roll(b, 1, 1), pltpu.roll(a, 1, 1))
        sb = b + jnp.where(first, pltpu.roll(a, 1, 1), pltpu.roll(b, 1, 1))
        sa = sa + jnp.where(last, pltpu.roll(b, bz - 1, 1), pltpu.roll(a, bz - 1, 1))
        sb = sb + jnp.where(last, pltpu.roll(a, bz - 1, 1), pltpu.roll(b, bz - 1, 1))
        sa = sa + pltpu.roll(sa, 1, 0) + pltpu.roll(sa, ey - 1, 0)
        sb = sb + pltpu.roll(sb, 1, 0) + pltpu.roll(sb, ey - 1, 0)
        return sa, sb

    def box(v):
        s = v + pltpu.roll(v, 1, 2) + pltpu.roll(v, v.shape[2] - 1, 2)
        s = s + pltpu.roll(s, 1, 1) + pltpu.roll(s, v.shape[1] - 1, 1)
        zero = jnp.zeros_like(s[:1])
        return s + jnp.concatenate([zero, s[:-1]], 0) + jnp.concatenate([s[1:], zero], 0)

    p_, q_ = iota((bz, bz), 0), iota((bz, bz), 1)
    down_a = jnp.where((p_ >> 1) == q_, 0.5, 0.0)
    down_b = jnp.where(((p_ + bz) >> 1) == q_, 0.5, 0.0)
    up_a = jnp.where((q_ >> 1) == p_, 1.0, 0.0)
    up_b = jnp.where(((q_ + bz) >> 1) == p_, 1.0, 0.0)
    quarter = bz // 4
    down_c = jnp.where((p_ < bz // 2) & ((p_ >> 1) == lax.rem(q_, quarter)), 0.5, 0.0)
    up_c = jnp.where(p_ == jnp.where(q_ < 3 * quarter, q_ >> 1, (q_ >> 1) + bz // 2), 1.0, 0.0)

    def restricted(of):
        for m in range(mx):
            a0, b0 = of(2 * m + 1)
            a1, b1 = of(2 * m + 2)
            xr0[m * ey:(m + 1) * ey, :] = a0 + a1
            xr1[m * ey:(m + 1) * ey, :] = b0 + b1
        n = mx * my
        a = xr0[pl.ds(0, n, stride=2), :] + xr0[pl.ds(1, n, stride=2), :]
        b = xr1[pl.ds(0, n, stride=2), :] + xr1[pl.ds(1, n, stride=2), :]
        return (dot(a, down_a) + dot(b, down_b)).reshape(mx, my, bz)

    turn = iota((my // 2, bz), 1) // quarter
    crow = iota((my // 2, bz), 0)

    def coarsened(v, lift):
        for m in range(qx):
            xm[m * my:(m + 1) * my, :] = v[2 + 2 * m] + v[3 + 2 * m]
        n = qx * my // 2
        a = xm[pl.ds(0, n, stride=2), :] + xm[pl.ds(1, n, stride=2), :]
        a = dot(a, down_c)
        rows = my // 2
        tile = a[:rows]
        for m in range(1, qx):
            tile = jnp.where(turn == m, a[m * rows:(m + 1) * rows], tile)
        return pltpu.roll(tile, 2 if lift else rows - 2, 0)

    xs = [x for x in range(-PART, qx + PART) if -kx * qx <= x < (kx + 1) * qx]

    def gathered(cr, cs, lifts):
        half = my // 4
        columns = {}
        for dx in sorted({x // qx for x in xs}):
            for dy in (-1, 0, 1):
                here = cs[...] if (dx, dy) == (0, 0) else cr[kx + dx, 1 + dy, 1]
                after = pltpu.roll(cr[kx + dx, 1 + dy, 2], quarter, 1)
                before = pltpu.roll(cr[kx + dx, 1 + dy, 0], 3 * quarter, 1)
                for m in range(qx):
                    tile = jnp.where(turn == (m + 1) % 4, after, here)
                    tile = jnp.where(turn == (m + 3) % 4, before, tile)
                    if m > 0:
                        tile = pltpu.roll(tile, bz - quarter * m, 1)
                    columns[dx * qx + m, dy] = tile
        arrays = []
        for lift in lifts:
            planes = []
            for x in xs:
                tiles = [columns[x, dy] for dy in (-1, 0, 1)]
                turned = [pltpu.roll(t, half, 0) for t in tiles]
                if lift:
                    tiles, turned = turned, tiles
                upper = jnp.where(crow < half, tiles[0], turned[1])
                lower = jnp.where(crow < half, tiles[2], 0.0)
                planes.append(jnp.concatenate([upper, lower], 0))
            arrays.append(jnp.stack(planes))
        return arrays

    def within(place, axis, size):
        place = place + me[axis] * size
        return (place >= 0) & (place < counts[axis] * size)

    for copy in copies:
        copy.wait()
    g = [g_ref[i] for i in range(bx)]
    fill(gc0, pk1, 0, g)
    fill(gc0, pk1, 1, [c_ref[i] for i in range(bx)])
    for buf in (zr2, im0, cr2):
        buf[...] = jnp.zeros_like(buf)
    pl.semaphore_wait(barrier, greeted)
    make_a = lambda n, o: fine_copy(0, n, o, gc0, pk1, zr1)
    begin(make_a, close)
    arrive(make_a, close)
    spread(zr1, 0, 0)
    spread(zr1, 1, 1)

    in_y = within(row - EDGE, 1, by)
    in_z = band & within(jnp.where(lane < bz // 2, lane + bz, lane - bz), 2, bz)
    for i in range(ex):
        in_x = within(jnp.full((ey, bz), i - WIDTH, jnp.int32), 0, bx)
        d0[i] = jnp.where(in_y & in_x, relaxation / (26.0 + gc0[1, i]), 0.0)
        d1[i] = jnp.where(in_y & in_x & in_z, relaxation / (26.0 + t1[1, i]), 0.0)

    c1 = restricted(lambda i: (gc0[1, i], t1[1, i]))
    shape = (mx, my, bz)
    zl = iota(shape, 2)
    zl = jnp.where(zl < 3 * quarter, zl, zl - bz)
    inside = within(iota(shape, 0) - 2, 0, bx // 2) & within(iota(shape, 1) - 4, 1, by // 2)
    inside = inside & within(zl, 2, bz // 2)
    mid[0] = jnp.where(inside, relaxation / (26.0 + c1), 0.0)
    mid[1] = 27.0 + c1
    cs1[...] = coarsened(c1, True)

    def inverse2(c2):
        shape = c2.shape
        z = iota(shape, 2)
        z = jnp.where(z < 2 * quarter, z, z - bz)
        ok = within(iota(shape, 0) + xs[0], 0, qx) & within(iota(shape, 1) - 4, 1, by // 4)
        ok = ok & within(z, 2, quarter) & (z >= -quarter)
        return jnp.where(ok, relaxation / (26.0 + c2), 0.0)

    def cycle(g_at, make_b, cs, cr, hook, second, finish):
        def e0(i):
            a, b = g_at(i)
            return d0[i] * a, d1[i] * b

        sums = {}

        def remainder(i):
            for k in (i - 1, i, i + 1):
                if k not in sums:
                    sums[k] = yz(*e0(k))
            a, b = g_at(i)
            ea, eb = e0(i)
            ra = a - (27.0 + gc0[1, i]) * ea + sums[i - 1][0] + sums[i][0] + sums[i + 1][0]
            rb = b - (27.0 + t1[1, i]) * eb + sums[i - 1][1] + sums[i][1] + sums[i + 1][1]
            return ra, rb

        g1 = restricted(remainder)
        f = mid[0] * g1
        mid[2] = g1
        tile = coarsened(g1 - mid[1] * f + box(f), False)
        cs[...] = jnp.where(crow < my // 4, tile, cs1[...])
        begin(make_b, near)
        hook()
        arrive(make_b, near)
        if cr is cr1:
            g2, c2 = gathered(cr, cs, (False, True))
            kept[0] = inverse2(c2)
            kept[1] = 27.0 + c2
        else:
            g2, = gathered(cr, cs, (False,))
        inv, diag = kept[0], kept[1]
        e = inv * g2
        for sweep in range(SWEEPS - 1):
            e = e + inv * (g2 - diag * e + box(e))
        second()
        nq = qx + 2
        e = jnp.concatenate([e[xs.index(x)][None] if x in xs else jnp.zeros_like(e[:1])
                             for x in range(-1, qx + 1)], 0)
        e = pltpu.roll(e, my - 2, 1)[:, :my // 2].reshape(nq * my // 2, bz)
        u = dot(e, up_c)
        um[pl.ds(0, nq * my // 2, stride=2), :] = u
        um[pl.ds(1, nq * my // 2, stride=2), :] = u
        u = um[...].reshape(nq, my, bz)
        u = jnp.concatenate([u[(m - 2) // 2 + 1][None] for m in range(mx)], 0)
        g1 = mid[2]
        f = mid[0] * g1 + u
        f = f + mid[0] * (g1 - mid[1] * f + box(f))
        nm = mx - 2
        f = f[1:mx - 1].reshape(nm * my, bz)
        for pf, up in ((pf0, up_a), (pf1, up_b)):
            w = dot(f, up)
            pf[pl.ds(0, nm * my, stride=2), :] = w
            pf[pl.ds(1, nm * my, stride=2), :] = w

        def e1(i):
            m = (i - WIDTH) // 2 + 1
            a, b = e0(i)
            return a + pf0[m * ey:(m + 1) * ey, :], b + pf1[m * ey:(m + 1) * ey, :]

        sums1, sums2 = {}, {}
        e2 = {}
        for i in range(WIDTH - 1, WIDTH + bx + 1):
            for k in (i - 1, i, i + 1):
                if k not in sums1:
                    sums1[k] = yz(*e1(k))
            ga, gb = g_at(i)
            ea, eb = e1(i)
            s = [sums1[i - 1][t] + sums1[i][t] + sums1[i + 1][t] for t in range(2)]
            za = ea + d0[i] * (ga - (27.0 + gc0[1, i]) * ea + s[0])
            zb = eb + d1[i] * (gb - (27.0 + t1[1, i]) * eb + s[1])
            e2[i] = za[EDGE:EDGE + by]
            sums2[i] = yz(za, zb)[0][EDGE:EDGE + by]
            k = i - 1
            if k - 1 in sums2:
                out = (27.0 + c_ref[k - WIDTH]) * e2[k] - (sums2[k - 1] + sums2[k] + sums2[k + 1])
                finish(k - WIDTH, e2[k], out)

    gamma, delta = [], []
    images = []

    def finish1(i, e, out):
        pre_ref[i] = e
        images.append(out)
        gamma.append(g_ref[i] * e)
        delta.append(out * e)

    nothing = lambda: None
    make_b = lambda n, o: coarse_copy(1, n, o, cs1, cr1)
    cycle(lambda i: (gc0[0, i], t1[0, i]), make_b, cs1, cr1, nothing, nothing, finish1)

    for i in range(bx):
        img_ref[i] = images[i]
    fill(im0, pk2, 0, images)
    make_c = lambda n, o: fine_copy(2, n, o, im0, pk2, zr2)
    begin(make_c, close)
    gs = jnp.sum(sum(gamma[1:], gamma[0]), axis=0, keepdims=True)
    ds = jnp.sum(sum(delta[1:], delta[0]), axis=0, keepdims=True)
    line_begin(2, jnp.where(iota((8, bz), 0) == 0, gs, ds))
    arrive(make_c, close)
    spread(zr2, 0, 2)

    def hook():
        line_begin(1, line_end(2))

    def second():
        line_begin(0, line_end(1))

    def finish2(i, e, out):
        twice_ref[i] = e
        image_twice_ref[i] = out

    make_d = lambda n, o: coarse_copy(3, n, o, cs2, cr2)
    cycle(lambda i: (im0[0, i], t1[2, i]), make_d, cs2, cr2, hook, second, finish2)

    total = jnp.sum(line_end(0), axis=1, keepdims=True)
    alpha_ref[...] = jnp.broadcast_to(total[0:1] / total[1:2], alpha_ref.shape)
    leave(make_a, close)
    leave(make_b, near)
    leave(make_c, close)
    leave(make_d, near)
    for axis, step, to in lines:
        line_copy(axis, step, to).wait_send()


def solution(mesh):
    counts = tuple(mesh.shape[a] for a in AXES)

    def shards(right_side, coefficient):
        bx, by, bz = block = right_side.shape
        assert SPAN * bx <= bz and by == 16 and bx % 4 == 0
        kx = max(1, min(-(-PART // (bx // 4)), counts[0] - 1))
        ex, ey = bx + SPAN, by + 2 * EDGE
        mx, my = bx // 2 + 4, ey // 2
        qx = bx // 4
        most = (2 * kx + 1) * 9
        planes = qx + 2 * min(PART, kx * qx)
        f32 = jnp.float32
        vmem = pl.BlockSpec(memory_space=pltpu.VMEM)
        precond, image, twice, image_twice, alpha, g = pl.pallas_call(
            functools.partial(kernel, counts, block, kx),
            out_shape=[pltpu.VMEM(block, f32)] * 4 + [pltpu.VMEM((1, 1, bz), f32), pltpu.VMEM(block, f32)],
            in_specs=[pl.BlockSpec(memory_space=pltpu.HBM)] * 2,
            out_specs=[vmem] * 6,
            scratch_shapes=[
                pltpu.VMEM(block, f32),
                pltpu.SemaphoreType.DMA((2,)),
                pltpu.VMEM((2, ex, ey, bz), f32),
                pltpu.VMEM((1, ex, ey, bz), f32),
                pltpu.VMEM((2, by, bz), f32),
                pltpu.VMEM((1, by, bz), f32),
                pltpu.VMEM((2, 3, 2, ey, bz), f32),
                pltpu.VMEM((2, 3, 1, ey, bz), f32),
                pltpu.VMEM((3, ex, ey, bz), f32),
                pltpu.VMEM((ex, ey, bz), f32),
                pltpu.VMEM((ex, ey, bz), f32),
                pltpu.VMEM((mx * ey, bz), f32),
                pltpu.VMEM((mx * ey, bz), f32),
                pltpu.VMEM(((mx - 2) * ey, bz), f32),
                pltpu.VMEM(((mx - 2) * ey, bz), f32),
                pltpu.VMEM((qx * my, bz), f32),
                pltpu.VMEM(((qx + 2) * my, bz), f32),
                pltpu.VMEM((my // 2, bz), f32),
                pltpu.VMEM((my // 2, bz), f32),
                pltpu.VMEM((2 * kx + 1, 3, 3, my // 2, bz), f32),
                pltpu.VMEM((2 * kx + 1, 3, 3, my // 2, bz), f32),
                pltpu.VMEM((2, planes, my, bz), f32),
                pltpu.VMEM((3, mx, my, bz), f32),
                pltpu.VMEM((3, 8, bz), f32),
                pltpu.VMEM((sum(counts), 8, bz), f32),
                pltpu.SemaphoreType.DMA((4, most)),
                pltpu.SemaphoreType.DMA((4, most)),
                pltpu.SemaphoreType.DMA((sum(counts),)),
                pltpu.SemaphoreType.DMA((sum(counts),)),
            ],
            compiler_params=pltpu.CompilerParams(collective_id=0, has_side_effects=True),
            name="relayed",
        )(right_side, coefficient)
        return (alpha * precond, g - alpha * image,
                precond - alpha * twice, image - alpha * image_twice)

    placed = (P(*AXES), P(*AXES))
    return jax.shard_map(
        shards, mesh=mesh, in_specs=placed, out_specs=(P(*AXES),) * 4, check_vma=False
    )
```

```python
import functools

import jax
import jax.numpy as jnp
from jax import lax
from jax.experimental import pallas as pl
from jax.experimental.pallas import tpu as pltpu
from jax.sharding import PartitionSpec as P

SWEEPS = 4
relaxation = 0.6

AXES = ("gx", "gy", "gz")
MESH = pl.DeviceIdType.MESH
WIDTH = 5
INNER = 3
EDGE = 8
SPAN = 2 * WIDTH
RIM = 4
PART = SWEEPS + 1


def dot(a, b):
    high = a.astype(jnp.bfloat16)
    low = (a - high.astype(jnp.float32)).astype(jnp.bfloat16)
    both = jnp.concatenate([high, low], 1)
    b = b.astype(jnp.bfloat16)
    return jnp.dot(both, jnp.concatenate([b, b], 0), preferred_element_type=jnp.float32)


def iota(shape, dim):
    return lax.broadcasted_iota(jnp.int32, shape, dim)


def total_of(values):
    while len(values) > 1:
        values = [a + b for a, b in zip(values[::2], values[1::2])] + values[len(values) & ~1:]
    return values[0]


def stages(counts):
    if max(counts) <= RIM:
        return [(0, 1, 2)]
    return [(2,), (1,), (0,)]


def partners(counts, group):
    steps = [(0, 0, 0)]
    for axis in group:
        steps = [s[:axis] + (k,) + s[axis + 1:] for s in steps for k in range(counts[axis])]
    return [s for s in steps if s != (0, 0, 0)]


def kernel(counts, block, kx, ky, g_hbm, c_hbm, pre_ref, img_ref, twice_ref, image_twice_ref, alpha_ref, g_ref,
           c_ref, gc0, im0, pk, pkx, zr, zrx, t1, d0, d1, xr0, xr1, pf0, pf1, xm, um,
           s0, s1, s2, r0, r1, r2, kept, mid, red_s, red_r, insem, ssem, rsem, lssem, lrsem):
    bx, by, bz = block
    me = [lax.axis_index(a) for a in AXES]
    ex, ey = bx + SPAN, by + 2 * EDGE
    ox, my = bx // 2, ey // 2
    qx, qy = bx // 4, by // 4
    half, quarter = bz // 2, bz // 4
    lane = iota((ey, bz), 1)
    row = iota((ey, bz), 0)
    lane8 = iota((8, bz), 1)
    row8 = iota((8, bz), 0)

    def valid(offset):
        ok = None
        for axis, step in enumerate(offset):
            if step == 0:
                continue
            place = me[axis] + step
            term = place >= 0 if step < 0 else place < counts[axis]
            ok = term if ok is None else jnp.logical_and(ok, term)
        return ok

    def target(offset):
        return tuple(m + s for m, s in zip(me, offset))

    near = [(dx, dy, dz) for dx in range(-kx, kx + 1) for dy in range(-ky, ky + 1) for dz in (-1, 0, 1)]
    near = [o for o in near if o != (0, 0, 0) and all(counts[a] > abs(o[a]) for a in range(3))]
    near.sort(key=lambda o: -sum(map(abs, o)))
    close = [o for o in near if abs(o[0]) <= 1 and abs(o[1]) <= 1]
    sides = [o for o in close if o[0] != 0 and o[2] == 0]
    later = [o for o in near if abs(o[1]) <= 1]

    groups = stages(counts)
    mates = []
    base = [0]
    for group in groups:
        mates.append(partners(counts, group))
        base.append(base[-1] + len(mates[-1]))

    def mate(step):
        return tuple(lax.rem(m + s, n) if s else m for m, s, n in zip(me, step, counts))

    copies = [pltpu.make_async_copy(src, dst, insem.at[n])
              for n, (src, dst) in enumerate(((g_hbm, g_ref), (c_hbm, c_ref)))]
    for copy in copies:
        copy.start()
    gc0[...] = jnp.zeros_like(gc0)
    zr[...] = jnp.zeros_like(zr)
    zrx[...] = jnp.zeros_like(zrx)

    barrier = pltpu.get_barrier_semaphore()
    for offset in near:
        @pl.when(valid(offset))
        def _(offset=offset):
            pl.semaphore_signal(barrier, inc=1, device_id=target(offset), device_id_type=MESH)
    greeted = 0
    if len(groups) > 1:
        for steps in mates:
            for step in steps:
                pl.semaphore_signal(barrier, inc=1, device_id=mate(step), device_id_type=MESH)
            greeted = greeted + len(steps)

    def options(axis, far):
        total = 1
        for step in range(1, far + 1):
            if counts[axis] > step:
                total = total + (me[axis] >= step).astype(jnp.int32)
                total = total + (me[axis] + step < counts[axis]).astype(jnp.int32)
        return total

    greeted = greeted + options(0, kx) * options(1, ky) * options(2, 1) - 1

    def row_ends(dy):
        if dy == 0:
            return 0, by, EDGE
        if dy > 0:
            return by - EDGE, EDGE, 0
        return 0, EDGE, EDGE + by

    def remote(src, dst, phase, n, offset):
        return pltpu.make_async_remote_copy(
            src_ref=src, dst_ref=dst, send_sem=ssem.at[phase, n], recv_sem=rsem.at[phase, n],
            device_id=target(offset), device_id_type=MESH)

    def planes_copy(phase, n, offset, first, size):
        dx, dy, dz = offset
        start, rows, goes = row_ends(dy)
        if dx == 0:
            px, tx, size = WIDTH, WIDTH, bx
        elif dx > 0:
            px, tx = WIDTH + bx - first - size, WIDTH - first - size
        else:
            px, tx = WIDTH + first, WIDTH + bx + first
        src = gc0.at[:, pl.ds(px, size), pl.ds(EDGE + start, rows), :]
        dst = gc0.at[:, pl.ds(tx, size), pl.ds(goes, rows), :]
        return remote(src, dst, phase, n, offset)

    def fine_copy(n, offset):
        dx, dy, dz = offset
        if dz == 0:
            return planes_copy(0, n, offset, 0, INNER)
        start, rows, goes = row_ends(dy)
        side = 0 if dz > 0 else 1
        if dx == 0:
            src = pk.at[:, pl.ds(start, rows), :]
            dst = zr.at[side, :, pl.ds(goes, rows), :]
        else:
            end = 0 if dx > 0 else 1
            src = pkx.at[end, pl.ds(start, rows), :]
            dst = zrx.at[side, end, pl.ds(goes, rows), :]
        return remote(src, dst, 0, n, offset)

    def outer_copy(n, offset):
        return planes_copy(1, n, offset, INNER, WIDTH - INNER)

    def part(offset, depth):
        dx, dy, dz = offset
        if abs(dx) > 1 or abs(dy) > 1:
            return 0, 1
        if dz != 0:
            return 4, 2
        if dx == 0:
            return 0, 4
        if dx < 0:
            return 0, 1 + depth
        return 4 - depth, 1 + depth

    def coarse_copy(phase, n, offset, s, r, depth):
        dx, dy, dz = offset
        at, size = part(offset, depth)
        return remote(s.at[pl.ds(at, size)], r.at[kx - dx, ky - dy, 1 - dz, pl.ds(at, size)], phase, n, offset)

    def begin(make, offsets):
        for n, offset in enumerate(offsets):
            @pl.when(valid(offset))
            def _(n=n, offset=offset):
                make(n, offset).start()

    def arrive(make, offsets):
        for n, offset in enumerate(offsets):
            @pl.when(valid(tuple(-s for s in offset)))
            def _(n=n, offset=offset):
                make(n, offset).wait_recv()

    def leave(make, offsets):
        for n, offset in enumerate(offsets):
            @pl.when(valid(offset))
            def _(n=n, offset=offset):
                make(n, offset).wait_send()

    def mate_copy(stage, k):
        n = base[stage] + k
        return pltpu.make_async_remote_copy(
            src_ref=red_s.at[stage], dst_ref=red_r.at[n], send_sem=lssem.at[n],
            recv_sem=lrsem.at[n], device_id=mate(mates[stage][k]), device_id_type=MESH)

    def sum_begin(stage, value):
        red_s[stage] = value
        for k in range(len(mates[stage])):
            mate_copy(stage, k).start()

    def sum_end(stage):
        for k in range(len(mates[stage])):
            mate_copy(stage, k).wait_recv()
        return total_of([red_s[stage]] + [red_r[base[stage] + k] for k in range(len(mates[stage]))])

    strip = (lane[:by] < WIDTH) | (lane[:by] >= bz - WIDTH)
    place = lax.rem(lane + WIDTH, bz)
    low = lax.rem(place, SPAN) < WIDTH
    band = (lane < WIDTH) | (lane >= bz - WIDTH)
    first, last = lane == 0, lane == bz - 1

    def turn_to(v, shift):
        shift = shift % bz
        return v if shift == 0 else pltpu.roll(v, shift, 1)

    def pack(planes):
        pieces = [turn_to(jnp.where(strip, plane, 0.0), SPAN * i) for i, plane in enumerate(planes)]
        ends = (total_of(pieces[bx - WIDTH:]), total_of(pieces[:WIDTH]))
        return ends, total_of(pieces[WIDTH:bx - WIDTH] + list(ends))

    def yz(a, b):
        sa = a + jnp.where(first, pltpu.roll(b, 1, 1), pltpu.roll(a, 1, 1))
        sb = b + jnp.where(first, pltpu.roll(a, 1, 1), pltpu.roll(b, 1, 1))
        sa = sa + jnp.where(last, pltpu.roll(b, bz - 1, 1), pltpu.roll(a, bz - 1, 1))
        sb = sb + jnp.where(last, pltpu.roll(a, bz - 1, 1), pltpu.roll(b, bz - 1, 1))
        sa = sa + pltpu.roll(sa, 1, 0) + pltpu.roll(sa, ey - 1, 0)
        sb = sb + pltpu.roll(sb, 1, 0) + pltpu.roll(sb, ey - 1, 0)
        return sa, sb

    def box(v):
        s = v + pltpu.roll(v, 1, 2) + pltpu.roll(v, v.shape[2] - 1, 2)
        s = s + pltpu.roll(s, 1, 1) + pltpu.roll(s, v.shape[1] - 1, 1)
        zero = jnp.zeros_like(s[:1])
        return s + jnp.concatenate([zero, s[:-1]], 0) + jnp.concatenate([s[1:], zero], 0)

    p_, q_ = iota((bz, bz), 0), iota((bz, bz), 1)
    down_a = jnp.where((p_ >> 1) == q_, 0.5, 0.0)
    down_b = jnp.where(((p_ + bz) >> 1) == q_, 0.5, 0.0)
    up_a = jnp.where((q_ >> 1) == p_, 1.0, 0.0)
    up_b = jnp.where(((q_ + bz) >> 1) == p_, 1.0, 0.0)
    down_c = jnp.where((p_ < half) & ((p_ >> 1) == lax.rem(q_, quarter)), 0.5, 0.0)
    up_c = jnp.where(p_ == jnp.where(q_ < 3 * quarter, q_ >> 1, (q_ >> 1) + half), 1.0, 0.0)

    lx = ox + 2

    def restricted(of):
        for m in range(lx):
            a0, b0 = of(2 * m + INNER)
            a1, b1 = of(2 * m + INNER + 1)
            xr0[m * ey:(m + 1) * ey, :] = a0 + a1
            xr1[m * ey:(m + 1) * ey, :] = b0 + b1
        n = lx * my
        a = xr0[pl.ds(0, n, stride=2), :] + xr0[pl.ds(1, n, stride=2), :]
        b = xr1[pl.ds(0, n, stride=2), :] + xr1[pl.ds(1, n, stride=2), :]
        return (dot(a, down_a) + dot(b, down_b)).reshape(lx, my, bz)

    turn = lane8 // quarter

    def coarsened(v):
        for m in range(qx):
            xm[m * my:(m + 1) * my, :] = v[2 * m] + v[2 * m + 1]
        n = qx * my // 2
        a = xm[pl.ds(0, n, stride=2), :] + xm[pl.ds(1, n, stride=2), :]
        a = dot(a, down_c)
        rows = my // 2
        tile = a[:rows]
        for m in range(1, qx):
            tile = jnp.where(turn == m, a[m * rows:(m + 1) * rows], tile)
        return pltpu.roll(tile, rows - 2, 0)

    rim = (lane8 < RIM) | ((lane8 >= half - RIM) & (lane8 < half))
    edge1 = my // 2 - by // 4

    def post(s, v1, tile):
        own = [v1[p][edge1:edge1 + by // 2] for p in range(ox)]
        s[0] = tile
        for k in range(ox // 2):
            s[1 + k] = jnp.where(lane8 < half, own[2 * k], pltpu.roll(own[2 * k + 1], half, 1))
        s[4] = tile
        s[5] = total_of([turn_to(jnp.where(rim, own[p], 0.0), RIM * p) for p in range(ox)])

    def middle(s, r, width):
        depth = RIM // 2 if width > 2 else 1

        def get(dx, dy, dz, k):
            if (dx, dy, dz) == (0, 0, 0):
                return s[k]
            if any(abs(d) >= n for d, n in zip((dx, dy, dz), counts)):
                return jnp.zeros((8, bz), jnp.float32)
            return r[kx + dx, ky + dy, 1 + dz, k]

        def rows(tiles):
            before, here, after = tiles
            return (pltpu.roll(jnp.where(row8 >= 4, before, here), 4, 0),
                    pltpu.roll(jnp.where(row8 >= 4, here, after), 4, 0))

        planes = []
        for dx in (-1, 0, 1):
            tiles = range(ox // 2 - depth, ox // 2) if dx < 0 else range(depth) if dx > 0 else range(ox // 2)
            ends = rows([jnp.where(lane8 < RIM * ox + RIM, get(dx, dy, 1, 5), get(dx, dy, -1, 5)) for dy in (-1, 0, 1)])
            for k in tiles:
                pair = rows([get(dx, dy, 0, 1 + k) for dy in (-1, 0, 1)])
                for odd in (0, 1):
                    p = 2 * k + odd
                    planes.append(jnp.concatenate([
                        jnp.where(lane8 < half, pltpu.roll(t, half, 1) if odd else t, turn_to(e, half - RIM * p))
                        for t, e in zip(pair, ends)], 0))
        return jnp.stack(planes)

    xs = [x for x in range(-PART, qx + PART) if -kx * qx <= x < (kx + 1) * qx]

    def gathered(s, r, far):
        zero = jnp.zeros((8, bz), jnp.float32)

        def get(dx, dy, dz):
            if (dx, dy, dz) == (0, 0, 0):
                return s[0]
            if any(abs(d) >= n for d, n in zip((dx, dy, dz), counts)) or abs(dy) > far:
                return zero
            return r[kx + dx, ky + dy, 1 + dz, part((-dx, -dy, -dz), 0)[0]]

        columns = {}
        for dx in sorted({x // qx for x in xs}):
            for dy in range(-2, 3):
                if abs(dy) > far:
                    continue
                here = get(dx, dy, 0)
                after = pltpu.roll(get(dx, dy, 1), quarter, 1)
                before = pltpu.roll(get(dx, dy, -1), 3 * quarter, 1)
                for m in range(qx):
                    tile = jnp.where(turn == (m + 1) % 4, after, here)
                    tile = jnp.where(turn == (m + 3) % 4, before, tile)
                    columns[dx * qx + m, dy] = turn_to(tile, -quarter * m)
        planes = []
        for x in xs:
            t = {dy: columns.get((x, dy), zero) for dy in range(-2, 3)}
            upper = jnp.where(row8 < qy, t[-1], pltpu.roll(t[0], 4, 0))
            if far > 1:
                lower = jnp.where(row8 < qy, t[1], pltpu.roll(jnp.where(row8 < 2, t[2], t[-2]), 4, 0))
            else:
                lower = jnp.where(row8 < qy, t[1], 0.0)
            planes.append(jnp.concatenate([upper, lower], 0))
        return jnp.stack(planes)

    def within(place, axis, size):
        place = place + me[axis] * size
        return (place >= 0) & (place < counts[axis] * size)

    for copy in copies:
        copy.wait()
    g = [g_ref[i] for i in range(bx)]
    c = [c_ref[i] for i in range(bx)]
    for i in range(bx):
        gc0[0, WIDTH + i, EDGE:EDGE + by, :] = g[i]
        gc0[1, WIDTH + i, EDGE:EDGE + by, :] = c[i]
    (g_last, g_first), pk[0] = pack(g)
    (c_last, c_first), pk[1] = pack(c)
    pkx[0] = g_last + turn_to(c_last, -SPAN * WIDTH)
    pkx[1] = g_first + turn_to(c_first, SPAN * WIDTH)
    pl.semaphore_wait(barrier, greeted)
    begin(fine_copy, close)

    for m in range(ox):
        xr0[m * ey + EDGE:m * ey + EDGE + by, :] = c[2 * m] + c[2 * m + 1]
    n = ox * my
    own1 = xr0[pl.ds(0, n, stride=2), :] + xr0[pl.ds(1, n, stride=2), :]
    own1 = dot(own1, down_a).reshape(ox, my, bz)
    post(s0, own1, coarsened(own1))
    make_c = lambda n, o: coarse_copy(2, n, o, s0, r0, RIM // 2)
    make_b = lambda n, o: coarse_copy(3, n, o, s1, r1, RIM // 2)
    make_d = lambda n, o: coarse_copy(4, n, o, s2, r2, 1)
    begin(outer_copy, sides)
    begin(make_c, near)

    in_y = within(row - EDGE, 1, by)
    in_z = band & within(jnp.where(lane < half, lane + bz, lane - bz), 2, bz)

    def spread(i):
        for f in range(2):
            if i < WIDTH:
                k = i
                piece = turn_to(ends[0], -SPAN * (bx - WIDTH + k - WIDTH * f))
            elif i >= WIDTH + bx:
                k = i - WIDTH - bx
                piece = turn_to(ends[1], -SPAN * (k + WIDTH * f))
            else:
                piece = turn_to(merged[f], -SPAN * (i - WIDTH))
            t1[f, i] = jnp.where(band, piece, 0.0)
        in_x = within(jnp.full((ey, bz), i - WIDTH, jnp.int32), 0, bx)
        d0[i] = jnp.where(in_y & in_x, relaxation / (26.0 + gc0[1, i]), 0.0)
        d1[i] = jnp.where(in_y & in_x & in_z, relaxation / (26.0 + t1[1, i]), 0.0)

    arrive(fine_copy, close)
    merged = [jnp.where(low, zr[0, f], zr[1, f]) for f in range(2)]
    ends = [jnp.where(low, zrx[0, e], zrx[1, e]) for e in range(2)]
    skip = WIDTH - INNER
    for i in range(skip, ex - skip):
        spread(i)

    def inside1(shape, width):
        zl = iota(shape, 2)
        zl = jnp.where(zl < 3 * quarter, zl, zl - bz)
        ok = within(iota(shape, 0) - width, 0, ox) & within(iota(shape, 1) - edge1, 1, by // 2)
        return ok & within(zl, 2, half) & (zl >= -RIM) & (zl < half + RIM)

    c1 = restricted(lambda i: (gc0[1, i], t1[1, i]))
    near0 = jnp.where(inside1((lx, my, bz), 1), relaxation / (26.0 + c1), 0.0)
    near1 = 27.0 + c1

    def coefficients():
        arrive(outer_copy, sides)
        for i in list(range(skip)) + list(range(ex - skip, ex)):
            spread(i)
        arrive(make_c, near)
        c1 = middle(s0, r0, RIM)
        ok = inside1(c1.shape, RIM)
        c1 = jnp.where(ok, c1, 0.0)
        mid[0] = jnp.where(ok, relaxation / (26.0 + c1), 0.0)
        mid[1] = 27.0 + c1
        c2 = gathered(s0, r0, ky)
        shape = c2.shape
        z = iota(shape, 2)
        z = jnp.where(z < 2 * quarter, z, z - bz)
        y = iota(shape, 1)
        y = jnp.where(y < my - 2, y, y - my) - qy
        ok = within(iota(shape, 0) + xs[0], 0, qx) & within(y, 1, qy)
        ok = ok & within(z, 2, quarter) & (z >= -quarter)
        c2 = jnp.where(ok, c2, 0.0)
        kept[0] = jnp.where(ok, relaxation / (26.0 + c2), 0.0)
        kept[1] = 27.0 + c2

    def cycle(g_at, near0, near1, s, r, make, offsets, far, width, hook, second, finish):
        def e0(i):
            a, b = g_at(i)
            return d0[i] * a, d1[i] * b

        sums = {}

        def remainder(i):
            for k in (i - 1, i, i + 1):
                if k not in sums:
                    sums[k] = yz(*e0(k))
            a, b = g_at(i)
            ea, eb = e0(i)
            ra = a - (27.0 + gc0[1, i]) * ea + sums[i - 1][0] + sums[i][0] + sums[i + 1][0]
            rb = b - (27.0 + t1[1, i]) * eb + sums[i - 1][1] + sums[i][1] + sums[i + 1][1]
            return ra, rb

        g1 = restricted(remainder)
        f = near0 * g1
        post(s, g1[1:1 + ox], coarsened((g1 - near1 * f + box(f))[1:1 + ox]))
        begin(make, offsets)
        hook()
        arrive(make, offsets)
        inv, diag = kept[0], kept[1]
        g2 = jnp.where(inv > 0.0, gathered(s, r, far), 0.0)
        e = inv * g2
        for sweep in range(SWEEPS - 1):
            e = e + inv * (g2 - diag * e + box(e))
        second()
        reach = (width + 1) // 2
        nq = qx + 2 * reach
        zero = jnp.zeros_like(e[:1])
        e = jnp.concatenate([e[xs.index(x)][None] if x in xs else zero for x in range(-reach, qx + reach)], 0)
        e = pltpu.roll(e, my - 2, 1)[:, :my // 2].reshape(nq * my // 2, bz)
        u = dot(e, up_c)
        um[pl.ds(0, nq * my // 2, stride=2), :] = u
        um[pl.ds(1, nq * my // 2, stride=2), :] = u
        u = um[:nq * my, :].reshape(nq, my, bz)
        span = width + 1
        mx = ox + 2 * span
        u = jnp.concatenate([u[(m - span) // 2 + reach][None] for m in range(mx)], 0)
        skip1 = RIM - span
        inv, diag = mid[0, skip1:skip1 + mx], mid[1, skip1:skip1 + mx]
        g1 = jnp.where(inv > 0.0, middle(s, r, span), 0.0)
        f = inv * g1 + u
        f = f + inv * (g1 - diag * f + box(f))
        nm = mx - 2
        f = f[1:mx - 1].reshape(nm * my, bz)
        for pf, up in ((pf0, up_a), (pf1, up_b)):
            w = dot(f, up)
            pf[pl.ds(0, nm * my, stride=2), :] = w
            pf[pl.ds(1, nm * my, stride=2), :] = w

        def e1(i):
            m = (i - WIDTH) // 2 + width
            a, b = e0(i)
            return a + pf0[m * ey:(m + 1) * ey, :], b + pf1[m * ey:(m + 1) * ey, :]

        sums1, sums2 = {}, {}
        e2 = {}
        wide = width > 1
        past = INNER + 1 if wide else 1
        for i in range(WIDTH - past, WIDTH + bx + past):
            for k in (i - 1, i, i + 1):
                if k not in sums1:
                    sums1[k] = yz(*e1(k))
            ga, gb = g_at(i)
            ea, eb = e1(i)
            s_ = [sums1[i - 1][t] + sums1[i][t] + sums1[i + 1][t] for t in range(2)]
            za = ea + d0[i] * (ga - (27.0 + gc0[1, i]) * ea + s_[0])
            zb = eb + d1[i] * (gb - (27.0 + t1[1, i]) * eb + s_[1])
            e2[i] = za, zb
            sums2[i] = yz(za, zb)
            k = i - 1
            if k - 1 in sums2:
                around = [sums2[k - 1][t] + sums2[k][t] + sums2[k + 1][t] for t in range(2)]
                za, zb = e2[k]
                finish(k, za, (27.0 + gc0[1, k]) * za - around[0],
                       (27.0 + t1[1, k]) * zb - around[1] if wide else None)

    gamma, delta = [], []

    def own(i):
        return WIDTH <= i < WIDTH + bx

    def finish1(i, e, out, out_b):
        im0[0, i] = out
        im0[1, i] = out_b
        if own(i):
            e, out = e[EDGE:EDGE + by], out[EDGE:EDGE + by]
            pre_ref[i - WIDTH] = e
            img_ref[i - WIDTH] = out
            gamma.append(g_ref[i - WIDTH] * e)
            delta.append(out * e)
        if i == WIDTH + bx - 1:
            gs = jnp.sum(total_of(gamma), axis=0, keepdims=True)
            ds = jnp.sum(total_of(delta), axis=0, keepdims=True)
            gs, ds = gs + pltpu.roll(gs, half, 1), ds + pltpu.roll(ds, half, 1)
            sum_begin(0, jnp.where(lane8[:1] < half, gs, ds))

    nothing = lambda: None
    cycle(lambda i: (gc0[0, i], t1[0, i]), near0, near1, s1, r1, make_b, near, ky, RIM - 1, coefficients, nothing, finish1)

    def relay(stage):
        if len(groups) > 1:
            sum_begin(stage, sum_end(stage - 1))

    def finish2(i, e, out, out_b):
        twice_ref[i - WIDTH] = e[EDGE:EDGE + by]
        image_twice_ref[i - WIDTH] = out[EDGE:EDGE + by]

    skip1 = RIM - 1
    cycle(lambda i: (im0[0, i], im0[1, i]), mid[0, skip1:skip1 + lx], mid[1, skip1:skip1 + lx], s2, r2, make_d, later, 1, 1,
          lambda: relay(1), lambda: relay(2), finish2)

    total = sum_end(len(groups) - 1)
    gs = jnp.sum(jnp.where(lane8[:1] < half, total, 0.0), axis=1, keepdims=True)
    ds = jnp.sum(jnp.where(lane8[:1] < half, 0.0, total), axis=1, keepdims=True)
    alpha_ref[...] = jnp.broadcast_to(gs / ds, (1, bz)).reshape(alpha_ref.shape)
    leave(fine_copy, close)
    leave(outer_copy, sides)
    leave(make_c, near)
    leave(make_b, near)
    leave(make_d, later)
    for stage in range(len(groups)):
        for k in range(len(mates[stage])):
            mate_copy(stage, k).wait_send()


def solution(mesh):
    counts = tuple(mesh.shape[a] for a in AXES)

    def shards(right_side, coefficient):
        bx, by, bz = block = right_side.shape
        assert SPAN <= bx and SPAN * bx <= bz and by == 16 and bx % 4 == 0
        kx = max(1, min(-(-PART // (bx // 4)), counts[0] - 1))
        ky = max(1, min(-(-PART // (by // 4)), counts[1] - 1))
        ex, ey = bx + SPAN, by + 2 * EDGE
        ox, my = bx // 2, ey // 2
        qx = bx // 4
        mx = ox + 2 * RIM
        most = (2 * kx + 1) * (2 * ky + 1) * 3
        planes = len([x for x in range(-PART, qx + PART) if -kx * qx <= x < (kx + 1) * qx])
        mates = [len(partners(counts, group)) for group in stages(counts)]
        f32 = jnp.float32
        vmem = pl.BlockSpec(memory_space=pltpu.VMEM)
        messages = [pltpu.VMEM((6, 8, bz), f32)] * 3
        messages += [pltpu.VMEM((2 * kx + 1, 2 * ky + 1, 3, 6, 8, bz), f32)] * 3
        precond, image, twice, image_twice, alpha, g = pl.pallas_call(
            functools.partial(kernel, counts, block, kx, ky),
            out_shape=[pltpu.VMEM(block, f32)] * 4 + [pltpu.VMEM((1, 1, bz), f32), pltpu.VMEM(block, f32)],
            in_specs=[pl.BlockSpec(memory_space=pltpu.HBM)] * 2,
            out_specs=[vmem] * 6,
            scratch_shapes=[
                pltpu.VMEM(block, f32),
                pltpu.VMEM((2, ex, ey, bz), f32),
                pltpu.VMEM((2, ex, ey, bz), f32),
                pltpu.VMEM((2, by, bz), f32),
                pltpu.VMEM((2, by, bz), f32),
                pltpu.VMEM((2, 2, ey, bz), f32),
                pltpu.VMEM((2, 2, ey, bz), f32),
                pltpu.VMEM((2, ex, ey, bz), f32),
                pltpu.VMEM((ex, ey, bz), f32),
                pltpu.VMEM((ex, ey, bz), f32),
                pltpu.VMEM(((ox + 2) * ey, bz), f32),
                pltpu.VMEM(((ox + 2) * ey, bz), f32),
                pltpu.VMEM(((mx - 2) * ey, bz), f32),
                pltpu.VMEM(((mx - 2) * ey, bz), f32),
                pltpu.VMEM((qx * my, bz), f32),
                pltpu.VMEM(((qx + 4) * my, bz), f32),
                *messages,
                pltpu.VMEM((2, planes, my, bz), f32),
                pltpu.VMEM((2, mx, my, bz), f32),
                pltpu.VMEM((len(mates), 1, bz), f32),
                pltpu.VMEM((sum(mates), 1, bz), f32),
                pltpu.SemaphoreType.DMA((2,)),
                pltpu.SemaphoreType.DMA((5, most)),
                pltpu.SemaphoreType.DMA((5, most)),
                pltpu.SemaphoreType.DMA((sum(mates),)),
                pltpu.SemaphoreType.DMA((sum(mates),)),
            ],
            compiler_params=pltpu.CompilerParams(collective_id=0, has_side_effects=True),
            name="relayed",
        )(right_side, coefficient)
        return (alpha * precond, g - alpha * image,
                precond - alpha * twice, image - alpha * image_twice)

    placed = (P(*AXES), P(*AXES))
    return jax.shard_map(
        shards, mesh=mesh, in_specs=placed, out_specs=(P(*AXES),) * 4, check_vma=False
    )
```

```python
import functools
import itertools

import jax
import jax.numpy as jnp
from jax import lax
from jax.experimental import pallas as pl
from jax.experimental.pallas import tpu as pltpu
from jax.sharding import PartitionSpec as P

SWEEPS = 4
relaxation = 0.6

AXES = ("gx", "gy", "gz")
MESH = pl.DeviceIdType.MESH
WIDTH = 5
INNER = 3
EDGE = 8
SPAN = 2 * WIDTH
RIM = 4
PART = SWEEPS + 1


def dot(a, b):
    high = a.astype(jnp.bfloat16)
    low = (a - high.astype(jnp.float32)).astype(jnp.bfloat16)
    both = jnp.concatenate([high, low], 1)
    b = b.astype(jnp.bfloat16)
    return jnp.dot(both, jnp.concatenate([b, b], 0), preferred_element_type=jnp.float32)


def iota(shape, dim):
    return lax.broadcasted_iota(jnp.int32, shape, dim)


def total_of(values):
    while len(values) > 1:
        values = [a + b for a, b in zip(values[::2], values[1::2])] + values[len(values) & ~1:]
    return values[0]


def stages(counts):
    if max(counts) <= RIM:
        return [(0, 1, 2)]
    return [(2,), (1,), (0,)]


def partners(counts, group):
    steps = [(0, 0, 0)]
    for axis in group:
        steps = [s[:axis] + (k,) + s[axis + 1:] for s in steps for k in range(counts[axis])]
    return [s for s in steps if s != (0, 0, 0)]


def kernel(counts, block, kx, ky, g_hbm, c_hbm, pre_ref, img_ref, twice_ref, image_twice_ref, alpha_ref, g_ref,
           c_ref, gc0, im0, pk, pkx, zr, zrx, t1, d0, d1, xr0, xr1, pf0, pf1, xm, um,
           s0, s1, s2, r0, r1, r2, kept, mid, red_s, red_r, units, insem, ssem, rsem, lssem, lrsem):
    bx, by, bz = block
    me = [lax.axis_index(a) for a in AXES]
    ex, ey = bx + SPAN, by + 2 * EDGE
    ox, my = bx // 2, ey // 2
    qx, qy = bx // 4, by // 4
    half, quarter = bz // 2, bz // 4
    lane = iota((ey, bz), 1)
    row = iota((ey, bz), 0)
    lane8 = iota((8, bz), 1)
    row8 = iota((8, bz), 0)

    def valid(offset):
        ok = None
        for axis, step in enumerate(offset):
            if step == 0:
                continue
            place = me[axis] + step
            term = place >= 0 if step < 0 else place < counts[axis]
            ok = term if ok is None else jnp.logical_and(ok, term)
        return ok

    def target(offset):
        return tuple(m + s for m, s in zip(me, offset))

    near = [(dx, dy, dz) for dx in range(-kx, kx + 1) for dy in range(-ky, ky + 1) for dz in (-1, 0, 1)]
    near = [o for o in near if o != (0, 0, 0) and all(counts[a] > abs(o[a]) for a in range(3))]
    near.sort(key=lambda o: -sum(map(abs, o)))
    close = [o for o in near if abs(o[0]) <= 1 and abs(o[1]) <= 1]
    sides = [o for o in close if o[0] != 0 and o[2] == 0]
    later = [o for o in near if abs(o[1]) <= 1]

    groups = stages(counts)
    mates = []
    base = [0]
    for group in groups:
        mates.append(partners(counts, group))
        base.append(base[-1] + len(mates[-1]))

    def mate(step):
        return tuple(lax.rem(m + s, n) if s else m for m, s, n in zip(me, step, counts))

    copies = [pltpu.make_async_copy(src, dst, insem.at[n])
              for n, (src, dst) in enumerate(((g_hbm, g_ref), (c_hbm, c_ref)))]
    for copy in copies:
        copy.start()
    gc0[...] = jnp.zeros_like(gc0)
    zr[...] = jnp.zeros_like(zr)
    zrx[...] = jnp.zeros_like(zrx)

    barrier = pltpu.get_barrier_semaphore()
    for offset in near:
        @pl.when(valid(offset))
        def _(offset=offset):
            pl.semaphore_signal(barrier, inc=1, device_id=target(offset), device_id_type=MESH)
    greeted = 0
    if len(groups) > 1:
        for steps in mates:
            for step in steps:
                pl.semaphore_signal(barrier, inc=1, device_id=mate(step), device_id_type=MESH)
            greeted = greeted + len(steps)

    def options(axis, far):
        total = 1
        for step in range(1, far + 1):
            if counts[axis] > step:
                total = total + (me[axis] >= step).astype(jnp.int32)
                total = total + (me[axis] + step < counts[axis]).astype(jnp.int32)
        return total

    greeted = greeted + options(0, kx) * options(1, ky) * options(2, 1) - 1

    def row_ends(dy):
        if dy == 0:
            return 0, by, EDGE
        if dy > 0:
            return by - EDGE, EDGE, 0
        return 0, EDGE, EDGE + by

    def remote(src, dst, phase, offset):
        pltpu.make_async_remote_copy(
            src_ref=src, dst_ref=dst, send_sem=ssem, recv_sem=rsem.at[phase],
            device_id=target(offset), device_id_type=MESH).start()

    def planes_copy(phase, offset, first, size):
        dx, dy, dz = offset
        start, rows, goes = row_ends(dy)
        if dx == 0:
            px, tx, size = WIDTH, WIDTH, bx
        elif dx > 0:
            px, tx = WIDTH + bx - first - size, WIDTH - first - size
        else:
            px, tx = WIDTH + first, WIDTH + bx + first
        src = gc0.at[:, pl.ds(px, size), pl.ds(EDGE + start, rows), :]
        dst = gc0.at[:, pl.ds(tx, size), pl.ds(goes, rows), :]
        return (src, dst, phase, offset)

    def fine_copy(offset):
        dx, dy, dz = offset
        if dz == 0:
            return planes_copy(0, offset, 0, INNER)
        start, rows, goes = row_ends(dy)
        side = 0 if dz > 0 else 1
        if dx == 0:
            src = pk.at[:, pl.ds(start, rows), :]
            dst = zr.at[side, :, pl.ds(goes, rows), :]
        else:
            end = 0 if dx > 0 else 1
            src = pkx.at[end, pl.ds(start, rows), :]
            dst = zrx.at[side, end, pl.ds(goes, rows), :]
        return (src, dst, 0, offset)

    def outer_copy(offset):
        return planes_copy(1, offset, INNER, WIDTH - INNER)

    def part(offset, depth):
        dx, dy, dz = offset
        if abs(dx) > 1 or abs(dy) > 1:
            return 0, 1
        if dz != 0:
            return 4, 2
        if dx == 0:
            return 0, 4
        if dx < 0:
            return 0, 1 + depth
        return 4 - depth, 1 + depth

    def coarse_copy(phase, offset, s, r, depth):
        dx, dy, dz = offset
        at, size = part(offset, depth)
        return (s.at[pl.ds(at, size)], r.at[kx - dx, ky - dy, 1 - dz, pl.ds(at, size)], phase, offset)

    def tiles(make, offset):
        size = 1
        for n in make(offset)[0].shape:
            size *= n
        assert size % (8 * bz) == 0
        return size // (8 * bz)

    def begin(make, offsets):
        for offset in offsets:
            @pl.when(valid(offset))
            def _(offset=offset):
                remote(*make(offset))

    def wait_for(sem, pairs):
        sizes = {}
        for make, offsets in pairs:
            for offset in offsets:
                key = tuple(map(abs, offset))
                sizes.setdefault(key, 0)
                if offset == key:
                    sizes[key] += tiles(make, offset)

        def amount(options):
            total = 0
            for (a, b, c), size in sizes.items():
                total = total + size * options[0][a] * options[1][b] * options[2][c]
            return total

        def number(place, count, step):
            return 1 if step == 0 else (place >= step) * 1 + (place + step < count) * 1

        def table(axis, place):
            return [number(place, counts[axis], k) for k in range(3)]

        here = []
        for axis in range(3):
            has = [1]
            for k in (1, 2):
                n = (me[axis] >= k).astype(jnp.int32) + (me[axis] + k < counts[axis]).astype(jnp.int32)
                has.append(n)
            here.append(has)
        total = amount(here)
        for value in sorted({amount(options) for options in itertools.product(
                *[[table(axis, place) for place in range(counts[axis])] for axis in range(3)])}):
            @pl.when(total == value)
            def _(value=value):
                some = units.at[pl.ds(0, value)]
                pltpu.make_async_copy(some, some, sem).wait()

    def arrive(phase, make, offsets):
        wait_for(rsem.at[phase], [(make, offsets)])

    def leave(pairs):
        wait_for(ssem, pairs)

    def mate_copy(stage, k):
        n = base[stage] + k
        return pltpu.make_async_remote_copy(
            src_ref=red_s.at[stage], dst_ref=red_r.at[n], send_sem=lssem.at[stage],
            recv_sem=lrsem.at[stage], device_id=mate(mates[stage][k]), device_id_type=MESH)

    def sum_begin(stage, value):
        red_s[stage] = value
        for k in range(len(mates[stage])):
            mate_copy(stage, k).start()

    def sum_end(stage):
        some = red_r.at[pl.ds(base[stage], len(mates[stage]))]
        pltpu.make_async_copy(some, some, lrsem.at[stage]).wait()
        return total_of([red_s[stage]] + [red_r[base[stage] + k] for k in range(len(mates[stage]))])

    strip = (lane[:by] < WIDTH) | (lane[:by] >= bz - WIDTH)
    place = lax.rem(lane + WIDTH, bz)
    low = lax.rem(place, SPAN) < WIDTH
    band = (lane < WIDTH) | (lane >= bz - WIDTH)
    first, last = lane == 0, lane == bz - 1

    def turn_to(v, shift):
        shift = shift % bz
        return v if shift == 0 else pltpu.roll(v, shift, 1)

    def pack(planes):
        pieces = [turn_to(jnp.where(strip, plane, 0.0), SPAN * i) for i, plane in enumerate(planes)]
        ends = (total_of(pieces[bx - WIDTH:]), total_of(pieces[:WIDTH]))
        return ends, total_of(pieces[WIDTH:bx - WIDTH] + list(ends))

    def yz(a, b):
        sa = a + jnp.where(first, pltpu.roll(b, 1, 1), pltpu.roll(a, 1, 1))
        sb = b + jnp.where(first, pltpu.roll(a, 1, 1), pltpu.roll(b, 1, 1))
        sa = sa + jnp.where(last, pltpu.roll(b, bz - 1, 1), pltpu.roll(a, bz - 1, 1))
        sb = sb + jnp.where(last, pltpu.roll(a, bz - 1, 1), pltpu.roll(b, bz - 1, 1))
        sa = sa + pltpu.roll(sa, 1, 0) + pltpu.roll(sa, ey - 1, 0)
        sb = sb + pltpu.roll(sb, 1, 0) + pltpu.roll(sb, ey - 1, 0)
        return sa, sb

    def box(v):
        s = v + pltpu.roll(v, 1, 2) + pltpu.roll(v, v.shape[2] - 1, 2)
        s = s + pltpu.roll(s, 1, 1) + pltpu.roll(s, v.shape[1] - 1, 1)
        zero = jnp.zeros_like(s[:1])
        return s + jnp.concatenate([zero, s[:-1]], 0) + jnp.concatenate([s[1:], zero], 0)

    p_, q_ = iota((bz, bz), 0), iota((bz, bz), 1)
    down_a = jnp.where((p_ >> 1) == q_, 0.5, 0.0)
    down_b = jnp.where(((p_ + bz) >> 1) == q_, 0.5, 0.0)
    up_a = jnp.where((q_ >> 1) == p_, 1.0, 0.0)
    up_b = jnp.where(((q_ + bz) >> 1) == p_, 1.0, 0.0)
    down_c = jnp.where((p_ < half) & ((p_ >> 1) == lax.rem(q_, quarter)), 0.5, 0.0)
    up_c = jnp.where(p_ == jnp.where(q_ < 3 * quarter, q_ >> 1, (q_ >> 1) + half), 1.0, 0.0)

    lx = ox + 2

    def restricted(of):
        for m in range(lx):
            a0, b0 = of(2 * m + INNER)
            a1, b1 = of(2 * m + INNER + 1)
            xr0[m * ey:(m + 1) * ey, :] = a0 + a1
            xr1[m * ey:(m + 1) * ey, :] = b0 + b1
        n = lx * my
        a = xr0[pl.ds(0, n, stride=2), :] + xr0[pl.ds(1, n, stride=2), :]
        b = xr1[pl.ds(0, n, stride=2), :] + xr1[pl.ds(1, n, stride=2), :]
        return (dot(a, down_a) + dot(b, down_b)).reshape(lx, my, bz)

    turn = lane8 // quarter

    def coarsened(v):
        for m in range(qx):
            xm[m * my:(m + 1) * my, :] = v[2 * m] + v[2 * m + 1]
        n = qx * my // 2
        a = xm[pl.ds(0, n, stride=2), :] + xm[pl.ds(1, n, stride=2), :]
        a = dot(a, down_c)
        rows = my // 2
        tile = a[:rows]
        for m in range(1, qx):
            tile = jnp.where(turn == m, a[m * rows:(m + 1) * rows], tile)
        return pltpu.roll(tile, rows - 2, 0)

    rim = (lane8 < RIM) | ((lane8 >= half - RIM) & (lane8 < half))
    edge1 = my // 2 - by // 4

    def post(s, v1, tile):
        own = [v1[p][edge1:edge1 + by // 2] for p in range(ox)]
        s[0] = tile
        for k in range(ox // 2):
            s[1 + k] = jnp.where(lane8 < half, own[2 * k], pltpu.roll(own[2 * k + 1], half, 1))
        s[4] = tile
        s[5] = total_of([turn_to(jnp.where(rim, own[p], 0.0), RIM * p) for p in range(ox)])

    def middle(s, r, width):
        depth = RIM // 2 if width > 2 else 1

        def get(dx, dy, dz, k):
            if (dx, dy, dz) == (0, 0, 0):
                return s[k]
            if any(abs(d) >= n for d, n in zip((dx, dy, dz), counts)):
                return jnp.zeros((8, bz), jnp.float32)
            return r[kx + dx, ky + dy, 1 + dz, k]

        def rows(tiles):
            before, here, after = tiles
            return (pltpu.roll(jnp.where(row8 >= 4, before, here), 4, 0),
                    pltpu.roll(jnp.where(row8 >= 4, here, after), 4, 0))

        planes = []
        for dx in (-1, 0, 1):
            tiles = range(ox // 2 - depth, ox // 2) if dx < 0 else range(depth) if dx > 0 else range(ox // 2)
            ends = rows([jnp.where(lane8 < RIM * ox + RIM, get(dx, dy, 1, 5), get(dx, dy, -1, 5)) for dy in (-1, 0, 1)])
            for k in tiles:
                pair = rows([get(dx, dy, 0, 1 + k) for dy in (-1, 0, 1)])
                for odd in (0, 1):
                    p = 2 * k + odd
                    planes.append(jnp.concatenate([
                        jnp.where(lane8 < half, pltpu.roll(t, half, 1) if odd else t, turn_to(e, half - RIM * p))
                        for t, e in zip(pair, ends)], 0))
        return jnp.stack(planes)

    xs = [x for x in range(-PART, qx + PART) if -kx * qx <= x < (kx + 1) * qx]

    def gathered(s, r, far):
        zero = jnp.zeros((8, bz), jnp.float32)

        def get(dx, dy, dz):
            if (dx, dy, dz) == (0, 0, 0):
                return s[0]
            if any(abs(d) >= n for d, n in zip((dx, dy, dz), counts)) or abs(dy) > far:
                return zero
            return r[kx + dx, ky + dy, 1 + dz, part((-dx, -dy, -dz), 0)[0]]

        columns = {}
        for dx in sorted({x // qx for x in xs}):
            for dy in range(-2, 3):
                if abs(dy) > far:
                    continue
                here = get(dx, dy, 0)
                after = pltpu.roll(get(dx, dy, 1), quarter, 1)
                before = pltpu.roll(get(dx, dy, -1), 3 * quarter, 1)
                for m in range(qx):
                    tile = jnp.where(turn == (m + 1) % 4, after, here)
                    tile = jnp.where(turn == (m + 3) % 4, before, tile)
                    columns[dx * qx + m, dy] = turn_to(tile, -quarter * m)
        planes = []
        for x in xs:
            t = {dy: columns.get((x, dy), zero) for dy in range(-2, 3)}
            upper = jnp.where(row8 < qy, t[-1], pltpu.roll(t[0], 4, 0))
            if far > 1:
                lower = jnp.where(row8 < qy, t[1], pltpu.roll(jnp.where(row8 < 2, t[2], t[-2]), 4, 0))
            else:
                lower = jnp.where(row8 < qy, t[1], 0.0)
            planes.append(jnp.concatenate([upper, lower], 0))
        return jnp.stack(planes)

    def within(place, axis, size):
        place = place + me[axis] * size
        return (place >= 0) & (place < counts[axis] * size)

    for copy in copies:
        copy.wait()
    g = [g_ref[i] for i in range(bx)]
    c = [c_ref[i] for i in range(bx)]
    for i in range(bx):
        gc0[0, WIDTH + i, EDGE:EDGE + by, :] = g[i]
        gc0[1, WIDTH + i, EDGE:EDGE + by, :] = c[i]
    (g_last, g_first), pk[0] = pack(g)
    (c_last, c_first), pk[1] = pack(c)
    pkx[0] = g_last + turn_to(c_last, -SPAN * WIDTH)
    pkx[1] = g_first + turn_to(c_first, SPAN * WIDTH)
    pl.semaphore_wait(barrier, greeted)
    begin(fine_copy, close)

    for m in range(ox):
        xr0[m * ey + EDGE:m * ey + EDGE + by, :] = c[2 * m] + c[2 * m + 1]
    n = ox * my
    own1 = xr0[pl.ds(0, n, stride=2), :] + xr0[pl.ds(1, n, stride=2), :]
    own1 = dot(own1, down_a).reshape(ox, my, bz)
    post(s0, own1, coarsened(own1))
    make_c = lambda o: coarse_copy(2, o, s0, r0, RIM // 2)
    make_b = lambda o: coarse_copy(3, o, s1, r1, RIM // 2)
    make_d = lambda o: coarse_copy(4, o, s2, r2, 1)
    begin(outer_copy, sides)
    begin(make_c, near)

    in_y = within(row - EDGE, 1, by)
    in_z = band & within(jnp.where(lane < half, lane + bz, lane - bz), 2, bz)

    def spread(i):
        for f in range(2):
            if i < WIDTH:
                k = i
                piece = turn_to(ends[0], -SPAN * (bx - WIDTH + k - WIDTH * f))
            elif i >= WIDTH + bx:
                k = i - WIDTH - bx
                piece = turn_to(ends[1], -SPAN * (k + WIDTH * f))
            else:
                piece = turn_to(merged[f], -SPAN * (i - WIDTH))
            t1[f, i] = jnp.where(band, piece, 0.0)
        in_x = within(jnp.full((ey, bz), i - WIDTH, jnp.int32), 0, bx)
        d0[i] = jnp.where(in_y & in_x, relaxation / (26.0 + gc0[1, i]), 0.0)
        d1[i] = jnp.where(in_y & in_x & in_z, relaxation / (26.0 + t1[1, i]), 0.0)

    arrive(0, fine_copy, close)
    merged = [jnp.where(low, zr[0, f], zr[1, f]) for f in range(2)]
    ends = [jnp.where(low, zrx[0, e], zrx[1, e]) for e in range(2)]
    skip = WIDTH - INNER
    for i in range(skip, ex - skip):
        spread(i)

    def inside1(shape, width):
        zl = iota(shape, 2)
        zl = jnp.where(zl < 3 * quarter, zl, zl - bz)
        ok = within(iota(shape, 0) - width, 0, ox) & within(iota(shape, 1) - edge1, 1, by // 2)
        return ok & within(zl, 2, half) & (zl >= -RIM) & (zl < half + RIM)

    c1 = restricted(lambda i: (gc0[1, i], t1[1, i]))
    near0 = jnp.where(inside1((lx, my, bz), 1), relaxation / (26.0 + c1), 0.0)
    near1 = 27.0 + c1

    def coefficients():
        arrive(1, outer_copy, sides)
        for i in list(range(skip)) + list(range(ex - skip, ex)):
            spread(i)
        arrive(2, make_c, near)
        c1 = middle(s0, r0, RIM)
        ok = inside1(c1.shape, RIM)
        c1 = jnp.where(ok, c1, 0.0)
        mid[0] = jnp.where(ok, relaxation / (26.0 + c1), 0.0)
        mid[1] = 27.0 + c1
        c2 = gathered(s0, r0, ky)
        shape = c2.shape
        z = iota(shape, 2)
        z = jnp.where(z < 2 * quarter, z, z - bz)
        y = iota(shape, 1)
        y = jnp.where(y < my - 2, y, y - my) - qy
        ok = within(iota(shape, 0) + xs[0], 0, qx) & within(y, 1, qy)
        ok = ok & within(z, 2, quarter) & (z >= -quarter)
        c2 = jnp.where(ok, c2, 0.0)
        kept[0] = jnp.where(ok, relaxation / (26.0 + c2), 0.0)
        kept[1] = 27.0 + c2

    def cycle(phase, g_at, near0, near1, s, r, make, offsets, far, width, hook, second, finish):
        def e0(i):
            a, b = g_at(i)
            return d0[i] * a, d1[i] * b

        sums = {}

        def remainder(i):
            for k in (i - 1, i, i + 1):
                if k not in sums:
                    sums[k] = yz(*e0(k))
            a, b = g_at(i)
            ea, eb = e0(i)
            ra = a - (27.0 + gc0[1, i]) * ea + sums[i - 1][0] + sums[i][0] + sums[i + 1][0]
            rb = b - (27.0 + t1[1, i]) * eb + sums[i - 1][1] + sums[i][1] + sums[i + 1][1]
            return ra, rb

        g1 = restricted(remainder)
        f = near0 * g1
        post(s, g1[1:1 + ox], coarsened((g1 - near1 * f + box(f))[1:1 + ox]))
        begin(make, offsets)
        hook()
        arrive(phase, make, offsets)
        inv, diag = kept[0], kept[1]
        g2 = jnp.where(inv > 0.0, gathered(s, r, far), 0.0)
        e = inv * g2
        for sweep in range(SWEEPS - 1):
            e = e + inv * (g2 - diag * e + box(e))
        second()
        reach = (width + 1) // 2
        nq = qx + 2 * reach
        zero = jnp.zeros_like(e[:1])
        e = jnp.concatenate([e[xs.index(x)][None] if x in xs else zero for x in range(-reach, qx + reach)], 0)
        e = pltpu.roll(e, my - 2, 1)[:, :my // 2].reshape(nq * my // 2, bz)
        u = dot(e, up_c)
        um[pl.ds(0, nq * my // 2, stride=2), :] = u
        um[pl.ds(1, nq * my // 2, stride=2), :] = u
        u = um[:nq * my, :].reshape(nq, my, bz)
        span = width + 1
        mx = ox + 2 * span
        u = jnp.concatenate([u[(m - span) // 2 + reach][None] for m in range(mx)], 0)
        skip1 = RIM - span
        inv, diag = mid[0, skip1:skip1 + mx], mid[1, skip1:skip1 + mx]
        g1 = jnp.where(inv > 0.0, middle(s, r, span), 0.0)
        f = inv * g1 + u
        f = f + inv * (g1 - diag * f + box(f))
        nm = mx - 2
        f = f[1:mx - 1].reshape(nm * my, bz)
        for pf, up in ((pf0, up_a), (pf1, up_b)):
            w = dot(f, up)
            pf[pl.ds(0, nm * my, stride=2), :] = w
            pf[pl.ds(1, nm * my, stride=2), :] = w

        def e1(i):
            m = (i - WIDTH) // 2 + width
            a, b = e0(i)
            return a + pf0[m * ey:(m + 1) * ey, :], b + pf1[m * ey:(m + 1) * ey, :]

        sums1, sums2 = {}, {}
        e2 = {}
        wide = width > 1
        past = INNER + 1 if wide else 1
        for i in range(WIDTH - past, WIDTH + bx + past):
            for k in (i - 1, i, i + 1):
                if k not in sums1:
                    sums1[k] = yz(*e1(k))
            ga, gb = g_at(i)
            ea, eb = e1(i)
            s_ = [sums1[i - 1][t] + sums1[i][t] + sums1[i + 1][t] for t in range(2)]
            za = ea + d0[i] * (ga - (27.0 + gc0[1, i]) * ea + s_[0])
            zb = eb + d1[i] * (gb - (27.0 + t1[1, i]) * eb + s_[1])
            e2[i] = za, zb
            sums2[i] = yz(za, zb)
            k = i - 1
            if k - 1 in sums2:
                around = [sums2[k - 1][t] + sums2[k][t] + sums2[k + 1][t] for t in range(2)]
                za, zb = e2[k]
                finish(k, za, (27.0 + gc0[1, k]) * za - around[0],
                       (27.0 + t1[1, k]) * zb - around[1] if wide else None)

    gamma, delta = [], []

    def own(i):
        return WIDTH <= i < WIDTH + bx

    def finish1(i, e, out, out_b):
        im0[0, i] = out
        im0[1, i] = out_b
        if own(i):
            e, out = e[EDGE:EDGE + by], out[EDGE:EDGE + by]
            pre_ref[i - WIDTH] = e
            img_ref[i - WIDTH] = out
            gamma.append(g_ref[i - WIDTH] * e)
            delta.append(out * e)
        if i == WIDTH + bx - 1:
            gs = jnp.sum(total_of(gamma), axis=0, keepdims=True)
            ds = jnp.sum(total_of(delta), axis=0, keepdims=True)
            gs, ds = gs + pltpu.roll(gs, half, 1), ds + pltpu.roll(ds, half, 1)
            sum_begin(0, jnp.where(lane8[:1] < half, gs, ds))

    nothing = lambda: None
    cycle(3, lambda i: (gc0[0, i], t1[0, i]), near0, near1, s1, r1, make_b, near, ky, RIM - 1, coefficients, nothing, finish1)

    def relay(stage):
        if len(groups) > 1:
            sum_begin(stage, sum_end(stage - 1))

    def finish2(i, e, out, out_b):
        twice_ref[i - WIDTH] = e[EDGE:EDGE + by]
        image_twice_ref[i - WIDTH] = out[EDGE:EDGE + by]

    skip1 = RIM - 1
    cycle(4, lambda i: (im0[0, i], im0[1, i]), mid[0, skip1:skip1 + lx], mid[1, skip1:skip1 + lx], s2, r2, make_d, later, 1, 1,
          lambda: relay(1), lambda: relay(2), finish2)

    total = sum_end(len(groups) - 1)
    gs = jnp.sum(jnp.where(lane8[:1] < half, total, 0.0), axis=1, keepdims=True)
    ds = jnp.sum(jnp.where(lane8[:1] < half, 0.0, total), axis=1, keepdims=True)
    alpha_ref[...] = jnp.broadcast_to(gs / ds, (1, bz)).reshape(alpha_ref.shape)
    leave([(fine_copy, close), (outer_copy, sides), (make_c, near), (make_b, near), (make_d, later)])
    for stage in range(len(groups)):
        some = red_r.at[pl.ds(base[stage], len(mates[stage]))]
        pltpu.make_async_copy(some, some, lssem.at[stage]).wait()


def solution(mesh):
    counts = tuple(mesh.shape[a] for a in AXES)

    def shards(right_side, coefficient):
        bx, by, bz = block = right_side.shape
        assert SPAN <= bx and SPAN * bx <= bz and by == 16 and bx % 4 == 0
        kx = max(1, min(-(-PART // (bx // 4)), counts[0] - 1))
        ky = max(1, min(-(-PART // (by // 4)), counts[1] - 1))
        ex, ey = bx + SPAN, by + 2 * EDGE
        ox, my = bx // 2, ey // 2
        qx = bx // 4
        mx = ox + 2 * RIM
        most = (2 * kx + 1) * (2 * ky + 1) * 3
        planes = len([x for x in range(-PART, qx + PART) if -kx * qx <= x < (kx + 1) * qx])
        mates = [len(partners(counts, group)) for group in stages(counts)]
        f32 = jnp.float32
        vmem = pl.BlockSpec(memory_space=pltpu.VMEM)
        messages = [pltpu.VMEM((6, 8, bz), f32)] * 3
        messages += [pltpu.VMEM((2 * kx + 1, 2 * ky + 1, 3, 6, 8, bz), f32)] * 3
        precond, image, twice, image_twice, alpha, g = pl.pallas_call(
            functools.partial(kernel, counts, block, kx, ky),
            out_shape=[pltpu.VMEM(block, f32)] * 4 + [pltpu.VMEM((1, 1, bz), f32), pltpu.VMEM(block, f32)],
            in_specs=[pl.BlockSpec(memory_space=pltpu.HBM)] * 2,
            out_specs=[vmem] * 6,
            scratch_shapes=[
                pltpu.VMEM(block, f32),
                pltpu.VMEM((2, ex, ey, bz), f32),
                pltpu.VMEM((2, ex, ey, bz), f32),
                pltpu.VMEM((2, by, bz), f32),
                pltpu.VMEM((2, by, bz), f32),
                pltpu.VMEM((2, 2, ey, bz), f32),
                pltpu.VMEM((2, 2, ey, bz), f32),
                pltpu.VMEM((2, ex, ey, bz), f32),
                pltpu.VMEM((ex, ey, bz), f32),
                pltpu.VMEM((ex, ey, bz), f32),
                pltpu.VMEM(((ox + 2) * ey, bz), f32),
                pltpu.VMEM(((ox + 2) * ey, bz), f32),
                pltpu.VMEM(((mx - 2) * ey, bz), f32),
                pltpu.VMEM(((mx - 2) * ey, bz), f32),
                pltpu.VMEM((qx * my, bz), f32),
                pltpu.VMEM(((qx + 4) * my, bz), f32),
                *messages,
                pltpu.VMEM((2, planes, my, bz), f32),
                pltpu.VMEM((2, mx, my, bz), f32),
                pltpu.VMEM((len(mates), 1, bz), f32),
                pltpu.VMEM((sum(mates), 1, bz), f32),
                pltpu.VMEM((16 * most, 8, bz), f32),
                pltpu.SemaphoreType.DMA((2,)),
                pltpu.SemaphoreType.DMA,
                pltpu.SemaphoreType.DMA((5,)),
                pltpu.SemaphoreType.DMA((len(mates),)),
                pltpu.SemaphoreType.DMA((len(mates),)),
            ],
            compiler_params=pltpu.CompilerParams(collective_id=0, has_side_effects=True),
            name="relayed",
        )(right_side, coefficient)
        return (alpha * precond, g - alpha * image,
                precond - alpha * twice, image - alpha * image_twice)

    placed = (P(*AXES), P(*AXES))
    return jax.shard_map(
        shards, mesh=mesh, in_specs=placed, out_specs=(P(*AXES),) * 4, check_vma=False
    )
```

```python
import functools
import itertools

import jax
import jax.numpy as jnp
from jax import lax
from jax.experimental import pallas as pl
from jax.experimental.pallas import tpu as pltpu
from jax.sharding import PartitionSpec as P

SWEEPS = 4
relaxation = 0.6

AXES = ("gx", "gy", "gz")
MESH = pl.DeviceIdType.MESH
WIDTH = 5
INNER = 3
EDGE = 8
SPAN = 2 * WIDTH
RIM = 4
PART = SWEEPS + 1


def dot(a, b):
    high = a.astype(jnp.bfloat16)
    low = (a - high.astype(jnp.float32)).astype(jnp.bfloat16)
    both = jnp.concatenate([high, low], 1)
    b = b.astype(jnp.bfloat16)
    return jnp.dot(both, jnp.concatenate([b, b], 0), preferred_element_type=jnp.float32)


def iota(shape, dim):
    return lax.broadcasted_iota(jnp.int32, shape, dim)


def total_of(values):
    while len(values) > 1:
        values = [a + b for a, b in zip(values[::2], values[1::2])] + values[len(values) & ~1:]
    return values[0]


def stages(counts):
    if max(counts) <= RIM:
        return [(0, 1, 2)]
    return [(2,), (1,), (0,)]


def partners(counts, group):
    steps = [(0, 0, 0)]
    for axis in group:
        steps = [s[:axis] + (k,) + s[axis + 1:] for s in steps for k in range(counts[axis])]
    return [s for s in steps if s != (0, 0, 0)]


def kernel(counts, block, kx, ky, g_hbm, c_hbm, pre_ref, img_ref, twice_ref, image_twice_ref, alpha_ref, g_ref,
           gc0, im0, pk, pkx, zr, zrx, t1, d0, d1, xr0, xr1, pf0, pf1, xm, um,
           s0, s1, s2, r0, r1, r2, kept, mid, red_s, red_r, units, insem, ssem, rsem, lssem, lrsem):
    bx, by, bz = block
    me = [lax.axis_index(a) for a in AXES]
    ex, ey = bx + SPAN, by + 2 * EDGE
    ox, my = bx // 2, ey // 2
    qx, qy = bx // 4, by // 4
    half, quarter = bz // 2, bz // 4
    lane = iota((ey, bz), 1)
    row = iota((ey, bz), 0)
    lane8 = iota((8, bz), 1)
    row8 = iota((8, bz), 0)

    def valid(offset):
        ok = None
        for axis, step in enumerate(offset):
            if step == 0:
                continue
            place = me[axis] + step
            term = place >= 0 if step < 0 else place < counts[axis]
            ok = term if ok is None else jnp.logical_and(ok, term)
        return ok

    def target(offset):
        return tuple(m + s for m, s in zip(me, offset))

    near = [(dx, dy, dz) for dx in range(-kx, kx + 1) for dy in range(-ky, ky + 1) for dz in (-1, 0, 1)]
    near = [o for o in near if o != (0, 0, 0) and all(counts[a] > abs(o[a]) for a in range(3))]
    near.sort(key=lambda o: -sum(map(abs, o)))
    close = [o for o in near if abs(o[0]) <= 1 and abs(o[1]) <= 1]
    sides = [o for o in close if o[0] != 0 and o[2] == 0]
    later = [o for o in near if abs(o[1]) <= 1]

    groups = stages(counts)
    mates = []
    base = [0]
    for group in groups:
        mates.append(partners(counts, group))
        base.append(base[-1] + len(mates[-1]))

    def mate(step):
        return tuple(lax.rem(m + s, n) if s else m for m, s, n in zip(me, step, counts))

    inside0 = gc0.at[:, pl.ds(WIDTH, bx), pl.ds(EDGE, by), :]
    copies = [pltpu.make_async_copy(src, inside0.at[n], insem.at[n]) for n, src in enumerate((g_hbm, c_hbm))]
    for copy in copies:
        copy.start()
    barrier = pltpu.get_barrier_semaphore()
    for offset in near:
        @pl.when(valid(offset))
        def _(offset=offset):
            pl.semaphore_signal(barrier, inc=1, device_id=target(offset), device_id_type=MESH)
    greeted = 0
    if len(groups) > 1:
        for steps in mates:
            for step in steps:
                pl.semaphore_signal(barrier, inc=1, device_id=mate(step), device_id_type=MESH)
            greeted = greeted + len(steps)

    def options(axis, far):
        total = 1
        for step in range(1, far + 1):
            if counts[axis] > step:
                total = total + (me[axis] >= step).astype(jnp.int32)
                total = total + (me[axis] + step < counts[axis]).astype(jnp.int32)
        return total

    greeted = greeted + options(0, kx) * options(1, ky) * options(2, 1) - 1

    def clear(ref):
        ref[...] = jnp.zeros(ref.shape, jnp.float32)

    for axis, edges in enumerate((
            [[gc0.at[:, pl.ds(0, WIDTH)], zrx.at[:, 0]], [gc0.at[:, pl.ds(WIDTH + bx, WIDTH)], zrx.at[:, 1]]],
            [[ref.at[..., pl.ds(at, EDGE), :] for ref in (gc0, zr, zrx)] for at in (0, EDGE + by)],
            [[ref.at[side] for ref in (zr, zrx)] for side in range(2)])):
        for refs, edge in zip(edges, (0, counts[axis] - 1)):
            @pl.when(me[axis] == edge)
            def _(refs=refs):
                for ref in refs:
                    clear(ref)

    def row_ends(dy):
        if dy == 0:
            return 0, by, EDGE
        if dy > 0:
            return by - EDGE, EDGE, 0
        return 0, EDGE, EDGE + by

    def remote(src, dst, phase, offset):
        pltpu.make_async_remote_copy(
            src_ref=src, dst_ref=dst, send_sem=ssem, recv_sem=rsem.at[phase],
            device_id=target(offset), device_id_type=MESH).start()

    def planes_copy(phase, offset, first, size):
        dx, dy, dz = offset
        start, rows, goes = row_ends(dy)
        if dx == 0:
            px, tx, size = WIDTH, WIDTH, bx
        elif dx > 0:
            px, tx = WIDTH + bx - first - size, WIDTH - first - size
        else:
            px, tx = WIDTH + first, WIDTH + bx + first
        src = gc0.at[:, pl.ds(px, size), pl.ds(EDGE + start, rows), :]
        dst = gc0.at[:, pl.ds(tx, size), pl.ds(goes, rows), :]
        return (src, dst, phase, offset)

    def fine_copy(offset):
        dx, dy, dz = offset
        if dz == 0:
            return planes_copy(0, offset, 0, INNER)
        start, rows, goes = row_ends(dy)
        side = 0 if dz > 0 else 1
        if dx == 0:
            src = pk.at[:, pl.ds(start, rows), :]
            dst = zr.at[side, :, pl.ds(goes, rows), :]
        else:
            end = 0 if dx > 0 else 1
            src = pkx.at[end, pl.ds(start, rows), :]
            dst = zrx.at[side, end, pl.ds(goes, rows), :]
        return (src, dst, 0, offset)

    def outer_copy(offset):
        return planes_copy(1, offset, INNER, WIDTH - INNER)

    def part(offset, depth):
        dx, dy, dz = offset
        if abs(dx) > 1 or abs(dy) > 1:
            return 0, 1
        if dz != 0:
            return 4, 1
        if dx == 0:
            return 0, 4
        if dx < 0:
            return 0, 1 + depth
        return 4 - depth, 1 + depth

    def coarse_copy(phase, offset, s, r, depth):
        dx, dy, dz = offset
        at, size = part(offset, depth)
        return (s.at[pl.ds(at, size)], r.at[kx - dx, ky - dy, 1 - dz, pl.ds(at, size)], phase, offset)

    def tiles(make, offset):
        size = 1
        for n in make(offset)[0].shape:
            size *= n
        assert size % (8 * bz) == 0
        return size // (8 * bz)

    def begin(make, offsets):
        for offset in offsets:
            @pl.when(valid(offset))
            def _(offset=offset):
                remote(*make(offset))

    def wait_for(sem, pairs):
        sizes = {}
        for make, offsets in pairs:
            for offset in offsets:
                key = tuple(map(abs, offset))
                sizes.setdefault(key, 0)
                if offset == key:
                    sizes[key] += tiles(make, offset)

        def amount(options):
            total = 0
            for (a, b, c), size in sizes.items():
                total = total + size * options[0][a] * options[1][b] * options[2][c]
            return total

        def number(place, count, step):
            return 1 if step == 0 else (place >= step) * 1 + (place + step < count) * 1

        def table(axis, place):
            return [number(place, counts[axis], k) for k in range(3)]

        here = []
        for axis in range(3):
            has = [1]
            for k in (1, 2):
                n = (me[axis] >= k).astype(jnp.int32) + (me[axis] + k < counts[axis]).astype(jnp.int32)
                has.append(n)
            here.append(has)
        total = amount(here)
        for value in sorted({amount(options) for options in itertools.product(
                *[[table(axis, place) for place in range(counts[axis])] for axis in range(3)])}):
            @pl.when(total == value)
            def _(value=value):
                some = units.at[pl.ds(0, value)]
                pltpu.make_async_copy(some, some, sem).wait()

    def arrive(phase, make, offsets):
        wait_for(rsem.at[phase], [(make, offsets)])

    def leave(pairs):
        wait_for(ssem, pairs)

    def mate_copy(stage, k):
        n = base[stage] + k
        return pltpu.make_async_remote_copy(
            src_ref=red_s.at[stage], dst_ref=red_r.at[n], send_sem=lssem.at[stage],
            recv_sem=lrsem.at[stage], device_id=mate(mates[stage][k]), device_id_type=MESH)

    def sum_begin(stage, value):
        red_s[stage] = value
        for k in range(len(mates[stage])):
            mate_copy(stage, k).start()

    def sum_end(stage):
        some = red_r.at[pl.ds(base[stage], len(mates[stage]))]
        pltpu.make_async_copy(some, some, lrsem.at[stage]).wait()
        return total_of([red_s[stage]] + [red_r[base[stage] + k] for k in range(len(mates[stage]))])

    strip = (lane[:by] < WIDTH) | (lane[:by] >= bz - WIDTH)
    place = lax.rem(lane + WIDTH, bz)
    low = lax.rem(place, SPAN) < WIDTH
    band = (lane < WIDTH) | (lane >= bz - WIDTH)
    first, last = lane == 0, lane == bz - 1

    def turn_to(v, shift):
        shift = shift % bz
        return v if shift == 0 else pltpu.roll(v, shift, 1)

    def pack(planes):
        pieces = [turn_to(jnp.where(strip, plane, 0.0), SPAN * i) for i, plane in enumerate(planes)]
        ends = (total_of(pieces[bx - WIDTH:]), total_of(pieces[:WIDTH]))
        return ends, total_of(pieces[WIDTH:bx - WIDTH] + list(ends))

    def yz(a, b):
        sa = a + jnp.where(first, pltpu.roll(b, 1, 1), pltpu.roll(a, 1, 1))
        sb = b + jnp.where(first, pltpu.roll(a, 1, 1), pltpu.roll(b, 1, 1))
        sa = sa + jnp.where(last, pltpu.roll(b, bz - 1, 1), pltpu.roll(a, bz - 1, 1))
        sb = sb + jnp.where(last, pltpu.roll(a, bz - 1, 1), pltpu.roll(b, bz - 1, 1))
        sa = sa + pltpu.roll(sa, 1, 0) + pltpu.roll(sa, ey - 1, 0)
        sb = sb + pltpu.roll(sb, 1, 0) + pltpu.roll(sb, ey - 1, 0)
        return sa, sb

    def box(v):
        s = v + pltpu.roll(v, 1, 2) + pltpu.roll(v, v.shape[2] - 1, 2)
        s = s + pltpu.roll(s, 1, 1) + pltpu.roll(s, v.shape[1] - 1, 1)
        zero = jnp.zeros_like(s[:1])
        return s + jnp.concatenate([zero, s[:-1]], 0) + jnp.concatenate([s[1:], zero], 0)

    p_, q_ = iota((bz, bz), 0), iota((bz, bz), 1)
    down_a = jnp.where((p_ >> 1) == q_, 0.5, 0.0)
    down_b = jnp.where(((p_ + bz) >> 1) == q_, 0.5, 0.0)
    up_a = jnp.where((q_ >> 1) == p_, 1.0, 0.0)
    up_b = jnp.where(((q_ + bz) >> 1) == p_, 1.0, 0.0)
    down_c = jnp.where((p_ < half) & ((p_ >> 1) == lax.rem(q_, quarter)), 0.5, 0.0)
    up_c = jnp.where(p_ == jnp.where(q_ < 3 * quarter, q_ >> 1, (q_ >> 1) + half), 1.0, 0.0)

    lx = ox + 2

    def restricted(of):
        for m in range(lx):
            a0, b0 = of(2 * m + INNER)
            a1, b1 = of(2 * m + INNER + 1)
            xr0[m * ey:(m + 1) * ey, :] = a0 + a1
            xr1[m * ey:(m + 1) * ey, :] = b0 + b1
        n = lx * my
        a = xr0[pl.ds(0, n, stride=2), :] + xr0[pl.ds(1, n, stride=2), :]
        b = xr1[pl.ds(0, n, stride=2), :] + xr1[pl.ds(1, n, stride=2), :]
        return (dot(a, down_a) + dot(b, down_b)).reshape(lx, my, bz)

    turn = lane8 // quarter

    def coarsened(v):
        for m in range(qx):
            xm[m * my:(m + 1) * my, :] = v[2 * m] + v[2 * m + 1]
        n = qx * my // 2
        a = xm[pl.ds(0, n, stride=2), :] + xm[pl.ds(1, n, stride=2), :]
        a = dot(a, down_c)
        rows = my // 2
        tile = a[:rows]
        for m in range(1, qx):
            tile = jnp.where(turn == m, a[m * rows:(m + 1) * rows], tile)
        return pltpu.roll(tile, rows - 2, 0)

    rim = (lane8 < RIM) | ((lane8 >= half - RIM) & (lane8 < half))
    edge1 = my // 2 - by // 4
    here_ends = (lane8 < RIM * ox) | ((lane8 >= half - RIM) & (lane8 < half - RIM + RIM * ox))

    def post(s, v1, tile):
        own = [v1[p][edge1:edge1 + by // 2] for p in range(ox)]
        ends = total_of([turn_to(jnp.where(rim, own[p], 0.0), RIM * p) for p in range(ox)])
        ends = jnp.where(here_ends, ends, pltpu.roll(turn_to(ends, RIM * ox), 4, 0))
        tile = jnp.where(row8 < qy, tile, ends)
        s[0] = tile
        for k in range(ox // 2):
            s[1 + k] = jnp.where(lane8 < half, own[2 * k], pltpu.roll(own[2 * k + 1], half, 1))
        s[4] = tile

    def middle(s, r, width):
        depth = RIM // 2 if width > 2 else 1

        def get(dx, dy, dz, k):
            if (dx, dy, dz) == (0, 0, 0):
                return s[k]
            if any(abs(d) >= n for d, n in zip((dx, dy, dz), counts)):
                return jnp.zeros((8, bz), jnp.float32)
            return r[kx + dx, ky + dy, 1 + dz, k]

        def rows(tiles):
            before, here, after = tiles
            return (pltpu.roll(jnp.where(row8 >= 4, before, here), 4, 0),
                    pltpu.roll(jnp.where(row8 >= 4, here, after), 4, 0))

        planes = []
        for dx in (-1, 0, 1):
            tiles = range(ox // 2 - depth, ox // 2) if dx < 0 else range(depth) if dx > 0 else range(ox // 2)
            ends = [jnp.where(lane8 < 2 * RIM * ox + RIM, get(dx, dy, 1, 4), get(dx, dy, -1, 4)) for dy in (-1, 0, 1)]
            ends = [jnp.where(row8 < 4, pltpu.roll(ends[k], 4, 0), turn_to(ends[k + 1], -RIM * ox)) for k in range(2)]
            for k in tiles:
                pair = rows([get(dx, dy, 0, 1 + k) for dy in (-1, 0, 1)])
                for odd in (0, 1):
                    p = 2 * k + odd
                    planes.append(jnp.concatenate([
                        jnp.where(lane8 < half, pltpu.roll(t, half, 1) if odd else t, turn_to(e, half - RIM * p))
                        for t, e in zip(pair, ends)], 0))
        return jnp.stack(planes)

    xs = [x for x in range(-PART, qx + PART) if -kx * qx <= x < (kx + 1) * qx]

    def gathered(s, r, far):
        zero = jnp.zeros((8, bz), jnp.float32)

        def get(dx, dy, dz):
            if (dx, dy, dz) == (0, 0, 0):
                return s[0]
            if any(abs(d) >= n for d, n in zip((dx, dy, dz), counts)) or abs(dy) > far:
                return zero
            return r[kx + dx, ky + dy, 1 + dz, part((-dx, -dy, -dz), 0)[0]]

        columns = {}
        for dx in sorted({x // qx for x in xs}):
            for dy in range(-2, 3):
                if abs(dy) > far:
                    continue
                here = get(dx, dy, 0)
                after = pltpu.roll(get(dx, dy, 1), quarter, 1)
                before = pltpu.roll(get(dx, dy, -1), 3 * quarter, 1)
                for m in range(qx):
                    tile = jnp.where(turn == (m + 1) % 4, after, here)
                    tile = jnp.where(turn == (m + 3) % 4, before, tile)
                    columns[dx * qx + m, dy] = turn_to(tile, -quarter * m)
        planes = []
        for x in xs:
            t = {dy: columns.get((x, dy), zero) for dy in range(-2, 3)}
            upper = jnp.where(row8 < qy, t[-1], pltpu.roll(t[0], 4, 0))
            if far > 1:
                lower = jnp.where(row8 < qy, t[1], pltpu.roll(jnp.where(row8 < 2, t[2], t[-2]), 4, 0))
            else:
                lower = jnp.where(row8 < qy, t[1], 0.0)
            planes.append(jnp.concatenate([upper, lower], 0))
        return jnp.stack(planes)

    def within(place, axis, size):
        place = place + me[axis] * size
        return (place >= 0) & (place < counts[axis] * size)

    for copy in copies:
        copy.wait()
    g, c = ([gc0[n, WIDTH + i, EDGE:EDGE + by, :] for i in range(bx)] for n in range(2))
    for i in range(bx):
        g_ref[i] = g[i]
    (g_last, g_first), pk[0] = pack(g)
    (c_last, c_first), pk[1] = pack(c)
    pkx[0] = g_last + turn_to(c_last, -SPAN * WIDTH)
    pkx[1] = g_first + turn_to(c_first, SPAN * WIDTH)

    for m in range(ox):
        xr0[m * ey + EDGE:m * ey + EDGE + by, :] = c[2 * m] + c[2 * m + 1]
    n = ox * my
    own1 = xr0[pl.ds(0, n, stride=2), :] + xr0[pl.ds(1, n, stride=2), :]
    own1 = dot(own1, down_a).reshape(ox, my, bz)
    post(s0, own1, coarsened(own1))

    def relay_copy(offset):
        dx, dy, dz = offset
        if (dy, dz) == (0, 0):
            return coarse_copy(2, offset, s0, r0, RIM // 2)
        far = abs(dx) > 1 or abs(dy) > 1
        at, size = part((-dx, 0, 0), RIM // 2)
        if far or dz != 0:
            at, size = 4 if dx == -1 else 0, 1
        src = s0.at[pl.ds(at, size)] if dx == 0 else r0.at[kx + dx, ky, 1, pl.ds(at, size)]
        goes = 0 if far else 4 if dz != 0 else at
        return src, r0.at[kx + dx, ky - dy, 1 - dz, pl.ds(goes, size)], 5, (0, dy, dz)

    along_x = [o for o in near if o[1] == o[2] == 0]
    onwards = [o for o in near if o not in along_x]
    make_b = lambda o: coarse_copy(3, o, s1, r1, RIM // 2)
    make_d = lambda o: coarse_copy(4, o, s2, r2, 1)
    pl.semaphore_wait(barrier, greeted)
    begin(relay_copy, along_x)
    begin(fine_copy, close)

    in_y = within(row - EDGE, 1, by)
    in_z = band & within(jnp.where(lane < half, lane + bz, lane - bz), 2, bz)

    def spread(i):
        for f in range(2):
            if i < WIDTH:
                k = i
                piece = turn_to(ends[0], -SPAN * (bx - WIDTH + k - WIDTH * f))
            elif i >= WIDTH + bx:
                k = i - WIDTH - bx
                piece = turn_to(ends[1], -SPAN * (k + WIDTH * f))
            else:
                piece = turn_to(merged[f], -SPAN * (i - WIDTH))
            t1[f, i] = jnp.where(band, piece, 0.0)
        in_x = within(jnp.full((ey, bz), i - WIDTH, jnp.int32), 0, bx)
        d0[i] = jnp.where(in_y & in_x, relaxation / (26.0 + gc0[1, i]), 0.0)
        d1[i] = jnp.where(in_y & in_x & in_z, relaxation / (26.0 + t1[1, i]), 0.0)

    arrive(2, relay_copy, along_x)
    begin(relay_copy, onwards)
    begin(outer_copy, sides)
    arrive(0, fine_copy, close)
    merged = [jnp.where(low, zr[0, f], zr[1, f]) for f in range(2)]
    ends = [jnp.where(low, zrx[0, e], zrx[1, e]) for e in range(2)]
    skip = WIDTH - INNER
    for i in range(skip, ex - skip):
        spread(i)

    def inside1(shape, width):
        zl = iota(shape, 2)
        zl = jnp.where(zl < 3 * quarter, zl, zl - bz)
        ok = within(iota(shape, 0) - width, 0, ox) & within(iota(shape, 1) - edge1, 1, by // 2)
        return ok & within(zl, 2, half) & (zl >= -RIM) & (zl < half + RIM)

    c1 = restricted(lambda i: (gc0[1, i], t1[1, i]))
    near0 = jnp.where(inside1((lx, my, bz), 1), relaxation / (26.0 + c1), 0.0)
    near1 = 27.0 + c1

    def coefficients():
        arrive(1, outer_copy, sides)
        for i in list(range(skip)) + list(range(ex - skip, ex)):
            spread(i)
        arrive(5, relay_copy, onwards)
        c1 = middle(s0, r0, RIM)
        ok = inside1(c1.shape, RIM)
        c1 = jnp.where(ok, c1, 0.0)
        mid[0] = jnp.where(ok, relaxation / (26.0 + c1), 0.0)
        mid[1] = 27.0 + c1
        c2 = gathered(s0, r0, ky)
        shape = c2.shape
        z = iota(shape, 2)
        z = jnp.where(z < 2 * quarter, z, z - bz)
        y = iota(shape, 1)
        y = jnp.where(y < my - 2, y, y - my) - qy
        ok = within(iota(shape, 0) + xs[0], 0, qx) & within(y, 1, qy)
        ok = ok & within(z, 2, quarter) & (z >= -quarter)
        c2 = jnp.where(ok, c2, 0.0)
        kept[0] = jnp.where(ok, relaxation / (26.0 + c2), 0.0)
        kept[1] = 27.0 + c2

    def cycle(phase, g_at, near0, near1, s, r, make, offsets, far, width, hook, second, finish):
        def e0(i):
            a, b = g_at(i)
            return d0[i] * a, d1[i] * b

        sums = {}

        def remainder(i):
            for k in (i - 1, i, i + 1):
                if k not in sums:
                    sums[k] = yz(*e0(k))
            a, b = g_at(i)
            ea, eb = e0(i)
            ra = a - (27.0 + gc0[1, i]) * ea + sums[i - 1][0] + sums[i][0] + sums[i + 1][0]
            rb = b - (27.0 + t1[1, i]) * eb + sums[i - 1][1] + sums[i][1] + sums[i + 1][1]
            return ra, rb

        g1 = restricted(remainder)
        f = near0 * g1
        post(s, g1[1:1 + ox], coarsened((g1 - near1 * f + box(f))[1:1 + ox]))
        begin(make, offsets)
        hook()
        arrive(phase, make, offsets)
        inv, diag = kept[0], kept[1]
        g2 = jnp.where(inv > 0.0, gathered(s, r, far), 0.0)
        e = inv * g2
        for sweep in range(SWEEPS - 1):
            e = e + inv * (g2 - diag * e + box(e))
        second()
        reach = (width + 1) // 2
        nq = qx + 2 * reach
        zero = jnp.zeros_like(e[:1])
        e = jnp.concatenate([e[xs.index(x)][None] if x in xs else zero for x in range(-reach, qx + reach)], 0)
        e = pltpu.roll(e, my - 2, 1)[:, :my // 2].reshape(nq * my // 2, bz)
        u = dot(e, up_c)
        um[pl.ds(0, nq * my // 2, stride=2), :] = u
        um[pl.ds(1, nq * my // 2, stride=2), :] = u
        u = um[:nq * my, :].reshape(nq, my, bz)
        span = width + 1
        mx = ox + 2 * span
        u = jnp.concatenate([u[(m - span) // 2 + reach][None] for m in range(mx)], 0)
        skip1 = RIM - span
        inv, diag = mid[0, skip1:skip1 + mx], mid[1, skip1:skip1 + mx]
        g1 = jnp.where(inv > 0.0, middle(s, r, span), 0.0)
        f = inv * g1 + u
        f = f + inv * (g1 - diag * f + box(f))
        nm = mx - 2
        f = f[1:mx - 1].reshape(nm * my, bz)
        for pf, up in ((pf0, up_a), (pf1, up_b)):
            w = dot(f, up)
            pf[pl.ds(0, nm * my, stride=2), :] = w
            pf[pl.ds(1, nm * my, stride=2), :] = w

        def e1(i):
            m = (i - WIDTH) // 2 + width
            a, b = e0(i)
            return a + pf0[m * ey:(m + 1) * ey, :], b + pf1[m * ey:(m + 1) * ey, :]

        sums1, sums2 = {}, {}
        e2 = {}
        wide = width > 1
        past = INNER + 1 if wide else 1
        for i in range(WIDTH - past, WIDTH + bx + past):
            for k in (i - 1, i, i + 1):
                if k not in sums1:
                    sums1[k] = yz(*e1(k))
            ga, gb = g_at(i)
            ea, eb = e1(i)
            s_ = [sums1[i - 1][t] + sums1[i][t] + sums1[i + 1][t] for t in range(2)]
            za = ea + d0[i] * (ga - (27.0 + gc0[1, i]) * ea + s_[0])
            zb = eb + d1[i] * (gb - (27.0 + t1[1, i]) * eb + s_[1])
            e2[i] = za, zb
            sums2[i] = yz(za, zb)
            k = i - 1
            if k - 1 in sums2:
                around = [sums2[k - 1][t] + sums2[k][t] + sums2[k + 1][t] for t in range(2)]
                za, zb = e2[k]
                finish(k, za, (27.0 + gc0[1, k]) * za - around[0],
                       (27.0 + t1[1, k]) * zb - around[1] if wide else None)

    gamma, delta = [], []

    def own(i):
        return WIDTH <= i < WIDTH + bx

    def finish1(i, e, out, out_b):
        im0[0, i] = out
        im0[1, i] = out_b
        if own(i):
            e, out = e[EDGE:EDGE + by], out[EDGE:EDGE + by]
            pre_ref[i - WIDTH] = e
            img_ref[i - WIDTH] = out
            gamma.append(g_ref[i - WIDTH] * e)
            delta.append(out * e)
        if i == WIDTH + bx - 1:
            gs = jnp.sum(total_of(gamma), axis=0, keepdims=True)
            ds = jnp.sum(total_of(delta), axis=0, keepdims=True)
            gs, ds = gs + pltpu.roll(gs, half, 1), ds + pltpu.roll(ds, half, 1)
            sum_begin(0, jnp.where(lane8[:1] < half, gs, ds))

    nothing = lambda: None
    cycle(3, lambda i: (gc0[0, i], t1[0, i]), near0, near1, s1, r1, make_b, near, ky, RIM - 1, coefficients, nothing, finish1)

    def relay(stage):
        if len(groups) > 1:
            sum_begin(stage, sum_end(stage - 1))

    def finish2(i, e, out, out_b):
        twice_ref[i - WIDTH] = e[EDGE:EDGE + by]
        image_twice_ref[i - WIDTH] = out[EDGE:EDGE + by]

    skip1 = RIM - 1
    cycle(4, lambda i: (im0[0, i], im0[1, i]), mid[0, skip1:skip1 + lx], mid[1, skip1:skip1 + lx], s2, r2, make_d, later, 1, 1,
          lambda: relay(1), lambda: relay(2), finish2)

    total = sum_end(len(groups) - 1)
    gs = jnp.sum(jnp.where(lane8[:1] < half, total, 0.0), axis=1, keepdims=True)
    ds = jnp.sum(jnp.where(lane8[:1] < half, 0.0, total), axis=1, keepdims=True)
    alpha_ref[...] = jnp.broadcast_to(gs / ds, (1, bz)).reshape(alpha_ref.shape)
    leave([(fine_copy, close), (outer_copy, sides), (relay_copy, near), (make_b, near), (make_d, later)])
    for stage in range(len(groups)):
        some = red_r.at[pl.ds(base[stage], len(mates[stage]))]
        pltpu.make_async_copy(some, some, lssem.at[stage]).wait()


def solution(mesh):
    counts = tuple(mesh.shape[a] for a in AXES)

    def shards(right_side, coefficient):
        bx, by, bz = block = right_side.shape
        assert SPAN <= bx and SPAN * bx <= bz and by == 16 and bx % 4 == 0
        kx = max(1, min(-(-PART // (bx // 4)), counts[0] - 1))
        ky = max(1, min(-(-PART // (by // 4)), counts[1] - 1))
        ex, ey = bx + SPAN, by + 2 * EDGE
        ox, my = bx // 2, ey // 2
        qx = bx // 4
        mx = ox + 2 * RIM
        most = (2 * kx + 1) * (2 * ky + 1) * 3
        planes = len([x for x in range(-PART, qx + PART) if -kx * qx <= x < (kx + 1) * qx])
        mates = [len(partners(counts, group)) for group in stages(counts)]
        f32 = jnp.float32
        vmem = pl.BlockSpec(memory_space=pltpu.VMEM)
        messages = [pltpu.VMEM((5, 8, bz), f32)] * 3
        messages += [pltpu.VMEM((2 * kx + 1, 2 * ky + 1, 3, 5, 8, bz), f32)] * 3
        precond, image, twice, image_twice, alpha, g = pl.pallas_call(
            functools.partial(kernel, counts, block, kx, ky),
            out_shape=[pltpu.VMEM(block, f32)] * 4 + [pltpu.VMEM((1, 1, bz), f32), pltpu.VMEM(block, f32)],
            in_specs=[pl.BlockSpec(memory_space=pltpu.HBM)] * 2,
            out_specs=[vmem] * 6,
            scratch_shapes=[
                pltpu.VMEM((2, ex, ey, bz), f32),
                pltpu.VMEM((2, ex, ey, bz), f32),
                pltpu.VMEM((2, by, bz), f32),
                pltpu.VMEM((2, by, bz), f32),
                pltpu.VMEM((2, 2, ey, bz), f32),
                pltpu.VMEM((2, 2, ey, bz), f32),
                pltpu.VMEM((2, ex, ey, bz), f32),
                pltpu.VMEM((ex, ey, bz), f32),
                pltpu.VMEM((ex, ey, bz), f32),
                pltpu.VMEM(((ox + 2) * ey, bz), f32),
                pltpu.VMEM(((ox + 2) * ey, bz), f32),
                pltpu.VMEM(((mx - 2) * ey, bz), f32),
                pltpu.VMEM(((mx - 2) * ey, bz), f32),
                pltpu.VMEM((qx * my, bz), f32),
                pltpu.VMEM(((qx + 4) * my, bz), f32),
                *messages,
                pltpu.VMEM((2, planes, my, bz), f32),
                pltpu.VMEM((2, mx, my, bz), f32),
                pltpu.VMEM((len(mates), 1, bz), f32),
                pltpu.VMEM((sum(mates), 1, bz), f32),
                pltpu.VMEM((16 * most, 8, bz), f32),
                pltpu.SemaphoreType.DMA((2,)),
                pltpu.SemaphoreType.DMA,
                pltpu.SemaphoreType.DMA((6,)),
                pltpu.SemaphoreType.DMA((len(mates),)),
                pltpu.SemaphoreType.DMA((len(mates),)),
            ],
            compiler_params=pltpu.CompilerParams(collective_id=0, has_side_effects=True),
            name="relayed",
        )(right_side, coefficient)
        return (alpha * precond, g - alpha * image,
                precond - alpha * twice, image - alpha * image_twice)

    placed = (P(*AXES), P(*AXES))
    return jax.shard_map(
        shards, mesh=mesh, in_specs=placed, out_specs=(P(*AXES),) * 4, check_vma=False
    )
```

```python
import functools
import itertools

import jax
import jax.numpy as jnp
from jax import lax
from jax.experimental import pallas as pl
from jax.experimental.pallas import tpu as pltpu
from jax.sharding import PartitionSpec as P

SWEEPS = 4
relaxation = 0.6

AXES = ("gx", "gy", "gz")
MESH = pl.DeviceIdType.MESH
WIDTH = 5
INNER = 3
EDGE = 8
SPAN = 2 * WIDTH
RIM = 4
PART = SWEEPS + 1


def pick(values, lanes):
    flat = values.reshape(-1, values.shape[-1])
    lanes = jnp.broadcast_to(lanes[:1], flat.shape)
    return jnp.take_along_axis(flat, lanes, axis=1).reshape(values.shape)


def iota(shape, dim):
    return lax.broadcasted_iota(jnp.int32, shape, dim)


def total_of(values):
    while len(values) > 1:
        values = [a + b for a, b in zip(values[::2], values[1::2])] + values[len(values) & ~1:]
    return values[0]


def stages(counts):
    if max(counts) <= RIM:
        return [(0, 1, 2)]
    return [(2,), (1,), (0,)]


def partners(counts, group):
    steps = [(0, 0, 0)]
    for axis in group:
        steps = [s[:axis] + (k,) + s[axis + 1:] for s in steps for k in range(counts[axis])]
    return [s for s in steps if s != (0, 0, 0)]


def kernel(counts, block, kx, ky, g_hbm, c_hbm, pre_ref, img_ref, twice_ref, image_twice_ref, alpha_ref, g_ref,
           gc0, im0, pk, pkx, zr, zrx, t1, d, k27, w27, ys, xr0, xr1, pf0, pf1, xm, um,
           s0, s1, s2, r0, r1, r2, kept, mid, red_s, red_r, units, insem, ssem, rsem, lssem, lrsem):
    bx, by, bz = block
    me = [lax.axis_index(a) for a in AXES]
    ex, ey = bx + SPAN, by + 2 * EDGE
    ox, my = bx // 2, ey // 2
    qx, qy = bx // 4, by // 4
    half, quarter = bz // 2, bz // 4
    lane = iota((ey, bz), 1)
    row = iota((ey, bz), 0)
    lane8 = iota((8, bz), 1)
    row8 = iota((8, bz), 0)

    def valid(offset):
        ok = None
        for axis, step in enumerate(offset):
            if step == 0:
                continue
            place = me[axis] + step
            term = place >= 0 if step < 0 else place < counts[axis]
            ok = term if ok is None else jnp.logical_and(ok, term)
        return ok

    def target(offset):
        return tuple(m + s for m, s in zip(me, offset))

    near = [(dx, dy, dz) for dx in range(-kx, kx + 1) for dy in range(-ky, ky + 1) for dz in (-1, 0, 1)]
    near = [o for o in near if o != (0, 0, 0) and all(counts[a] > abs(o[a]) for a in range(3))]
    near.sort(key=lambda o: -sum(map(abs, o)))
    close = [o for o in near if abs(o[0]) <= 1 and abs(o[1]) <= 1]
    sides = [o for o in close if o[0] != 0 and o[2] == 0]
    later = [o for o in near if abs(o[1]) <= 1]

    groups = stages(counts)
    mates = []
    base = [0]
    for group in groups:
        mates.append(partners(counts, group))
        base.append(base[-1] + len(mates[-1]))

    def mate(step):
        return tuple(lax.rem(m + s, n) if s else m for m, s, n in zip(me, step, counts))

    inside0 = gc0.at[:, pl.ds(WIDTH, bx), pl.ds(EDGE, by), :]
    copies = [pltpu.make_async_copy(src, inside0.at[n], insem.at[n]) for n, src in enumerate((g_hbm, c_hbm))]
    for copy in copies:
        copy.start()
    barrier = pltpu.get_barrier_semaphore()
    for offset in near:
        @pl.when(valid(offset))
        def _(offset=offset):
            pl.semaphore_signal(barrier, inc=1, device_id=target(offset), device_id_type=MESH)
    greeted = 0
    if len(groups) > 1:
        for steps in mates:
            for step in steps:
                pl.semaphore_signal(barrier, inc=1, device_id=mate(step), device_id_type=MESH)
            greeted = greeted + len(steps)

    def options(axis, far):
        total = 1
        for step in range(1, far + 1):
            if counts[axis] > step:
                total = total + (me[axis] >= step).astype(jnp.int32)
                total = total + (me[axis] + step < counts[axis]).astype(jnp.int32)
        return total

    greeted = greeted + options(0, kx) * options(1, ky) * options(2, 1) - 1

    def clear(ref):
        ref[...] = jnp.zeros(ref.shape, jnp.float32)

    for axis, edges in enumerate((
            [[gc0.at[:, pl.ds(0, WIDTH)], zrx.at[:, 0]], [gc0.at[:, pl.ds(WIDTH + bx, WIDTH)], zrx.at[:, 1]]],
            [[ref.at[..., pl.ds(at, EDGE), :] for ref in (gc0, zr, zrx)] for at in (0, EDGE + by)],
            [[ref.at[side] for ref in (zr, zrx)] for side in range(2)])):
        for refs, edge in zip(edges, (0, counts[axis] - 1)):
            @pl.when(me[axis] == edge)
            def _(refs=refs):
                for ref in refs:
                    clear(ref)

    for at in (0, EDGE + ey):
        ys[:, :, at:at + EDGE, :] = jnp.zeros((2, ex, EDGE, bz), jnp.float32)

    def row_ends(dy):
        if dy == 0:
            return 0, by, EDGE
        if dy > 0:
            return by - EDGE, EDGE, 0
        return 0, EDGE, EDGE + by

    def remote(src, dst, phase, offset):
        pltpu.make_async_remote_copy(
            src_ref=src, dst_ref=dst, send_sem=ssem, recv_sem=rsem.at[phase],
            device_id=target(offset), device_id_type=MESH).start()

    def planes_copy(phase, offset, first, size):
        dx, dy, dz = offset
        start, rows, goes = row_ends(dy)
        if dx == 0:
            px, tx, size = WIDTH, WIDTH, bx
        elif dx > 0:
            px, tx = WIDTH + bx - first - size, WIDTH - first - size
        else:
            px, tx = WIDTH + first, WIDTH + bx + first
        src = gc0.at[:, pl.ds(px, size), pl.ds(EDGE + start, rows), :]
        dst = gc0.at[:, pl.ds(tx, size), pl.ds(goes, rows), :]
        return (src, dst, phase, offset)

    def fine_copy(offset):
        dx, dy, dz = offset
        if dz == 0:
            return planes_copy(0, offset, 0, INNER)
        start, rows, goes = row_ends(dy)
        side = 0 if dz > 0 else 1
        if dx == 0:
            src = pk.at[:, pl.ds(start, rows), :]
            dst = zr.at[side, :, pl.ds(goes, rows), :]
        else:
            end = 0 if dx > 0 else 1
            src = pkx.at[end, pl.ds(start, rows), :]
            dst = zrx.at[side, end, pl.ds(goes, rows), :]
        return (src, dst, 0, offset)

    def outer_copy(offset):
        return planes_copy(1, offset, INNER, WIDTH - INNER)

    def part(offset, depth):
        dx, dy, dz = offset
        if abs(dx) > 1 or abs(dy) > 1:
            return 0, 1
        if dz != 0:
            return 4, 1
        if dx == 0:
            return 0, 4
        if dx < 0:
            return 0, 1 + depth
        return 4 - depth, 1 + depth

    def coarse_copy(phase, offset, s, r, depth):
        dx, dy, dz = offset
        at, size = part(offset, depth)
        return (s.at[pl.ds(at, size)], r.at[kx - dx, ky - dy, 1 - dz, pl.ds(at, size)], phase, offset)

    def tiles(make, offset):
        size = 1
        for n in make(offset)[0].shape:
            size *= n
        assert size % (8 * bz) == 0
        return size // (8 * bz)

    def begin(make, offsets):
        for offset in offsets:
            @pl.when(valid(offset))
            def _(offset=offset):
                remote(*make(offset))

    def wait_for(sem, pairs):
        sizes = {}
        for make, offsets in pairs:
            for offset in offsets:
                key = tuple(map(abs, offset))
                sizes.setdefault(key, 0)
                if offset == key:
                    sizes[key] += tiles(make, offset)

        def amount(options):
            total = 0
            for (a, b, c), size in sizes.items():
                total = total + size * options[0][a] * options[1][b] * options[2][c]
            return total

        def number(place, count, step):
            return 1 if step == 0 else (place >= step) * 1 + (place + step < count) * 1

        def table(axis, place):
            return [number(place, counts[axis], k) for k in range(3)]

        here = []
        for axis in range(3):
            has = [1]
            for k in (1, 2):
                n = (me[axis] >= k).astype(jnp.int32) + (me[axis] + k < counts[axis]).astype(jnp.int32)
                has.append(n)
            here.append(has)
        total = amount(here)
        for value in sorted({amount(options) for options in itertools.product(
                *[[table(axis, place) for place in range(counts[axis])] for axis in range(3)])}):
            @pl.when(total == value)
            def _(value=value):
                some = units.at[pl.ds(0, value)]
                pltpu.make_async_copy(some, some, sem).wait()

    def arrive(phase, make, offsets):
        wait_for(rsem.at[phase], [(make, offsets)])

    def leave(pairs):
        wait_for(ssem, pairs)

    def mate_copy(stage, k):
        n = base[stage] + k
        return pltpu.make_async_remote_copy(
            src_ref=red_s.at[stage], dst_ref=red_r.at[n], send_sem=lssem.at[stage],
            recv_sem=lrsem.at[stage], device_id=mate(mates[stage][k]), device_id_type=MESH)

    def sum_begin(stage, value):
        red_s[stage] = value
        for k in range(len(mates[stage])):
            mate_copy(stage, k).start()

    def sum_end(stage):
        some = red_r.at[pl.ds(base[stage], len(mates[stage]))]
        pltpu.make_async_copy(some, some, lrsem.at[stage]).wait()
        return total_of([red_s[stage]] + [red_r[base[stage] + k] for k in range(len(mates[stage]))])

    strip = (lane[:by] < WIDTH) | (lane[:by] >= bz - WIDTH)
    place = lax.rem(lane + WIDTH, bz)
    low = lax.rem(place, SPAN) < WIDTH
    band = (lane < WIDTH) | (lane >= bz - WIDTH)
    first, last = lane == 0, lane == bz - 1

    def turn_to(v, shift):
        shift = shift % bz
        return v if shift == 0 else pltpu.roll(v, shift, 1)

    def pack(planes):
        pieces = [turn_to(jnp.where(strip, plane, 0.0), SPAN * i) for i, plane in enumerate(planes)]
        ends = (total_of(pieces[bx - WIDTH:]), total_of(pieces[:WIDTH]))
        return ends, total_of(pieces[WIDTH:bx - WIDTH] + list(ends))

    def lines(v, wide):
        a, b = v
        la, ra = pltpu.roll(a, 1, 1), pltpu.roll(a, bz - 1, 1)
        lb, rb = pltpu.roll(b, 1, 1), pltpu.roll(b, bz - 1, 1)
        sa = a + jnp.where(first, lb, la) + jnp.where(last, rb, ra)
        return sa, b + jnp.where(first, la, lb) + jnp.where(last, ra, rb) if wide else None

    def boxes(value, start, stop, wide=True):
        held, pairs = {}, {}

        def at(i):
            if i not in held:
                held[i] = value(i)
            return held[i]

        def pair(i):
            if i not in pairs:
                pairs[i] = [p + q for p, q in zip(at(i), at(i + 1))]
            return pairs[i]

        def result(i):
            if (i - start) % 2 == 0:
                around = [p + q for p, q in zip(at(i - 1), pair(i))]
            else:
                around = [p + q for p, q in zip(pair(i - 1), at(i + 1))]
            total = []
            for t in range(2):
                ys[t, i, EDGE:EDGE + ey, :] = around[t]
                total.append(around[t] + ys[t, i, EDGE - 1:EDGE - 1 + ey, :] + ys[t, i, EDGE + 1:EDGE + 1 + ey, :])
            return lines(total, wide)

        return at, result

    def box(v):
        s = v + pltpu.roll(v, 1, 2) + pltpu.roll(v, v.shape[2] - 1, 2)
        s = s + pltpu.roll(s, 1, 1) + pltpu.roll(s, v.shape[1] - 1, 1)
        zero = jnp.zeros_like(s[:1])
        return s + jnp.concatenate([zero, s[:-1]], 0) + jnp.concatenate([s[1:], zero], 0)

    down = (2 * lane8) % bz
    down_c = (2 * lane8) % half
    up_a = lane8 >> 1
    up_b = (lane8 + bz) >> 1
    up_c = jnp.where(lane8 < 3 * quarter, lane8 >> 1, (lane8 >> 1) + half)

    def paired(v):
        return v + pltpu.roll(v, bz - 1, v.ndim - 1)

    lx = ox + 2

    def restricted(of):
        for m in range(lx):
            a0, b0 = of(2 * m + INNER)
            a1, b1 = of(2 * m + INNER + 1)
            xr0[m * ey:(m + 1) * ey, :] = a0 + a1
            xr1[m * ey:(m + 1) * ey, :] = b0 + b1
        n = lx * my
        a = xr0[pl.ds(0, n, stride=2), :] + xr0[pl.ds(1, n, stride=2), :]
        b = xr1[pl.ds(0, n, stride=2), :] + xr1[pl.ds(1, n, stride=2), :]
        a, b = pick(paired(0.5 * a), down), pick(paired(0.5 * b), down)
        return jnp.where(iota(a.shape, 1) < half, a, b).reshape(lx, my, bz)

    turn = lane8 // quarter

    def coarsened(v):
        for m in range(qx):
            xm[m * my:(m + 1) * my, :] = v[2 * m] + v[2 * m + 1]
        n = qx * my // 2
        a = xm[pl.ds(0, n, stride=2), :] + xm[pl.ds(1, n, stride=2), :]
        a = pick(paired(0.5 * a), down_c)
        rows = my // 2
        tile = a[:rows]
        for m in range(1, qx):
            tile = jnp.where(turn == m, a[m * rows:(m + 1) * rows], tile)
        return pltpu.roll(tile, rows - 2, 0)

    rim = (lane8 < RIM) | ((lane8 >= half - RIM) & (lane8 < half))
    edge1 = my // 2 - by // 4
    here_ends = (lane8 < RIM * ox) | ((lane8 >= half - RIM) & (lane8 < half - RIM + RIM * ox))

    def post(s, v1, tile):
        own = [v1[p][edge1:edge1 + by // 2] for p in range(ox)]
        ends = total_of([turn_to(jnp.where(rim, own[p], 0.0), RIM * p) for p in range(ox)])
        ends = jnp.where(here_ends, ends, pltpu.roll(turn_to(ends, RIM * ox), 4, 0))
        tile = jnp.where(row8 < qy, tile, ends)
        s[0] = tile
        for k in range(ox // 2):
            s[1 + k] = jnp.where(lane8 < half, own[2 * k], pltpu.roll(own[2 * k + 1], half, 1))
        s[4] = tile

    def middle(s, r, width):
        depth = RIM // 2 if width > 2 else 1

        def get(dx, dy, dz, k):
            if (dx, dy, dz) == (0, 0, 0):
                return s[k]
            if any(abs(d) >= n for d, n in zip((dx, dy, dz), counts)):
                return jnp.zeros((8, bz), jnp.float32)
            return r[kx + dx, ky + dy, 1 + dz, k]

        def rows(tiles):
            before, here, after = tiles
            return (pltpu.roll(jnp.where(row8 >= 4, before, here), 4, 0),
                    pltpu.roll(jnp.where(row8 >= 4, here, after), 4, 0))

        planes = []
        for dx in (-1, 0, 1):
            tiles = range(ox // 2 - depth, ox // 2) if dx < 0 else range(depth) if dx > 0 else range(ox // 2)
            ends = [jnp.where(lane8 < 2 * RIM * ox + RIM, get(dx, dy, 1, 4), get(dx, dy, -1, 4)) for dy in (-1, 0, 1)]
            ends = [jnp.where(row8 < 4, pltpu.roll(ends[k], 4, 0), turn_to(ends[k + 1], -RIM * ox)) for k in range(2)]
            for k in tiles:
                pair = rows([get(dx, dy, 0, 1 + k) for dy in (-1, 0, 1)])
                for odd in (0, 1):
                    p = 2 * k + odd
                    planes.append(jnp.concatenate([
                        jnp.where(lane8 < half, pltpu.roll(t, half, 1) if odd else t, turn_to(e, half - RIM * p))
                        for t, e in zip(pair, ends)], 0))
        return jnp.stack(planes)

    xs = [x for x in range(-PART, qx + PART) if -kx * qx <= x < (kx + 1) * qx]

    def gathered(s, r, far):
        zero = jnp.zeros((8, bz), jnp.float32)

        def get(dx, dy, dz):
            if (dx, dy, dz) == (0, 0, 0):
                return s[0]
            if any(abs(d) >= n for d, n in zip((dx, dy, dz), counts)) or abs(dy) > far:
                return zero
            return r[kx + dx, ky + dy, 1 + dz, part((-dx, -dy, -dz), 0)[0]]

        columns = {}
        for dx in sorted({x // qx for x in xs}):
            for dy in range(-2, 3):
                if abs(dy) > far:
                    continue
                here = get(dx, dy, 0)
                after = pltpu.roll(get(dx, dy, 1), quarter, 1)
                before = pltpu.roll(get(dx, dy, -1), 3 * quarter, 1)
                for m in range(qx):
                    tile = jnp.where(turn == (m + 1) % 4, after, here)
                    tile = jnp.where(turn == (m + 3) % 4, before, tile)
                    columns[dx * qx + m, dy] = turn_to(tile, -quarter * m)
        planes = []
        for x in xs:
            t = {dy: columns.get((x, dy), zero) for dy in range(-2, 3)}
            upper = jnp.where(row8 < qy, t[-1], pltpu.roll(t[0], 4, 0))
            if far > 1:
                lower = jnp.where(row8 < qy, t[1], pltpu.roll(jnp.where(row8 < 2, t[2], t[-2]), 4, 0))
            else:
                lower = jnp.where(row8 < qy, t[1], 0.0)
            planes.append(jnp.concatenate([upper, lower], 0))
        return jnp.stack(planes)

    def within(place, axis, size):
        place = place + me[axis] * size
        return (place >= 0) & (place < counts[axis] * size)

    for copy in copies:
        copy.wait()
    g, c = ([gc0[n, WIDTH + i, EDGE:EDGE + by, :] for i in range(bx)] for n in range(2))
    for i in range(bx):
        g_ref[i] = g[i]
    (g_last, g_first), pk[0] = pack(g)
    (c_last, c_first), pk[1] = pack(c)
    pkx[0] = g_last + turn_to(c_last, -SPAN * WIDTH)
    pkx[1] = g_first + turn_to(c_first, SPAN * WIDTH)

    for m in range(ox):
        xr0[m * ey + EDGE:m * ey + EDGE + by, :] = c[2 * m] + c[2 * m + 1]
    n = ox * my
    own1 = xr0[pl.ds(0, n, stride=2), :] + xr0[pl.ds(1, n, stride=2), :]
    own1 = pick(paired(0.5 * own1), down).reshape(ox, my, bz)
    post(s0, own1, coarsened(own1))

    def relay_copy(offset):
        dx, dy, dz = offset
        if (dy, dz) == (0, 0):
            return coarse_copy(2, offset, s0, r0, RIM // 2)
        far = abs(dx) > 1 or abs(dy) > 1
        at, size = part((-dx, 0, 0), RIM // 2)
        if far or dz != 0:
            at, size = 4 if dx == -1 else 0, 1
        src = s0.at[pl.ds(at, size)] if dx == 0 else r0.at[kx + dx, ky, 1, pl.ds(at, size)]
        goes = 0 if far else 4 if dz != 0 else at
        return src, r0.at[kx + dx, ky - dy, 1 - dz, pl.ds(goes, size)], 5, (0, dy, dz)

    along_x = [o for o in near if o[1] == o[2] == 0]
    onwards = [o for o in near if o not in along_x]
    make_b = lambda o: coarse_copy(3, o, s1, r1, RIM // 2)
    make_d = lambda o: coarse_copy(4, o, s2, r2, 1)
    pl.semaphore_wait(barrier, greeted)
    begin(relay_copy, along_x)
    begin(fine_copy, close)

    in_y = within(row - EDGE, 1, by)
    in_z = band & within(jnp.where(lane < half, lane + bz, lane - bz), 2, bz)

    def spread(i):
        for f in range(2):
            if i < WIDTH:
                k = i
                piece = turn_to(ends[0], -SPAN * (bx - WIDTH + k - WIDTH * f))
            elif i >= WIDTH + bx:
                k = i - WIDTH - bx
                piece = turn_to(ends[1], -SPAN * (k + WIDTH * f))
            else:
                piece = turn_to(merged[f], -SPAN * (i - WIDTH))
            t1[f, i] = jnp.where(band, piece, 0.0)
        in_x = within(jnp.full((ey, bz), i - WIDTH, jnp.int32), 0, bx)
        ca, cb = gc0[1, i], t1[1, i]
        da = jnp.where(in_y & in_x, relaxation / (26.0 + ca), 0.0)
        db = jnp.where(in_y & in_x & in_z, relaxation / (26.0 + cb), 0.0)
        ka, kb = 27.0 + ca, 27.0 + cb
        for ref, a, b in ((d, da, db), (k27, ka, kb), (w27, 1.0 - da * ka, 1.0 - db * kb)):
            ref[0, i], ref[1, i] = a, b

    arrive(2, relay_copy, along_x)
    begin(relay_copy, onwards)
    begin(outer_copy, sides)
    arrive(0, fine_copy, close)
    merged = [jnp.where(low, zr[0, f], zr[1, f]) for f in range(2)]
    ends = [jnp.where(low, zrx[0, e], zrx[1, e]) for e in range(2)]
    skip = WIDTH - INNER
    for i in range(skip, ex - skip):
        spread(i)

    def inside1(shape, width):
        zl = iota(shape, 2)
        zl = jnp.where(zl < 3 * quarter, zl, zl - bz)
        ok = within(iota(shape, 0) - width, 0, ox) & within(iota(shape, 1) - edge1, 1, by // 2)
        return ok & within(zl, 2, half) & (zl >= -RIM) & (zl < half + RIM)

    c1 = restricted(lambda i: (gc0[1, i], t1[1, i]))
    near0 = jnp.where(inside1((lx, my, bz), 1), relaxation / (26.0 + c1), 0.0)
    near1 = 27.0 + c1

    def coefficients():
        arrive(1, outer_copy, sides)
        for i in list(range(skip)) + list(range(ex - skip, ex)):
            spread(i)
        arrive(5, relay_copy, onwards)
        c1 = middle(s0, r0, RIM)
        ok = inside1(c1.shape, RIM)
        c1 = jnp.where(ok, c1, 0.0)
        mid[0] = jnp.where(ok, relaxation / (26.0 + c1), 0.0)
        mid[1] = 27.0 + c1
        c2 = gathered(s0, r0, ky)
        shape = c2.shape
        z = iota(shape, 2)
        z = jnp.where(z < 2 * quarter, z, z - bz)
        y = iota(shape, 1)
        y = jnp.where(y < my - 2, y, y - my) - qy
        ok = within(iota(shape, 0) + xs[0], 0, qx) & within(y, 1, qy)
        ok = ok & within(z, 2, quarter) & (z >= -quarter)
        c2 = jnp.where(ok, c2, 0.0)
        kept[0] = jnp.where(ok, relaxation / (26.0 + c2), 0.0)
        kept[1] = 27.0 + c2

    def cycle(phase, g_at, near0, near1, s, r, make, offsets, far, width, hook, second, finish):
        def e0(i):
            a, b = g_at(i)
            return d[0, i] * a, d[1, i] * b

        start = WIDTH - 2
        at, result = boxes(e0, start, ex - start)

        def remainder(i):
            a, b = g_at(i)
            sa, sb = result(i)
            return w27[0, i] * a + sa, w27[1, i] * b + sb

        g1 = restricted(remainder)
        f = near0 * g1
        post(s, g1[1:1 + ox], coarsened((g1 - near1 * f + box(f))[1:1 + ox]))
        begin(make, offsets)
        hook()
        arrive(phase, make, offsets)
        inv, diag = kept[0], kept[1]
        g2 = jnp.where(inv > 0.0, gathered(s, r, far), 0.0)
        e = inv * g2
        for sweep in range(SWEEPS - 1):
            e = e + inv * (g2 - diag * e + box(e))
        second()
        reach = (width + 1) // 2
        nq = qx + 2 * reach
        zero = jnp.zeros_like(e[:1])
        e = jnp.concatenate([e[xs.index(x)][None] if x in xs else zero for x in range(-reach, qx + reach)], 0)
        e = pltpu.roll(e, my - 2, 1)[:, :my // 2].reshape(nq * my // 2, bz)
        u = pick(e, up_c)
        um[pl.ds(0, nq * my // 2, stride=2), :] = u
        um[pl.ds(1, nq * my // 2, stride=2), :] = u
        u = um[:nq * my, :].reshape(nq, my, bz)
        span = width + 1
        mx = ox + 2 * span
        u = jnp.concatenate([u[(m - span) // 2 + reach][None] for m in range(mx)], 0)
        skip1 = RIM - span
        inv, diag = mid[0, skip1:skip1 + mx], mid[1, skip1:skip1 + mx]
        g1 = jnp.where(inv > 0.0, middle(s, r, span), 0.0)
        f = inv * g1 + u
        f = f + inv * (g1 - diag * f + box(f))
        nm = mx - 2
        f = f[1:mx - 1].reshape(nm * my, bz)
        for pf, up in ((pf0, up_a), (pf1, up_b)):
            w = pick(f, up)
            pf[pl.ds(0, nm * my, stride=2), :] = w
            pf[pl.ds(1, nm * my, stride=2), :] = w

        def e1(i):
            m = (i - WIDTH) // 2 + width
            a, b = e0(i)
            return a + pf0[m * ey:(m + 1) * ey, :], b + pf1[m * ey:(m + 1) * ey, :]

        wide = width > 1
        past = INNER + 1 if wide else 1
        at1, result1 = boxes(e1, WIDTH - past, WIDTH + bx + past)

        def e2(i):
            return [w27[t, i] * a + e + d[t, i] * s_ for t, (a, e, s_) in enumerate(zip(at1(i), e0(i), result1(i)))]

        at2, result2 = boxes(e2, WIDTH - past + 1, WIDTH + bx + past - 1, wide)
        for i in range(WIDTH - past + 1, WIDTH + bx + past - 1):
            a, b = at2(i)
            sa, sb = result2(i)
            finish(i, a, k27[0, i] * a - sa, k27[1, i] * b - sb if wide else None)

    gamma, delta = [], []

    def own(i):
        return WIDTH <= i < WIDTH + bx

    def finish1(i, e, out, out_b):
        im0[0, i] = out
        im0[1, i] = out_b
        if own(i):
            e, out = e[EDGE:EDGE + by], out[EDGE:EDGE + by]
            pre_ref[i - WIDTH] = e
            img_ref[i - WIDTH] = out
            gamma.append(g_ref[i - WIDTH] * e)
            delta.append(out * e)
        if i == WIDTH + bx - 1:
            gs = jnp.sum(total_of(gamma), axis=0, keepdims=True)
            ds = jnp.sum(total_of(delta), axis=0, keepdims=True)
            gs, ds = gs + pltpu.roll(gs, half, 1), ds + pltpu.roll(ds, half, 1)
            sum_begin(0, jnp.where(lane8[:1] < half, gs, ds))

    nothing = lambda: None
    cycle(3, lambda i: (gc0[0, i], t1[0, i]), near0, near1, s1, r1, make_b, near, ky, RIM - 1, coefficients, nothing, finish1)

    def relay(stage):
        if len(groups) > 1:
            sum_begin(stage, sum_end(stage - 1))

    def finish2(i, e, out, out_b):
        twice_ref[i - WIDTH] = e[EDGE:EDGE + by]
        image_twice_ref[i - WIDTH] = out[EDGE:EDGE + by]

    skip1 = RIM - 1
    cycle(4, lambda i: (im0[0, i], im0[1, i]), mid[0, skip1:skip1 + lx], mid[1, skip1:skip1 + lx], s2, r2, make_d, later, 1, 1,
          lambda: relay(1), lambda: relay(2), finish2)

    total = sum_end(len(groups) - 1)
    gs = jnp.sum(jnp.where(lane8[:1] < half, total, 0.0), axis=1, keepdims=True)
    ds = jnp.sum(jnp.where(lane8[:1] < half, 0.0, total), axis=1, keepdims=True)
    alpha_ref[...] = jnp.broadcast_to(gs / ds, (1, bz)).reshape(alpha_ref.shape)
    leave([(fine_copy, close), (outer_copy, sides), (relay_copy, near), (make_b, near), (make_d, later)])
    for stage in range(len(groups)):
        some = red_r.at[pl.ds(base[stage], len(mates[stage]))]
        pltpu.make_async_copy(some, some, lssem.at[stage]).wait()


def solution(mesh):
    counts = tuple(mesh.shape[a] for a in AXES)

    def shards(right_side, coefficient):
        bx, by, bz = block = right_side.shape
        assert SPAN <= bx and SPAN * bx <= bz and by == 16 and bx % 4 == 0
        kx = max(1, min(-(-PART // (bx // 4)), counts[0] - 1))
        ky = max(1, min(-(-PART // (by // 4)), counts[1] - 1))
        ex, ey = bx + SPAN, by + 2 * EDGE
        ox, my = bx // 2, ey // 2
        qx = bx // 4
        mx = ox + 2 * RIM
        most = (2 * kx + 1) * (2 * ky + 1) * 3
        planes = len([x for x in range(-PART, qx + PART) if -kx * qx <= x < (kx + 1) * qx])
        mates = [len(partners(counts, group)) for group in stages(counts)]
        f32 = jnp.float32
        vmem = pl.BlockSpec(memory_space=pltpu.VMEM)
        messages = [pltpu.VMEM((5, 8, bz), f32)] * 3
        messages += [pltpu.VMEM((2 * kx + 1, 2 * ky + 1, 3, 5, 8, bz), f32)] * 3
        precond, image, twice, image_twice, alpha, g = pl.pallas_call(
            functools.partial(kernel, counts, block, kx, ky),
            out_shape=[pltpu.VMEM(block, f32)] * 4 + [pltpu.VMEM((1, 1, bz), f32), pltpu.VMEM(block, f32)],
            in_specs=[pl.BlockSpec(memory_space=pltpu.HBM)] * 2,
            out_specs=[vmem] * 6,
            scratch_shapes=[
                pltpu.VMEM((2, ex, ey, bz), f32),
                pltpu.VMEM((2, ex, ey, bz), f32),
                pltpu.VMEM((2, by, bz), f32),
                pltpu.VMEM((2, by, bz), f32),
                pltpu.VMEM((2, 2, ey, bz), f32),
                pltpu.VMEM((2, 2, ey, bz), f32),
                pltpu.VMEM((2, ex, ey, bz), f32),
                *[pltpu.VMEM((2, ex, ey, bz), f32)] * 3,
                pltpu.VMEM((2, ex, ey + 2 * EDGE, bz), f32),
                pltpu.VMEM(((ox + 2) * ey, bz), f32),
                pltpu.VMEM(((ox + 2) * ey, bz), f32),
                pltpu.VMEM(((mx - 2) * ey, bz), f32),
                pltpu.VMEM(((mx - 2) * ey, bz), f32),
                pltpu.VMEM((qx * my, bz), f32),
                pltpu.VMEM(((qx + 4) * my, bz), f32),
                *messages,
                pltpu.VMEM((2, planes, my, bz), f32),
                pltpu.VMEM((2, mx, my, bz), f32),
                pltpu.VMEM((len(mates), 1, bz), f32),
                pltpu.VMEM((sum(mates), 1, bz), f32),
                pltpu.VMEM((16 * most, 8, bz), f32),
                pltpu.SemaphoreType.DMA((2,)),
                pltpu.SemaphoreType.DMA,
                pltpu.SemaphoreType.DMA((6,)),
                pltpu.SemaphoreType.DMA((len(mates),)),
                pltpu.SemaphoreType.DMA((len(mates),)),
            ],
            compiler_params=pltpu.CompilerParams(collective_id=0, has_side_effects=True),
            name="relayed",
        )(right_side, coefficient)
        return (alpha * precond, g - alpha * image,
                precond - alpha * twice, image - alpha * image_twice)

    placed = (P(*AXES), P(*AXES))
    return jax.shard_map(
        shards, mesh=mesh, in_specs=placed, out_specs=(P(*AXES),) * 4, check_vma=False
    )
```

```python
import functools
import itertools

import jax
import jax.numpy as jnp
from jax import lax
from jax.experimental import pallas as pl
from jax.experimental.pallas import tpu as pltpu
from jax.sharding import PartitionSpec as P

SWEEPS = 4
relaxation = 0.6

AXES = ("gx", "gy", "gz")
MESH = pl.DeviceIdType.MESH
WIDTH = 5
INNER = 3
EDGE = 8
SPAN = 2 * WIDTH
RIM = 4
PART = SWEEPS + 1


def pick(values, lanes):
    flat = values.reshape(-1, values.shape[-1])
    lanes = jnp.broadcast_to(lanes[:1], flat.shape)
    return jnp.take_along_axis(flat, lanes, axis=1).reshape(values.shape)


def iota(shape, dim):
    return lax.broadcasted_iota(jnp.int32, shape, dim)


def total_of(values):
    while len(values) > 1:
        values = [a + b for a, b in zip(values[::2], values[1::2])] + values[len(values) & ~1:]
    return values[0]


def stages(counts):
    if max(counts) <= RIM:
        return [(0, 1, 2)]
    return [(2,), (1,), (0,)]


def partners(counts, group):
    steps = [(0, 0, 0)]
    for axis in group:
        steps = [s[:axis] + (k,) + s[axis + 1:] for s in steps for k in range(counts[axis])]
    return [s for s in steps if s != (0, 0, 0)]


def kernel(counts, block, kx, ky, g_hbm, c_hbm, pre_ref, img_ref, twice_ref, image_twice_ref, alpha_ref, g_ref,
           gc0, im0, pk, pkx, zr, zrx, t1, d, k27, w27, ys, xr0, xr1, pf0, pf1, xm, um,
           s0, s1, s2, r0, r1, r2, kept, mid, red_s, red_r, units, insem, ssem, rsem, lssem, lrsem):
    bx, by, bz = block
    me = [lax.axis_index(a) for a in AXES]
    ex, ey = bx + SPAN, by + 2 * EDGE
    ox, my = bx // 2, ey // 2
    qx, qy = bx // 4, by // 4
    half, quarter = bz // 2, bz // 4
    lane = iota((ey, bz), 1)
    row = iota((ey, bz), 0)
    lane8 = iota((8, bz), 1)
    row8 = iota((8, bz), 0)

    def valid(offset):
        ok = None
        for axis, step in enumerate(offset):
            if step == 0:
                continue
            place = me[axis] + step
            term = place >= 0 if step < 0 else place < counts[axis]
            ok = term if ok is None else jnp.logical_and(ok, term)
        return ok

    def target(offset):
        return tuple(m + s for m, s in zip(me, offset))

    near = [(dx, dy, dz) for dx in range(-kx, kx + 1) for dy in range(-ky, ky + 1) for dz in (-1, 0, 1)]
    near = [o for o in near if o != (0, 0, 0) and all(counts[a] > abs(o[a]) for a in range(3))]
    near.sort(key=lambda o: -sum(map(abs, o)))
    close = [o for o in near if abs(o[0]) <= 1 and abs(o[1]) <= 1]
    sides = [o for o in close if o[0] != 0 and o[2] == 0]
    later = [o for o in near if abs(o[1]) <= 1]

    groups = stages(counts)
    mates = []
    base = [0]
    for group in groups:
        mates.append(partners(counts, group))
        base.append(base[-1] + len(mates[-1]))

    def mate(step):
        return tuple(lax.rem(m + s, n) if s else m for m, s, n in zip(me, step, counts))

    inside0 = gc0.at[:, pl.ds(WIDTH, bx), pl.ds(EDGE, by), :]
    copies = [pltpu.make_async_copy(src, inside0.at[n], insem.at[n]) for n, src in enumerate((g_hbm, c_hbm))]
    for copy in copies:
        copy.start()
    barrier = pltpu.get_barrier_semaphore()
    for offset in near:
        @pl.when(valid(offset))
        def _(offset=offset):
            pl.semaphore_signal(barrier, inc=1, device_id=target(offset), device_id_type=MESH)
    greeted = 0
    if len(groups) > 1:
        for steps in mates:
            for step in steps:
                pl.semaphore_signal(barrier, inc=1, device_id=mate(step), device_id_type=MESH)
            greeted = greeted + len(steps)

    def options(axis, far):
        total = 1
        for step in range(1, far + 1):
            if counts[axis] > step:
                total = total + (me[axis] >= step).astype(jnp.int32)
                total = total + (me[axis] + step < counts[axis]).astype(jnp.int32)
        return total

    greeted = greeted + options(0, kx) * options(1, ky) * options(2, 1) - 1

    def clear(ref):
        ref[...] = jnp.zeros(ref.shape, jnp.float32)

    for axis, edges in enumerate((
            [[gc0.at[:, pl.ds(0, WIDTH)], zrx.at[:, 0]], [gc0.at[:, pl.ds(WIDTH + bx, WIDTH)], zrx.at[:, 1]]],
            [[ref.at[..., pl.ds(at, WIDTH), :] for ref in (gc0, zr, zrx)] for at in (EDGE - WIDTH, EDGE + by)],
            [[ref.at[side] for ref in (zr, zrx)] for side in range(2)])):
        for refs, edge in zip(edges, (0, counts[axis] - 1)):
            @pl.when(me[axis] == edge)
            def _(refs=refs):
                for ref in refs:
                    clear(ref)

    for ref in (gc0, zr, zrx):
        clear(ref.at[..., pl.ds(0, EDGE - WIDTH), :])
        clear(ref.at[..., pl.ds(ey - EDGE + WIDTH, EDGE - WIDTH), :])
    for at in (0, EDGE + ey):
        ys[:, :, at:at + EDGE, :] = jnp.zeros((2, ex, EDGE, bz), jnp.float32)

    def row_ends(dy):
        if dy == 0:
            return 0, by, EDGE
        if dy > 0:
            return by - WIDTH, WIDTH, EDGE - WIDTH
        return 0, WIDTH, EDGE + by

    def remote(src, dst, phase, offset):
        pltpu.make_async_remote_copy(
            src_ref=src, dst_ref=dst, send_sem=ssem, recv_sem=rsem.at[phase],
            device_id=target(offset), device_id_type=MESH).start()

    def planes_copy(phase, offset, first, size):
        dx, dy, dz = offset
        start, rows, goes = row_ends(dy)
        if dx == 0:
            px, tx, size = WIDTH, WIDTH, bx
        elif dx > 0:
            px, tx = WIDTH + bx - first - size, WIDTH - first - size
        else:
            px, tx = WIDTH + first, WIDTH + bx + first
        src = gc0.at[:, pl.ds(px, size), pl.ds(EDGE + start, rows), :]
        dst = gc0.at[:, pl.ds(tx, size), pl.ds(goes, rows), :]
        return (src, dst, phase, offset)

    def fine_copy(offset):
        dx, dy, dz = offset
        if dz == 0:
            return planes_copy(0, offset, 0, INNER)
        start, rows, goes = row_ends(dy)
        side = 0 if dz > 0 else 1
        if dx == 0:
            src = pk.at[:, pl.ds(start, rows), :]
            dst = zr.at[side, :, pl.ds(goes, rows), :]
        else:
            end = 0 if dx > 0 else 1
            src = pkx.at[end, pl.ds(start, rows), :]
            dst = zrx.at[side, end, pl.ds(goes, rows), :]
        return (src, dst, 0, offset)

    def outer_copy(offset):
        return planes_copy(1, offset, INNER, WIDTH - INNER)

    def part(offset, depth):
        dx, dy, dz = offset
        if abs(dx) > 1 or abs(dy) > 1:
            return 0, 1
        if dz != 0:
            return 4, 1
        if dx == 0:
            return 0, 4
        if dx < 0:
            return 0, 1 + depth
        return 4 - depth, 1 + depth

    def coarse_copy(phase, offset, s, r, depth):
        dx, dy, dz = offset
        at, size = part(offset, depth)
        return (s.at[pl.ds(at, size)], r.at[kx - dx, ky - dy, 1 - dz, pl.ds(at, size)], phase, offset)

    def tiles(make, offset):
        size = 1
        for n in make(offset)[0].shape:
            size *= n
        assert size % bz == 0
        return size // bz

    def begin(make, offsets):
        for offset in offsets:
            @pl.when(valid(offset))
            def _(offset=offset):
                remote(*make(offset))

    def wait_for(sem, pairs):
        sizes = {}
        for make, offsets in pairs:
            for offset in offsets:
                key = tuple(map(abs, offset))
                sizes.setdefault(key, 0)
                if offset == key:
                    sizes[key] += tiles(make, offset)

        def amount(options):
            total = 0
            for (a, b, c), size in sizes.items():
                total = total + size * options[0][a] * options[1][b] * options[2][c]
            return total

        def number(place, count, step):
            return 1 if step == 0 else (place >= step) * 1 + (place + step < count) * 1

        def table(axis, place):
            return [number(place, counts[axis], k) for k in range(3)]

        here = []
        for axis in range(3):
            has = [1]
            for k in (1, 2):
                n = (me[axis] >= k).astype(jnp.int32) + (me[axis] + k < counts[axis]).astype(jnp.int32)
                has.append(n)
            here.append(has)
        total = amount(here)
        for value in sorted({amount(options) for options in itertools.product(
                *[[table(axis, place) for place in range(counts[axis])] for axis in range(3)])}):
            @pl.when(total == value)
            def _(value=value):
                some = units.at[pl.ds(0, value)]
                pltpu.make_async_copy(some, some, sem).wait()

    def arrive(phase, make, offsets):
        wait_for(rsem.at[phase], [(make, offsets)])

    def leave(pairs):
        wait_for(ssem, pairs)

    def mate_copy(stage, k):
        n = base[stage] + k
        return pltpu.make_async_remote_copy(
            src_ref=red_s.at[stage], dst_ref=red_r.at[n], send_sem=lssem.at[stage],
            recv_sem=lrsem.at[stage], device_id=mate(mates[stage][k]), device_id_type=MESH)

    def sum_begin(stage, value):
        red_s[stage] = value
        for k in range(len(mates[stage])):
            mate_copy(stage, k).start()

    def sum_end(stage):
        some = red_r.at[pl.ds(base[stage], len(mates[stage]))]
        pltpu.make_async_copy(some, some, lrsem.at[stage]).wait()
        return total_of([red_s[stage]] + [red_r[base[stage] + k] for k in range(len(mates[stage]))])

    strip = (lane[:by] < WIDTH) | (lane[:by] >= bz - WIDTH)
    place = lax.rem(lane + WIDTH, bz)
    low = lax.rem(place, SPAN) < WIDTH
    band = (lane < WIDTH) | (lane >= bz - WIDTH)
    first, last = lane == 0, lane == bz - 1

    def turn_to(v, shift):
        shift = shift % bz
        return v if shift == 0 else pltpu.roll(v, shift, 1)

    def pack(planes):
        pieces = [turn_to(jnp.where(strip, plane, 0.0), SPAN * i) for i, plane in enumerate(planes)]
        ends = (total_of(pieces[bx - WIDTH:]), total_of(pieces[:WIDTH]))
        return ends, total_of(pieces[WIDTH:bx - WIDTH] + list(ends))

    def lines(v, wide):
        a, b = v
        la, ra = pltpu.roll(a, 1, 1), pltpu.roll(a, bz - 1, 1)
        lb, rb = pltpu.roll(b, 1, 1), pltpu.roll(b, bz - 1, 1)
        sa = a + jnp.where(first, lb, la) + jnp.where(last, rb, ra)
        return sa, b + jnp.where(first, la, lb) + jnp.where(last, ra, rb) if wide else None

    def boxes(value, start, stop, wide=True):
        held, pairs = {}, {}

        def at(i):
            if i not in held:
                held[i] = value(i)
            return held[i]

        def pair(i):
            if i not in pairs:
                pairs[i] = [p + q for p, q in zip(at(i), at(i + 1))]
            return pairs[i]

        def result(i):
            if (i - start) % 2 == 0:
                around = [p + q for p, q in zip(at(i - 1), pair(i))]
            else:
                around = [p + q for p, q in zip(pair(i - 1), at(i + 1))]
            total = []
            for t in range(2):
                ys[t, i, EDGE:EDGE + ey, :] = around[t]
                total.append(around[t] + ys[t, i, EDGE - 1:EDGE - 1 + ey, :] + ys[t, i, EDGE + 1:EDGE + 1 + ey, :])
            return lines(total, wide)

        return at, result

    def box(v):
        s = v + pltpu.roll(v, 1, 2) + pltpu.roll(v, v.shape[2] - 1, 2)
        s = s + pltpu.roll(s, 1, 1) + pltpu.roll(s, v.shape[1] - 1, 1)
        zero = jnp.zeros_like(s[:1])
        return s + jnp.concatenate([zero, s[:-1]], 0) + jnp.concatenate([s[1:], zero], 0)

    down = (2 * lane8) % bz
    down_c = (2 * lane8) % half
    up_a = lane8 >> 1
    up_b = (lane8 + bz) >> 1
    up_c = jnp.where(lane8 < 3 * quarter, lane8 >> 1, (lane8 >> 1) + half)

    def paired(v):
        return v + pltpu.roll(v, bz - 1, v.ndim - 1)

    lx = ox + 2

    def restricted(of):
        for m in range(lx):
            a0, b0 = of(2 * m + INNER)
            a1, b1 = of(2 * m + INNER + 1)
            xr0[m * ey:(m + 1) * ey, :] = a0 + a1
            xr1[m * ey:(m + 1) * ey, :] = b0 + b1
        n = lx * my
        a = xr0[pl.ds(0, n, stride=2), :] + xr0[pl.ds(1, n, stride=2), :]
        b = xr1[pl.ds(0, n, stride=2), :] + xr1[pl.ds(1, n, stride=2), :]
        a, b = pick(paired(0.5 * a), down), pick(paired(0.5 * b), down)
        return jnp.where(iota(a.shape, 1) < half, a, b).reshape(lx, my, bz)

    turn = lane8 // quarter

    def coarsened(v):
        for m in range(qx):
            xm[m * my:(m + 1) * my, :] = v[2 * m] + v[2 * m + 1]
        n = qx * my // 2
        a = xm[pl.ds(0, n, stride=2), :] + xm[pl.ds(1, n, stride=2), :]
        a = pick(paired(0.5 * a), down_c)
        rows = my // 2
        tile = a[:rows]
        for m in range(1, qx):
            tile = jnp.where(turn == m, a[m * rows:(m + 1) * rows], tile)
        return pltpu.roll(tile, rows - 2, 0)

    rim = (lane8 < RIM) | ((lane8 >= half - RIM) & (lane8 < half))
    edge1 = my // 2 - by // 4
    here_ends = (lane8 < RIM * ox) | ((lane8 >= half - RIM) & (lane8 < half - RIM + RIM * ox))

    def post(s, v1, tile):
        own = [v1[p][edge1:edge1 + by // 2] for p in range(ox)]
        ends = total_of([turn_to(jnp.where(rim, own[p], 0.0), RIM * p) for p in range(ox)])
        ends = jnp.where(here_ends, ends, pltpu.roll(turn_to(ends, RIM * ox), 4, 0))
        tile = jnp.where(row8 < qy, tile, ends)
        s[0] = tile
        for k in range(ox // 2):
            s[1 + k] = jnp.where(lane8 < half, own[2 * k], pltpu.roll(own[2 * k + 1], half, 1))
        s[4] = tile

    def middle(s, r, width):
        depth = RIM // 2 if width > 2 else 1

        def get(dx, dy, dz, k):
            if (dx, dy, dz) == (0, 0, 0):
                return s[k]
            if any(abs(d) >= n for d, n in zip((dx, dy, dz), counts)):
                return jnp.zeros((8, bz), jnp.float32)
            return r[kx + dx, ky + dy, 1 + dz, k]

        def rows(tiles):
            before, here, after = tiles
            return (pltpu.roll(jnp.where(row8 >= 4, before, here), 4, 0),
                    pltpu.roll(jnp.where(row8 >= 4, here, after), 4, 0))

        planes = []
        for dx in (-1, 0, 1):
            tiles = range(ox // 2 - depth, ox // 2) if dx < 0 else range(depth) if dx > 0 else range(ox // 2)
            ends = [jnp.where(lane8 < 2 * RIM * ox + RIM, get(dx, dy, 1, 4), get(dx, dy, -1, 4)) for dy in (-1, 0, 1)]
            ends = [jnp.where(row8 < 4, pltpu.roll(ends[k], 4, 0), turn_to(ends[k + 1], -RIM * ox)) for k in range(2)]
            for k in tiles:
                pair = rows([get(dx, dy, 0, 1 + k) for dy in (-1, 0, 1)])
                for odd in (0, 1):
                    p = 2 * k + odd
                    planes.append(jnp.concatenate([
                        jnp.where(lane8 < half, pltpu.roll(t, half, 1) if odd else t, turn_to(e, half - RIM * p))
                        for t, e in zip(pair, ends)], 0))
        return jnp.stack(planes)

    xs = [x for x in range(-PART, qx + PART) if -kx * qx <= x < (kx + 1) * qx]

    def gathered(s, r, far):
        zero = jnp.zeros((8, bz), jnp.float32)

        def get(dx, dy, dz):
            if (dx, dy, dz) == (0, 0, 0):
                return s[0]
            if any(abs(d) >= n for d, n in zip((dx, dy, dz), counts)) or abs(dy) > far:
                return zero
            return r[kx + dx, ky + dy, 1 + dz, part((-dx, -dy, -dz), 0)[0]]

        columns = {}
        for dx in sorted({x // qx for x in xs}):
            for dy in range(-2, 3):
                if abs(dy) > far:
                    continue
                here = get(dx, dy, 0)
                after = pltpu.roll(get(dx, dy, 1), quarter, 1)
                before = pltpu.roll(get(dx, dy, -1), 3 * quarter, 1)
                for m in range(qx):
                    tile = jnp.where(turn == (m + 1) % 4, after, here)
                    tile = jnp.where(turn == (m + 3) % 4, before, tile)
                    columns[dx * qx + m, dy] = turn_to(tile, -quarter * m)
        planes = []
        for x in xs:
            t = {dy: columns.get((x, dy), zero) for dy in range(-2, 3)}
            upper = jnp.where(row8 < qy, t[-1], pltpu.roll(t[0], 4, 0))
            if far > 1:
                lower = jnp.where(row8 < qy, t[1], pltpu.roll(jnp.where(row8 < 2, t[2], t[-2]), 4, 0))
            else:
                lower = jnp.where(row8 < qy, t[1], 0.0)
            planes.append(jnp.concatenate([upper, lower], 0))
        return jnp.stack(planes)

    def within(place, axis, size):
        place = place + me[axis] * size
        return (place >= 0) & (place < counts[axis] * size)

    for copy in copies:
        copy.wait()
    g, c = ([gc0[n, WIDTH + i, EDGE:EDGE + by, :] for i in range(bx)] for n in range(2))
    for i in range(bx):
        g_ref[i] = g[i]
    (g_last, g_first), pk[0] = pack(g)
    (c_last, c_first), pk[1] = pack(c)
    pkx[0] = g_last + turn_to(c_last, -SPAN * WIDTH)
    pkx[1] = g_first + turn_to(c_first, SPAN * WIDTH)

    for m in range(ox):
        xr0[m * ey + EDGE:m * ey + EDGE + by, :] = c[2 * m] + c[2 * m + 1]
    n = ox * my
    own1 = xr0[pl.ds(0, n, stride=2), :] + xr0[pl.ds(1, n, stride=2), :]
    own1 = pick(paired(0.5 * own1), down).reshape(ox, my, bz)
    post(s0, own1, coarsened(own1))

    def relay_copy(offset):
        dx, dy, dz = offset
        if (dy, dz) == (0, 0):
            return coarse_copy(2, offset, s0, r0, RIM // 2)
        far = abs(dx) > 1 or abs(dy) > 1
        at, size = part((-dx, 0, 0), RIM // 2)
        if far or dz != 0:
            at, size = 4 if dx == -1 else 0, 1
        src = s0.at[pl.ds(at, size)] if dx == 0 else r0.at[kx + dx, ky, 1, pl.ds(at, size)]
        goes = 0 if far else 4 if dz != 0 else at
        return src, r0.at[kx + dx, ky - dy, 1 - dz, pl.ds(goes, size)], 5, (0, dy, dz)

    along_x = [o for o in near if o[1] == o[2] == 0]
    onwards = [o for o in near if o not in along_x]
    make_b = lambda o: coarse_copy(3, o, s1, r1, RIM // 2)
    make_d = lambda o: coarse_copy(4, o, s2, r2, 1)
    pl.semaphore_wait(barrier, greeted)
    begin(relay_copy, along_x)
    begin(fine_copy, close)

    in_y = within(row - EDGE, 1, by)
    in_z = band & within(jnp.where(lane < half, lane + bz, lane - bz), 2, bz)

    def spread(i):
        for f in range(2):
            if i < WIDTH:
                k = i
                piece = turn_to(ends[0], -SPAN * (bx - WIDTH + k - WIDTH * f))
            elif i >= WIDTH + bx:
                k = i - WIDTH - bx
                piece = turn_to(ends[1], -SPAN * (k + WIDTH * f))
            else:
                piece = turn_to(merged[f], -SPAN * (i - WIDTH))
            t1[f, i] = jnp.where(band, piece, 0.0)
        in_x = within(jnp.full((ey, bz), i - WIDTH, jnp.int32), 0, bx)
        ca, cb = gc0[1, i], t1[1, i]
        da = jnp.where(in_y & in_x, relaxation / (26.0 + ca), 0.0)
        db = jnp.where(in_y & in_x & in_z, relaxation / (26.0 + cb), 0.0)
        ka, kb = 27.0 + ca, 27.0 + cb
        for ref, a, b in ((d, da, db), (k27, ka, kb), (w27, 1.0 - da * ka, 1.0 - db * kb)):
            ref[0, i], ref[1, i] = a, b

    arrive(2, relay_copy, along_x)
    begin(relay_copy, onwards)
    begin(outer_copy, sides)
    arrive(0, fine_copy, close)
    merged = [jnp.where(low, zr[0, f], zr[1, f]) for f in range(2)]
    ends = [jnp.where(low, zrx[0, e], zrx[1, e]) for e in range(2)]
    skip = WIDTH - INNER
    for i in range(skip, ex - skip):
        spread(i)

    def inside1(shape, width):
        zl = iota(shape, 2)
        zl = jnp.where(zl < 3 * quarter, zl, zl - bz)
        ok = within(iota(shape, 0) - width, 0, ox) & within(iota(shape, 1) - edge1, 1, by // 2)
        return ok & within(zl, 2, half) & (zl >= -RIM) & (zl < half + RIM)

    c1 = restricted(lambda i: (gc0[1, i], t1[1, i]))
    near0 = jnp.where(inside1((lx, my, bz), 1), relaxation / (26.0 + c1), 0.0)
    near1 = 27.0 + c1

    def coefficients():
        arrive(1, outer_copy, sides)
        for i in list(range(skip)) + list(range(ex - skip, ex)):
            spread(i)
        arrive(5, relay_copy, onwards)
        c1 = middle(s0, r0, RIM)
        ok = inside1(c1.shape, RIM)
        c1 = jnp.where(ok, c1, 0.0)
        mid[0] = jnp.where(ok, relaxation / (26.0 + c1), 0.0)
        mid[1] = 27.0 + c1
        c2 = gathered(s0, r0, ky)
        shape = c2.shape
        z = iota(shape, 2)
        z = jnp.where(z < 2 * quarter, z, z - bz)
        y = iota(shape, 1)
        y = jnp.where(y < my - 2, y, y - my) - qy
        ok = within(iota(shape, 0) + xs[0], 0, qx) & within(y, 1, qy)
        ok = ok & within(z, 2, quarter) & (z >= -quarter)
        c2 = jnp.where(ok, c2, 0.0)
        kept[0] = jnp.where(ok, relaxation / (26.0 + c2), 0.0)
        kept[1] = 27.0 + c2

    def cycle(phase, g_at, near0, near1, s, r, make, offsets, far, width, hook, second, finish):
        def e0(i):
            a, b = g_at(i)
            return d[0, i] * a, d[1, i] * b

        start = WIDTH - 2
        at, result = boxes(e0, start, ex - start)

        def remainder(i):
            a, b = g_at(i)
            sa, sb = result(i)
            return w27[0, i] * a + sa, w27[1, i] * b + sb

        g1 = restricted(remainder)
        f = near0 * g1
        post(s, g1[1:1 + ox], coarsened((g1 - near1 * f + box(f))[1:1 + ox]))
        begin(make, offsets)
        hook()
        arrive(phase, make, offsets)
        inv, diag = kept[0], kept[1]
        g2 = jnp.where(inv > 0.0, gathered(s, r, far), 0.0)
        e = inv * g2
        for sweep in range(SWEEPS - 1):
            e = e + inv * (g2 - diag * e + box(e))
        second()
        reach = (width + 1) // 2
        nq = qx + 2 * reach
        zero = jnp.zeros_like(e[:1])
        e = jnp.concatenate([e[xs.index(x)][None] if x in xs else zero for x in range(-reach, qx + reach)], 0)
        e = pltpu.roll(e, my - 2, 1)[:, :my // 2].reshape(nq * my // 2, bz)
        u = pick(e, up_c)
        um[pl.ds(0, nq * my // 2, stride=2), :] = u
        um[pl.ds(1, nq * my // 2, stride=2), :] = u
        u = um[:nq * my, :].reshape(nq, my, bz)
        span = width + 1
        mx = ox + 2 * span
        u = jnp.concatenate([u[(m - span) // 2 + reach][None] for m in range(mx)], 0)
        skip1 = RIM - span
        inv, diag = mid[0, skip1:skip1 + mx], mid[1, skip1:skip1 + mx]
        g1 = jnp.where(inv > 0.0, middle(s, r, span), 0.0)
        f = inv * g1 + u
        f = f + inv * (g1 - diag * f + box(f))
        nm = mx - 2
        f = f[1:mx - 1].reshape(nm * my, bz)
        for pf, up in ((pf0, up_a), (pf1, up_b)):
            w = pick(f, up)
            pf[pl.ds(0, nm * my, stride=2), :] = w
            pf[pl.ds(1, nm * my, stride=2), :] = w

        def e1(i):
            m = (i - WIDTH) // 2 + width
            a, b = e0(i)
            return a + pf0[m * ey:(m + 1) * ey, :], b + pf1[m * ey:(m + 1) * ey, :]

        wide = width > 1
        past = INNER + 1 if wide else 1
        at1, result1 = boxes(e1, WIDTH - past, WIDTH + bx + past)

        def e2(i):
            return [w27[t, i] * a + e + d[t, i] * s_ for t, (a, e, s_) in enumerate(zip(at1(i), e0(i), result1(i)))]

        at2, result2 = boxes(e2, WIDTH - past + 1, WIDTH + bx + past - 1, wide)
        for i in range(WIDTH - past + 1, WIDTH + bx + past - 1):
            a, b = at2(i)
            sa, sb = result2(i)
            finish(i, a, k27[0, i] * a - sa, k27[1, i] * b - sb if wide else None)

    gamma, delta = [], []

    def own(i):
        return WIDTH <= i < WIDTH + bx

    def finish1(i, e, out, out_b):
        im0[0, i] = out
        im0[1, i] = out_b
        if own(i):
            e, out = e[EDGE:EDGE + by], out[EDGE:EDGE + by]
            pre_ref[i - WIDTH] = e
            img_ref[i - WIDTH] = out
            gamma.append(g_ref[i - WIDTH] * e)
            delta.append(out * e)
        if i == WIDTH + bx - 1:
            gs = jnp.sum(total_of(gamma), axis=0, keepdims=True)
            ds = jnp.sum(total_of(delta), axis=0, keepdims=True)
            gs, ds = gs + pltpu.roll(gs, half, 1), ds + pltpu.roll(ds, half, 1)
            sum_begin(0, jnp.where(lane8[:1] < half, gs, ds))

    nothing = lambda: None
    cycle(3, lambda i: (gc0[0, i], t1[0, i]), near0, near1, s1, r1, make_b, near, ky, RIM - 1, coefficients, nothing, finish1)

    def relay(stage):
        if len(groups) > 1:
            sum_begin(stage, sum_end(stage - 1))

    def finish2(i, e, out, out_b):
        twice_ref[i - WIDTH] = e[EDGE:EDGE + by]
        image_twice_ref[i - WIDTH] = out[EDGE:EDGE + by]

    skip1 = RIM - 1
    cycle(4, lambda i: (im0[0, i], im0[1, i]), mid[0, skip1:skip1 + lx], mid[1, skip1:skip1 + lx], s2, r2, make_d, later, 1, 1,
          lambda: relay(1), lambda: relay(2), finish2)

    total = sum_end(len(groups) - 1)
    gs = jnp.sum(jnp.where(lane8[:1] < half, total, 0.0), axis=1, keepdims=True)
    ds = jnp.sum(jnp.where(lane8[:1] < half, 0.0, total), axis=1, keepdims=True)
    alpha_ref[...] = jnp.broadcast_to(gs / ds, (1, bz)).reshape(alpha_ref.shape)
    leave([(fine_copy, close), (outer_copy, sides), (relay_copy, near), (make_b, near), (make_d, later)])
    for stage in range(len(groups)):
        some = red_r.at[pl.ds(base[stage], len(mates[stage]))]
        pltpu.make_async_copy(some, some, lssem.at[stage]).wait()


def solution(mesh):
    counts = tuple(mesh.shape[a] for a in AXES)

    def shards(right_side, coefficient):
        bx, by, bz = block = right_side.shape
        assert SPAN <= bx and SPAN * bx <= bz and by == 16 and bx % 4 == 0
        kx = max(1, min(-(-PART // (bx // 4)), counts[0] - 1))
        ky = max(1, min(-(-PART // (by // 4)), counts[1] - 1))
        ex, ey = bx + SPAN, by + 2 * EDGE
        ox, my = bx // 2, ey // 2
        qx = bx // 4
        mx = ox + 2 * RIM
        most = (2 * kx + 1) * (2 * ky + 1) * 3
        planes = len([x for x in range(-PART, qx + PART) if -kx * qx <= x < (kx + 1) * qx])
        mates = [len(partners(counts, group)) for group in stages(counts)]
        f32 = jnp.float32
        vmem = pl.BlockSpec(memory_space=pltpu.VMEM)
        messages = [pltpu.VMEM((5, 8, bz), f32)] * 3
        messages += [pltpu.VMEM((2 * kx + 1, 2 * ky + 1, 3, 5, 8, bz), f32)] * 3
        precond, image, twice, image_twice, alpha, g = pl.pallas_call(
            functools.partial(kernel, counts, block, kx, ky),
            out_shape=[pltpu.VMEM(block, f32)] * 4 + [pltpu.VMEM((1, 1, bz), f32), pltpu.VMEM(block, f32)],
            in_specs=[pl.BlockSpec(memory_space=pltpu.HBM)] * 2,
            out_specs=[vmem] * 6,
            scratch_shapes=[
                pltpu.VMEM((2, ex, ey, bz), f32),
                pltpu.VMEM((2, ex, ey, bz), f32),
                pltpu.VMEM((2, by, bz), f32),
                pltpu.VMEM((2, by, bz), f32),
                pltpu.VMEM((2, 2, ey, bz), f32),
                pltpu.VMEM((2, 2, ey, bz), f32),
                pltpu.VMEM((2, ex, ey, bz), f32),
                *[pltpu.VMEM((2, ex, ey, bz), f32)] * 3,
                pltpu.VMEM((2, ex, ey + 2 * EDGE, bz), f32),
                pltpu.VMEM(((ox + 2) * ey, bz), f32),
                pltpu.VMEM(((ox + 2) * ey, bz), f32),
                pltpu.VMEM(((mx - 2) * ey, bz), f32),
                pltpu.VMEM(((mx - 2) * ey, bz), f32),
                pltpu.VMEM((qx * my, bz), f32),
                pltpu.VMEM(((qx + 4) * my, bz), f32),
                *messages,
                pltpu.VMEM((2, planes, my, bz), f32),
                pltpu.VMEM((2, mx, my, bz), f32),
                pltpu.VMEM((len(mates), 1, bz), f32),
                pltpu.VMEM((sum(mates), 1, bz), f32),
                pltpu.VMEM((128 * most, 1, bz), f32),
                pltpu.SemaphoreType.DMA((2,)),
                pltpu.SemaphoreType.DMA,
                pltpu.SemaphoreType.DMA((6,)),
                pltpu.SemaphoreType.DMA((len(mates),)),
                pltpu.SemaphoreType.DMA((len(mates),)),
            ],
            compiler_params=pltpu.CompilerParams(collective_id=0, has_side_effects=True),
            name="relayed",
        )(right_side, coefficient)
        return (alpha * precond, g - alpha * image,
                precond - alpha * twice, image - alpha * image_twice)

    placed = (P(*AXES), P(*AXES))
    return jax.shard_map(
        shards, mesh=mesh, in_specs=placed, out_specs=(P(*AXES),) * 4, check_vma=False
    )
```

```python
import functools
import itertools

import jax
import jax.numpy as jnp
from jax import lax
from jax.experimental import pallas as pl
from jax.experimental.pallas import tpu as pltpu
from jax.sharding import PartitionSpec as P

SWEEPS = 4
relaxation = 0.6

AXES = ("gx", "gy", "gz")
MESH = pl.DeviceIdType.MESH
WIDTH = 5
INNER = 3
EDGE = 8
SPAN = 2 * WIDTH
RIM = 4
PART = SWEEPS + 1


def pick(values, lanes):
    flat = values.reshape(-1, values.shape[-1])
    lanes = jnp.broadcast_to(lanes[:1], flat.shape)
    return jnp.take_along_axis(flat, lanes, axis=1).reshape(values.shape)


def iota(shape, dim):
    return lax.broadcasted_iota(jnp.int32, shape, dim)


def total_of(values):
    while len(values) > 1:
        values = [a + b for a, b in zip(values[::2], values[1::2])] + values[len(values) & ~1:]
    return values[0]


def stages(counts):
    if max(counts) <= RIM:
        return [(0, 1, 2)]
    return [(2,), (1,), (0,)]


def partners(counts, group):
    steps = [(0, 0, 0)]
    for axis in group:
        steps = [s[:axis] + (k,) + s[axis + 1:] for s in steps for k in range(counts[axis])]
    return [s for s in steps if s != (0, 0, 0)]


def kernel(counts, block, kx, ky, g_hbm, c_hbm, pre_ref, img_ref, twice_ref, image_twice_ref, alpha_ref, g_ref,
           gc0, im0, pk, pkx, zr, zrx, t1, d, k27, w27, ys, xr0, xr1, pf0, pf1, xm, um,
           s0, s1, s2, r0, r1, r2, kept, mid, red_s, red_r, units, insem, ssem, rsem, lssem, lrsem):
    bx, by, bz = block
    me = [lax.axis_index(a) for a in AXES]
    ex, ey = bx + SPAN, by + 2 * EDGE
    ox, my = bx // 2, ey // 2
    qx, qy = bx // 4, by // 4
    half, quarter = bz // 2, bz // 4
    lane = iota((ey, bz), 1)
    row = iota((ey, bz), 0)
    lane8 = iota((8, bz), 1)
    row8 = iota((8, bz), 0)

    def valid(offset):
        ok = None
        for axis, step in enumerate(offset):
            if step == 0:
                continue
            place = me[axis] + step
            term = place >= 0 if step < 0 else place < counts[axis]
            ok = term if ok is None else jnp.logical_and(ok, term)
        return ok

    def target(offset):
        return tuple(m + s for m, s in zip(me, offset))

    near = [(dx, dy, dz) for dx in range(-kx, kx + 1) for dy in range(-ky, ky + 1) for dz in (-1, 0, 1)]
    near = [o for o in near if o != (0, 0, 0) and all(counts[a] > abs(o[a]) for a in range(3))]
    near.sort(key=lambda o: -sum(map(abs, o)))
    close = [o for o in near if abs(o[0]) <= 1 and abs(o[1]) <= 1]
    sides = [o for o in close if o[0] != 0 and o[2] == 0]
    later = [o for o in near if abs(o[1]) <= 1]

    groups = stages(counts)
    mates = []
    base = [0]
    for group in groups:
        mates.append(partners(counts, group))
        base.append(base[-1] + len(mates[-1]))

    def mate(step):
        return tuple(lax.rem(m + s, n) if s else m for m, s, n in zip(me, step, counts))

    inside0 = gc0.at[:, pl.ds(WIDTH, bx), pl.ds(EDGE, by), :]
    copies = [pltpu.make_async_copy(src, inside0.at[n], insem.at[n]) for n, src in enumerate((g_hbm, c_hbm))]
    for copy in copies:
        copy.start()
    greet = [o for o in near if abs(o[1]) <= 1 and (abs(o[0]) <= 1 or o[1] == o[2] == 0)]
    barrier = pltpu.get_barrier_semaphore()
    for offset in greet:
        @pl.when(valid(offset))
        def _(offset=offset):
            pl.semaphore_signal(barrier, inc=1, device_id=target(offset), device_id_type=MESH)
    greeted = 0
    if len(groups) > 1:
        for steps in mates:
            for step in steps:
                pl.semaphore_signal(barrier, inc=1, device_id=mate(step), device_id_type=MESH)
            greeted = greeted + len(steps)

    def options(axis, step):
        if counts[axis] <= step:
            return 0
        return (me[axis] >= step).astype(jnp.int32) + (me[axis] + step < counts[axis]).astype(jnp.int32)

    around = (1 + options(0, 1)) * (1 + options(1, 1)) * (1 + options(2, 1)) - 1
    greeted = greeted + around + sum(options(0, step) for step in range(2, kx + 1))

    def clear(ref):
        ref[...] = jnp.zeros(ref.shape, jnp.float32)

    for axis, edges in enumerate((
            [[gc0.at[:, pl.ds(0, WIDTH)], zrx.at[:, 0]], [gc0.at[:, pl.ds(WIDTH + bx, WIDTH)], zrx.at[:, 1]]],
            [[ref.at[..., pl.ds(at, WIDTH), :] for ref in (gc0, zr, zrx)] for at in (EDGE - WIDTH, EDGE + by)],
            [[ref.at[side] for ref in (zr, zrx)] for side in range(2)])):
        for refs, edge in zip(edges, (0, counts[axis] - 1)):
            @pl.when(me[axis] == edge)
            def _(refs=refs):
                for ref in refs:
                    clear(ref)

    for ref in (gc0, zr, zrx):
        clear(ref.at[..., pl.ds(0, EDGE - WIDTH), :])
        clear(ref.at[..., pl.ds(ey - EDGE + WIDTH, EDGE - WIDTH), :])
    for at in (0, EDGE + ey):
        ys[:, :, at:at + EDGE, :] = jnp.zeros((2, ex, EDGE, bz), jnp.float32)

    def row_ends(dy):
        if dy == 0:
            return 0, by, EDGE
        if dy > 0:
            return by - WIDTH, WIDTH, EDGE - WIDTH
        return 0, WIDTH, EDGE + by

    def remote(src, dst, phase, offset):
        pltpu.make_async_remote_copy(
            src_ref=src, dst_ref=dst, send_sem=ssem, recv_sem=rsem.at[phase],
            device_id=target(offset), device_id_type=MESH).start()

    def planes_copy(phase, offset, first, size):
        dx, dy, dz = offset
        start, rows, goes = row_ends(dy)
        if dx == 0:
            px, tx, size = WIDTH, WIDTH, bx
        elif dx > 0:
            px, tx = WIDTH + bx - first - size, WIDTH - first - size
        else:
            px, tx = WIDTH + first, WIDTH + bx + first
        src = gc0.at[:, pl.ds(px, size), pl.ds(EDGE + start, rows), :]
        dst = gc0.at[:, pl.ds(tx, size), pl.ds(goes, rows), :]
        return (src, dst, phase, offset)

    def fine_copy(offset):
        dx, dy, dz = offset
        if dz == 0:
            return planes_copy(0, offset, 0, INNER)
        start, rows, goes = row_ends(dy)
        side = 0 if dz > 0 else 1
        if dx == 0:
            src = pk.at[:, pl.ds(start, rows), :]
            dst = zr.at[side, :, pl.ds(goes, rows), :]
        else:
            end = 0 if dx > 0 else 1
            src = pkx.at[end, pl.ds(start, rows), :]
            dst = zrx.at[side, end, pl.ds(goes, rows), :]
        return (src, dst, 0, offset)

    def outer_copy(offset):
        return planes_copy(1, offset, INNER, WIDTH - INNER)

    def part(offset, depth):
        dx, dy, dz = offset
        if abs(dx) > 1 or abs(dy) > 1:
            return 0, 1
        if dz != 0:
            return 4, 1
        if dx == 0:
            return 0, 4
        if dx < 0:
            return 0, 1 + depth
        return 4 - depth, 1 + depth

    def coarse_copy(phase, offset, s, r, depth):
        dx, dy, dz = offset
        at, size = part(offset, depth)
        return (s.at[pl.ds(at, size)], r.at[kx - dx, ky - dy, 1 - dz, pl.ds(at, size)], phase, offset)

    def tiles(make, offset):
        size = 1
        for n in make(offset)[0].shape:
            size *= n
        assert size % bz == 0
        return size // bz

    def begin(make, offsets):
        for offset in offsets:
            @pl.when(valid(offset))
            def _(offset=offset):
                remote(*make(offset))

    def wait_for(sem, pairs):
        sizes = {}
        for make, offsets in pairs:
            for offset in offsets:
                key = tuple(map(abs, offset))
                sizes.setdefault(key, 0)
                if offset == key:
                    sizes[key] += tiles(make, offset)

        def amount(options):
            total = 0
            for (a, b, c), size in sizes.items():
                total = total + size * options[0][a] * options[1][b] * options[2][c]
            return total

        def number(place, count, step):
            return 1 if step == 0 else (place >= step) * 1 + (place + step < count) * 1

        def table(axis, place):
            return [number(place, counts[axis], k) for k in range(3)]

        here = []
        for axis in range(3):
            has = [1]
            for k in (1, 2):
                n = (me[axis] >= k).astype(jnp.int32) + (me[axis] + k < counts[axis]).astype(jnp.int32)
                has.append(n)
            here.append(has)
        total = amount(here)
        for value in sorted({amount(options) for options in itertools.product(
                *[[table(axis, place) for place in range(counts[axis])] for axis in range(3)])}):
            @pl.when(total == value)
            def _(value=value):
                some = units.at[pl.ds(0, value)]
                pltpu.make_async_copy(some, some, sem).wait()

    def arrive(phase, make, offsets):
        wait_for(rsem.at[phase], [(make, offsets)])

    def leave(pairs):
        wait_for(ssem, pairs)

    def mate_copy(stage, k):
        n = base[stage] + k
        return pltpu.make_async_remote_copy(
            src_ref=red_s.at[stage], dst_ref=red_r.at[n], send_sem=lssem.at[stage],
            recv_sem=lrsem.at[stage], device_id=mate(mates[stage][k]), device_id_type=MESH)

    def sum_begin(stage, value):
        red_s[stage] = value
        for k in range(len(mates[stage])):
            mate_copy(stage, k).start()

    def sum_end(stage):
        some = red_r.at[pl.ds(base[stage], len(mates[stage]))]
        pltpu.make_async_copy(some, some, lrsem.at[stage]).wait()
        return total_of([red_s[stage]] + [red_r[base[stage] + k] for k in range(len(mates[stage]))])

    strip = (lane[:by] < WIDTH) | (lane[:by] >= bz - WIDTH)
    place = lax.rem(lane + WIDTH, bz)
    low = lax.rem(place, SPAN) < WIDTH
    band = (lane < WIDTH) | (lane >= bz - WIDTH)
    first, last = lane == 0, lane == bz - 1

    def turn_to(v, shift):
        shift = shift % bz
        return v if shift == 0 else pltpu.roll(v, shift, 1)

    def pack(planes):
        pieces = [turn_to(jnp.where(strip, plane, 0.0), SPAN * i) for i, plane in enumerate(planes)]
        ends = (total_of(pieces[bx - WIDTH:]), total_of(pieces[:WIDTH]))
        return ends, total_of(pieces[WIDTH:bx - WIDTH] + list(ends))

    def lines(v, wide):
        a, b = v
        la, ra = pltpu.roll(a, 1, 1), pltpu.roll(a, bz - 1, 1)
        lb, rb = pltpu.roll(b, 1, 1), pltpu.roll(b, bz - 1, 1)
        sa = a + jnp.where(first, lb, la) + jnp.where(last, rb, ra)
        return sa, b + jnp.where(first, la, lb) + jnp.where(last, ra, rb) if wide else None

    def boxes(value, start, stop, wide=True):
        held, pairs = {}, {}

        def at(i):
            if i not in held:
                held[i] = value(i)
            return held[i]

        def pair(i):
            if i not in pairs:
                pairs[i] = [p + q for p, q in zip(at(i), at(i + 1))]
            return pairs[i]

        def result(i):
            if (i - start) % 2 == 0:
                around = [p + q for p, q in zip(at(i - 1), pair(i))]
            else:
                around = [p + q for p, q in zip(pair(i - 1), at(i + 1))]
            total = []
            for t in range(2):
                ys[t, i, EDGE:EDGE + ey, :] = around[t]
                total.append(around[t] + ys[t, i, EDGE - 1:EDGE - 1 + ey, :] + ys[t, i, EDGE + 1:EDGE + 1 + ey, :])
            return lines(total, wide)

        return at, result

    def box(v):
        s = v + pltpu.roll(v, 1, 2) + pltpu.roll(v, v.shape[2] - 1, 2)
        s = s + pltpu.roll(s, 1, 1) + pltpu.roll(s, v.shape[1] - 1, 1)
        zero = jnp.zeros_like(s[:1])
        return s + jnp.concatenate([zero, s[:-1]], 0) + jnp.concatenate([s[1:], zero], 0)

    down = (2 * lane8) % bz
    down_c = (2 * lane8) % half
    up_a = lane8 >> 1
    up_b = (lane8 + bz) >> 1
    up_c = jnp.where(lane8 < 3 * quarter, lane8 >> 1, (lane8 >> 1) + half)

    def paired(v):
        return v + pltpu.roll(v, bz - 1, v.ndim - 1)

    lx = ox + 2

    def restricted(of):
        for m in range(lx):
            a0, b0 = of(2 * m + INNER)
            a1, b1 = of(2 * m + INNER + 1)
            xr0[m * ey:(m + 1) * ey, :] = a0 + a1
            xr1[m * ey:(m + 1) * ey, :] = b0 + b1
        n = lx * my
        a = xr0[pl.ds(0, n, stride=2), :] + xr0[pl.ds(1, n, stride=2), :]
        b = xr1[pl.ds(0, n, stride=2), :] + xr1[pl.ds(1, n, stride=2), :]
        a, b = pick(paired(0.5 * a), down), pick(paired(0.5 * b), down)
        return jnp.where(iota(a.shape, 1) < half, a, b).reshape(lx, my, bz)

    turn = lane8 // quarter

    def coarsened(v):
        for m in range(qx):
            xm[m * my:(m + 1) * my, :] = v[2 * m] + v[2 * m + 1]
        n = qx * my // 2
        a = xm[pl.ds(0, n, stride=2), :] + xm[pl.ds(1, n, stride=2), :]
        a = pick(paired(0.5 * a), down_c)
        rows = my // 2
        tile = a[:rows]
        for m in range(1, qx):
            tile = jnp.where(turn == m, a[m * rows:(m + 1) * rows], tile)
        return pltpu.roll(tile, rows - 2, 0)

    rim = (lane8 < RIM) | ((lane8 >= half - RIM) & (lane8 < half))
    edge1 = my // 2 - by // 4
    here_ends = (lane8 < RIM * ox) | ((lane8 >= half - RIM) & (lane8 < half - RIM + RIM * ox))

    def post(s, v1, tile):
        own = [v1[p][edge1:edge1 + by // 2] for p in range(ox)]
        ends = total_of([turn_to(jnp.where(rim, own[p], 0.0), RIM * p) for p in range(ox)])
        ends = jnp.where(here_ends, ends, pltpu.roll(turn_to(ends, RIM * ox), 4, 0))
        tile = jnp.where(row8 < qy, tile, ends)
        s[0] = tile
        for k in range(ox // 2):
            s[1 + k] = jnp.where(lane8 < half, own[2 * k], pltpu.roll(own[2 * k + 1], half, 1))
        s[4] = tile

    def middle(s, r, width):
        depth = RIM // 2 if width > 2 else 1

        def get(dx, dy, dz, k):
            if (dx, dy, dz) == (0, 0, 0):
                return s[k]
            if any(abs(d) >= n for d, n in zip((dx, dy, dz), counts)):
                return jnp.zeros((8, bz), jnp.float32)
            return r[kx + dx, ky + dy, 1 + dz, k]

        def rows(tiles):
            before, here, after = tiles
            return (pltpu.roll(jnp.where(row8 >= 4, before, here), 4, 0),
                    pltpu.roll(jnp.where(row8 >= 4, here, after), 4, 0))

        planes = []
        for dx in (-1, 0, 1):
            tiles = range(ox // 2 - depth, ox // 2) if dx < 0 else range(depth) if dx > 0 else range(ox // 2)
            ends = [jnp.where(lane8 < 2 * RIM * ox + RIM, get(dx, dy, 1, 4), get(dx, dy, -1, 4)) for dy in (-1, 0, 1)]
            ends = [jnp.where(row8 < 4, pltpu.roll(ends[k], 4, 0), turn_to(ends[k + 1], -RIM * ox)) for k in range(2)]
            for k in tiles:
                pair = rows([get(dx, dy, 0, 1 + k) for dy in (-1, 0, 1)])
                for odd in (0, 1):
                    p = 2 * k + odd
                    planes.append(jnp.concatenate([
                        jnp.where(lane8 < half, pltpu.roll(t, half, 1) if odd else t, turn_to(e, half - RIM * p))
                        for t, e in zip(pair, ends)], 0))
        return jnp.stack(planes)

    xs = [x for x in range(-PART, qx + PART) if -kx * qx <= x < (kx + 1) * qx]

    def gathered(s, r, far):
        zero = jnp.zeros((8, bz), jnp.float32)

        def get(dx, dy, dz):
            if (dx, dy, dz) == (0, 0, 0):
                return s[0]
            if any(abs(d) >= n for d, n in zip((dx, dy, dz), counts)) or abs(dy) > far:
                return zero
            return r[kx + dx, ky + dy, 1 + dz, part((-dx, -dy, -dz), 0)[0]]

        columns = {}
        for dx in sorted({x // qx for x in xs}):
            for dy in range(-2, 3):
                if abs(dy) > far:
                    continue
                here = get(dx, dy, 0)
                after = pltpu.roll(get(dx, dy, 1), quarter, 1)
                before = pltpu.roll(get(dx, dy, -1), 3 * quarter, 1)
                for m in range(qx):
                    tile = jnp.where(turn == (m + 1) % 4, after, here)
                    tile = jnp.where(turn == (m + 3) % 4, before, tile)
                    columns[dx * qx + m, dy] = turn_to(tile, -quarter * m)
        planes = []
        for x in xs:
            t = {dy: columns.get((x, dy), zero) for dy in range(-2, 3)}
            upper = jnp.where(row8 < qy, t[-1], pltpu.roll(t[0], 4, 0))
            if far > 1:
                lower = jnp.where(row8 < qy, t[1], pltpu.roll(jnp.where(row8 < 2, t[2], t[-2]), 4, 0))
            else:
                lower = jnp.where(row8 < qy, t[1], 0.0)
            planes.append(jnp.concatenate([upper, lower], 0))
        return jnp.stack(planes)

    def within(place, axis, size):
        place = place + me[axis] * size
        return (place >= 0) & (place < counts[axis] * size)

    for copy in copies:
        copy.wait()
    g, c = ([gc0[n, WIDTH + i, EDGE:EDGE + by, :] for i in range(bx)] for n in range(2))
    for i in range(bx):
        g_ref[i] = g[i]
    (g_last, g_first), pk[0] = pack(g)
    (c_last, c_first), pk[1] = pack(c)
    pkx[0] = g_last + turn_to(c_last, -SPAN * WIDTH)
    pkx[1] = g_first + turn_to(c_first, SPAN * WIDTH)

    for m in range(ox):
        xr0[m * ey + EDGE:m * ey + EDGE + by, :] = c[2 * m] + c[2 * m + 1]
    n = ox * my
    own1 = xr0[pl.ds(0, n, stride=2), :] + xr0[pl.ds(1, n, stride=2), :]
    own1 = pick(paired(0.5 * own1), down).reshape(ox, my, bz)
    post(s0, own1, coarsened(own1))

    def relay_copy(offset):
        dx, dy, dz = offset
        if (dy, dz) == (0, 0):
            return coarse_copy(2, offset, s0, r0, RIM // 2)
        far = abs(dx) > 1 or abs(dy) > 1
        at, size = part((-dx, 0, 0), RIM // 2)
        if far or dz != 0:
            at, size = 4 if dx == -1 else 0, 1
        src = s0.at[pl.ds(at, size)] if dx == 0 else r0.at[kx + dx, ky, 1, pl.ds(at, size)]
        goes = 0 if far else 4 if dz != 0 else at
        return src, r0.at[kx + dx, ky - dy, 1 - dz, pl.ds(goes, size)], 5, (0, dy, dz)

    along_x = [o for o in near if o[1] == o[2] == 0]
    onwards = [o for o in near if o not in along_x]
    make_b = lambda o: coarse_copy(3, o, s1, r1, RIM // 2)
    make_d = lambda o: coarse_copy(4, o, s2, r2, 1)
    pl.semaphore_wait(barrier, greeted)
    begin(relay_copy, along_x)
    begin(fine_copy, close)

    in_y = within(row - EDGE, 1, by)

    def factors(t, i, rows, c, inverse):
        d[t, i, rows], k27[t, i, rows] = inverse, 27.0 + c
        w27[t, i, rows] = 1.0 - inverse * (27.0 + c)

    def spread(i):
        if own(i):
            shifts = [SPAN * (i - WIDTH)] * 2
            packs, scale = merged, 0
        elif i < WIDTH:
            shifts = [SPAN * (bx - WIDTH + i), SPAN * (bx - WIDTH + i - WIDTH)]
            packs, scale = [ends[0]] * 2, 1
        else:
            shifts = [SPAN * (i - WIDTH - bx), SPAN * (i - bx)]
            packs, scale = [ends[1]] * 2, 2
        t1[0, i] = turn_to(packs[0], -shifts[0])
        cb = t1[1, i] = turn_to(packs[1], -shifts[1])
        factors(1, i, slice(None), cb, scales_b[scale] / (26.0 + cb))
        for at, size in ((0, EDGE), (EDGE + by, EDGE)) if own(i) else ((0, ey),):
            rows = slice(at, at + size)
            c = gc0[1, i, rows]
            factors(0, i, rows, c, scales_a[scale][rows] / (26.0 + c))

    def own(i):
        return WIDTH <= i < WIDTH + bx

    def kept_if(ok):
        return jnp.where(ok, relaxation, 0.0)

    in_x = [True, me[0] > 0, me[0] + 1 < counts[0]]
    in_z = jnp.where(lane < half, jnp.full((ey, bz), kept_if(me[2] + 1 < counts[2]), jnp.float32),
                     jnp.full((ey, bz), kept_if(me[2] > 0), jnp.float32))
    scales_a = [jnp.where(in_y, kept_if(ok), 0.0) for ok in in_x]
    scales_b = [jnp.where(in_y & band & ok, in_z, 0.0) for ok in in_x]
    for i in range(bx):
        factors(0, WIDTH + i, slice(EDGE, EDGE + by), c[i], relaxation / (26.0 + c[i]))

    arrive(2, relay_copy, along_x)
    begin(relay_copy, [o for o in onwards if abs(o[1]) <= 1])
    begin(outer_copy, sides)
    arrive(0, fine_copy, close)
    begin(relay_copy, [o for o in onwards if abs(o[1]) > 1])
    merged = [jnp.where(low, zr[0, f], zr[1, f]) for f in range(2)]
    ends = [jnp.where(low, zrx[0, e], zrx[1, e]) for e in range(2)]
    skip = WIDTH - INNER
    for i in range(skip, ex - skip):
        spread(i)

    def inside1(shape, width):
        zl = iota(shape, 2)
        zl = jnp.where(zl < 3 * quarter, zl, zl - bz)
        ok = within(iota(shape, 0) - width, 0, ox) & within(iota(shape, 1) - edge1, 1, by // 2)
        return ok & within(zl, 2, half) & (zl >= -RIM) & (zl < half + RIM)

    c1 = restricted(lambda i: (gc0[1, i], t1[1, i]))
    near0 = jnp.where(inside1((lx, my, bz), 1), relaxation / (26.0 + c1), 0.0)
    near1 = 27.0 + c1

    def coefficients():
        arrive(1, outer_copy, sides)
        for i in list(range(skip)) + list(range(ex - skip, ex)):
            spread(i)
        arrive(5, relay_copy, onwards)
        c1 = middle(s0, r0, RIM)
        ok = inside1(c1.shape, RIM)
        c1 = jnp.where(ok, c1, 0.0)
        mid[0] = jnp.where(ok, relaxation / (26.0 + c1), 0.0)
        mid[1] = 27.0 + c1
        c2 = gathered(s0, r0, ky)
        shape = c2.shape
        z = iota(shape, 2)
        z = jnp.where(z < 2 * quarter, z, z - bz)
        y = iota(shape, 1)
        y = jnp.where(y < my - 2, y, y - my) - qy
        ok = within(iota(shape, 0) + xs[0], 0, qx) & within(y, 1, qy)
        ok = ok & within(z, 2, quarter) & (z >= -quarter)
        c2 = jnp.where(ok, c2, 0.0)
        kept[0] = jnp.where(ok, relaxation / (26.0 + c2), 0.0)
        kept[1] = 27.0 + c2

    def cycle(phase, g_at, near0, near1, s, r, make, offsets, far, width, hook, second, finish):
        def e0(i):
            a, b = g_at(i)
            return d[0, i] * a, d[1, i] * b

        start = WIDTH - 2
        at, result = boxes(e0, start, ex - start)

        def remainder(i):
            a, b = g_at(i)
            sa, sb = result(i)
            return w27[0, i] * a + sa, w27[1, i] * b + sb

        g1 = restricted(remainder)
        f = near0 * g1
        post(s, g1[1:1 + ox], coarsened((g1 - near1 * f + box(f))[1:1 + ox]))
        begin(make, offsets)
        hook()
        arrive(phase, make, offsets)
        inv, diag = kept[0], kept[1]
        g2 = jnp.where(inv > 0.0, gathered(s, r, far), 0.0)
        reach = (width + 1) // 2
        e = inv * g2
        lowest = 0
        for sweep in range(SWEEPS - 1):
            left = reach + SWEEPS - 2 - sweep
            keep = [n for n, x in enumerate(xs) if -left <= x < qx + left]
            some = slice(keep[0], keep[-1] + 1)
            part_ = slice(keep[0] - lowest, keep[-1] + 1 - lowest)
            e = e[part_] + inv[some] * (g2[some] - diag[some] * e[part_] + box(e)[part_])
            lowest = keep[0]
        second()
        held = xs[lowest:lowest + e.shape[0]]
        nq = qx + 2 * reach
        zero = jnp.zeros_like(e[:1])
        e = jnp.concatenate([e[held.index(x)][None] if x in held else zero for x in range(-reach, qx + reach)], 0)
        e = pltpu.roll(e, my - 2, 1)[:, :my // 2].reshape(nq * my // 2, bz)
        u = pick(e, up_c)
        um[pl.ds(0, nq * my // 2, stride=2), :] = u
        um[pl.ds(1, nq * my // 2, stride=2), :] = u
        u = um[:nq * my, :].reshape(nq, my, bz)
        span = width + 1
        mx = ox + 2 * span
        u = jnp.concatenate([u[(m - span) // 2 + reach][None] for m in range(mx)], 0)
        skip1 = RIM - span
        inv, diag = mid[0, skip1:skip1 + mx], mid[1, skip1:skip1 + mx]
        g1 = jnp.where(inv > 0.0, middle(s, r, span), 0.0)
        f = inv * g1 + u
        f = f + inv * (g1 - diag * f + box(f))
        nm = mx - 2
        f = f[1:mx - 1].reshape(nm * my, bz)
        for pf, up in ((pf0, up_a), (pf1, up_b)):
            w = pick(f, up)
            pf[pl.ds(0, nm * my, stride=2), :] = w
            pf[pl.ds(1, nm * my, stride=2), :] = w

        def e1(i):
            m = (i - WIDTH) // 2 + width
            a, b = e0(i)
            return a + pf0[m * ey:(m + 1) * ey, :], b + pf1[m * ey:(m + 1) * ey, :]

        wide = width > 1
        past = INNER + 1 if wide else 1
        at1, result1 = boxes(e1, WIDTH - past, WIDTH + bx + past)

        def e2(i):
            return [w27[t, i] * a + e + d[t, i] * s_ for t, (a, e, s_) in enumerate(zip(at1(i), e0(i), result1(i)))]

        at2, result2 = boxes(e2, WIDTH - past + 1, WIDTH + bx + past - 1, wide)
        for i in range(WIDTH - past + 1, WIDTH + bx + past - 1):
            a, b = at2(i)
            sa, sb = result2(i)
            finish(i, a, k27[0, i] * a - sa, k27[1, i] * b - sb if wide else None)

    gamma, delta = [], []

    def finish1(i, e, out, out_b):
        im0[0, i] = out
        im0[1, i] = out_b
        if own(i):
            e, out = e[EDGE:EDGE + by], out[EDGE:EDGE + by]
            pre_ref[i - WIDTH] = e
            img_ref[i - WIDTH] = out
            gamma.append(g_ref[i - WIDTH] * e)
            delta.append(out * e)
        if i == WIDTH + bx - 1:
            gs = jnp.sum(total_of(gamma), axis=0, keepdims=True)
            ds = jnp.sum(total_of(delta), axis=0, keepdims=True)
            gs, ds = gs + pltpu.roll(gs, half, 1), ds + pltpu.roll(ds, half, 1)
            sum_begin(0, jnp.where(lane8[:1] < half, gs, ds))

    nothing = lambda: None
    cycle(3, lambda i: (gc0[0, i], t1[0, i]), near0, near1, s1, r1, make_b, near, ky, RIM - 1, coefficients, nothing, finish1)

    def relay(stage):
        if len(groups) > 1:
            sum_begin(stage, sum_end(stage - 1))

    def finish2(i, e, out, out_b):
        twice_ref[i - WIDTH] = e[EDGE:EDGE + by]
        image_twice_ref[i - WIDTH] = out[EDGE:EDGE + by]

    skip1 = RIM - 1
    cycle(4, lambda i: (im0[0, i], im0[1, i]), mid[0, skip1:skip1 + lx], mid[1, skip1:skip1 + lx], s2, r2, make_d, later, 1, 1,
          lambda: relay(1), lambda: relay(2), finish2)

    total = sum_end(len(groups) - 1)
    gs = jnp.sum(jnp.where(lane8[:1] < half, total, 0.0), axis=1, keepdims=True)
    ds = jnp.sum(jnp.where(lane8[:1] < half, 0.0, total), axis=1, keepdims=True)
    alpha_ref[...] = jnp.broadcast_to(gs / ds, (1, bz)).reshape(alpha_ref.shape)
    leave([(fine_copy, close), (outer_copy, sides), (relay_copy, near), (make_b, near), (make_d, later)])
    for stage in range(len(groups)):
        some = red_r.at[pl.ds(base[stage], len(mates[stage]))]
        pltpu.make_async_copy(some, some, lssem.at[stage]).wait()


def solution(mesh):
    counts = tuple(mesh.shape[a] for a in AXES)

    def shards(right_side, coefficient):
        bx, by, bz = block = right_side.shape
        assert SPAN <= bx and SPAN * bx <= bz and by == 16 and bx % 4 == 0
        kx = max(1, min(-(-PART // (bx // 4)), counts[0] - 1))
        ky = max(1, min(-(-PART // (by // 4)), counts[1] - 1))
        ex, ey = bx + SPAN, by + 2 * EDGE
        ox, my = bx // 2, ey // 2
        qx = bx // 4
        mx = ox + 2 * RIM
        most = (2 * kx + 1) * (2 * ky + 1) * 3
        planes = len([x for x in range(-PART, qx + PART) if -kx * qx <= x < (kx + 1) * qx])
        mates = [len(partners(counts, group)) for group in stages(counts)]
        f32 = jnp.float32
        vmem = pl.BlockSpec(memory_space=pltpu.VMEM)
        messages = [pltpu.VMEM((5, 8, bz), f32)] * 3
        messages += [pltpu.VMEM((2 * kx + 1, 2 * ky + 1, 3, 5, 8, bz), f32)] * 3
        precond, image, twice, image_twice, alpha, g = pl.pallas_call(
            functools.partial(kernel, counts, block, kx, ky),
            out_shape=[pltpu.VMEM(block, f32)] * 4 + [pltpu.VMEM((1, 1, bz), f32), pltpu.VMEM(block, f32)],
            in_specs=[pl.BlockSpec(memory_space=pltpu.HBM)] * 2,
            out_specs=[vmem] * 6,
            scratch_shapes=[
                pltpu.VMEM((2, ex, ey, bz), f32),
                pltpu.VMEM((2, ex, ey, bz), f32),
                pltpu.VMEM((2, by, bz), f32),
                pltpu.VMEM((2, by, bz), f32),
                pltpu.VMEM((2, 2, ey, bz), f32),
                pltpu.VMEM((2, 2, ey, bz), f32),
                pltpu.VMEM((2, ex, ey, bz), f32),
                *[pltpu.VMEM((2, ex, ey, bz), f32)] * 3,
                pltpu.VMEM((2, ex, ey + 2 * EDGE, bz), f32),
                pltpu.VMEM(((ox + 2) * ey, bz), f32),
                pltpu.VMEM(((ox + 2) * ey, bz), f32),
                pltpu.VMEM(((mx - 2) * ey, bz), f32),
                pltpu.VMEM(((mx - 2) * ey, bz), f32),
                pltpu.VMEM((qx * my, bz), f32),
                pltpu.VMEM(((qx + 4) * my, bz), f32),
                *messages,
                pltpu.VMEM((2, planes, my, bz), f32),
                pltpu.VMEM((2, mx, my, bz), f32),
                pltpu.VMEM((len(mates), 1, bz), f32),
                pltpu.VMEM((sum(mates), 1, bz), f32),
                pltpu.VMEM((128 * most, 1, bz), f32),
                pltpu.SemaphoreType.DMA((2,)),
                pltpu.SemaphoreType.DMA,
                pltpu.SemaphoreType.DMA((6,)),
                pltpu.SemaphoreType.DMA((len(mates),)),
                pltpu.SemaphoreType.DMA((len(mates),)),
            ],
            compiler_params=pltpu.CompilerParams(collective_id=0, has_side_effects=True),
            name="relayed",
        )(right_side, coefficient)
        return (alpha * precond, g - alpha * image,
                precond - alpha * twice, image - alpha * image_twice)

    placed = (P(*AXES), P(*AXES))
    return jax.shard_map(
        shards, mesh=mesh, in_specs=placed, out_specs=(P(*AXES),) * 4, check_vma=False
    )
```

```python
import functools
import itertools

import jax
import jax.numpy as jnp
from jax import lax
from jax.experimental import pallas as pl
from jax.experimental.pallas import tpu as pltpu
from jax.sharding import PartitionSpec as P

SWEEPS = 4
relaxation = 0.6

AXES = ("gx", "gy", "gz")
MESH = pl.DeviceIdType.MESH
WIDTH = 5
INNER = 3
EDGE = 8
SPAN = 2 * WIDTH
RIM = 4
PART = SWEEPS + 1


def pick(values, lanes):
    flat = values.reshape(-1, values.shape[-1])
    lanes = jnp.broadcast_to(lanes[:1], flat.shape)
    return jnp.take_along_axis(flat, lanes, axis=1).reshape(values.shape)


def iota(shape, dim):
    return lax.broadcasted_iota(jnp.int32, shape, dim)


def total_of(values):
    while len(values) > 1:
        values = [a + b for a, b in zip(values[::2], values[1::2])] + values[len(values) & ~1:]
    return values[0]


def stages(counts):
    if max(counts) <= RIM:
        return [(0, 1, 2)]
    return [(2,), (1,), (0,)]


def partners(counts, group):
    steps = [(0, 0, 0)]
    for axis in group:
        steps = [s[:axis] + (k,) + s[axis + 1:] for s in steps for k in range(counts[axis])]
    return [s for s in steps if s != (0, 0, 0)]


def kernel(counts, block, kx, ky, g_hbm, c_hbm, pre_ref, img_ref, twice_ref, image_twice_ref, alpha_ref, g_ref,
           gc0, im0, pk, pkx, zr, zrx, t1, d, k27, w27, ys, xr0, xr1, pf0, pf1, xm, um,
           s0, s1, s2, r0, r1, r2, kept, mid, red_s, red_r, units, insem, ssem, rsem, lssem, lrsem):
    bx, by, bz = block
    me = [lax.axis_index(a) for a in AXES]
    ex, ey = bx + SPAN, by + 2 * EDGE
    ox, my = bx // 2, ey // 2
    qx, qy = bx // 4, by // 4
    half, quarter = bz // 2, bz // 4
    lane = iota((ey, bz), 1)
    row = iota((ey, bz), 0)
    lane8 = iota((8, bz), 1)
    row8 = iota((8, bz), 0)

    def valid(offset):
        ok = None
        for axis, step in enumerate(offset):
            if step == 0:
                continue
            place = me[axis] + step
            term = place >= 0 if step < 0 else place < counts[axis]
            ok = term if ok is None else jnp.logical_and(ok, term)
        return ok

    def target(offset):
        return tuple(m + s for m, s in zip(me, offset))

    near = [(dx, dy, dz) for dx in range(-kx, kx + 1) for dy in range(-ky, ky + 1) for dz in (-1, 0, 1)]
    near = [o for o in near if o != (0, 0, 0) and all(counts[a] > abs(o[a]) for a in range(3))]
    near.sort(key=lambda o: -sum(map(abs, o)))
    close = [o for o in near if abs(o[0]) <= 1 and abs(o[1]) <= 1]
    sides = [o for o in close if o[0] != 0 and o[2] == 0]
    later = [o for o in near if abs(o[1]) <= 1]

    groups = stages(counts)
    mates = []
    base = [0]
    for group in groups:
        mates.append(partners(counts, group))
        base.append(base[-1] + len(mates[-1]))

    def mate(step):
        return tuple(lax.rem(m + s, n) if s else m for m, s, n in zip(me, step, counts))

    inside0 = gc0.at[:, pl.ds(WIDTH, bx), pl.ds(EDGE, by), :]
    copies = [pltpu.make_async_copy(src, inside0.at[n], insem.at[n]) for n, src in enumerate((g_hbm, c_hbm))]
    for copy in copies:
        copy.start()
    greet = [o for o in near if abs(o[1]) <= 1 and (abs(o[0]) <= 1 or o[1] == o[2] == 0)]
    barrier = pltpu.get_barrier_semaphore()
    for offset in greet:
        @pl.when(valid(offset))
        def _(offset=offset):
            pl.semaphore_signal(barrier, inc=1, device_id=target(offset), device_id_type=MESH)
    greeted = 0
    if len(groups) > 1:
        for steps in mates:
            for step in steps:
                pl.semaphore_signal(barrier, inc=1, device_id=mate(step), device_id_type=MESH)
            greeted = greeted + len(steps)

    def options(axis, step):
        if counts[axis] <= step:
            return 0
        return (me[axis] >= step).astype(jnp.int32) + (me[axis] + step < counts[axis]).astype(jnp.int32)

    around = (1 + options(0, 1)) * (1 + options(1, 1)) * (1 + options(2, 1)) - 1
    greeted = greeted + around + sum(options(0, step) for step in range(2, kx + 1))

    def clear(ref):
        ref[...] = jnp.zeros(ref.shape, jnp.float32)

    for axis, edges in enumerate((
            [[gc0.at[:, pl.ds(0, WIDTH)], zrx.at[:, 0]], [gc0.at[:, pl.ds(WIDTH + bx, WIDTH)], zrx.at[:, 1]]],
            [[ref.at[..., pl.ds(at, WIDTH), :] for ref in (gc0, zr, zrx)] for at in (EDGE - WIDTH, EDGE + by)],
            [[ref.at[side] for ref in (zr, zrx)] for side in range(2)])):
        for refs, edge in zip(edges, (0, counts[axis] - 1)):
            @pl.when(me[axis] == edge)
            def _(refs=refs):
                for ref in refs:
                    clear(ref)

    for ref in (gc0, zr, zrx):
        clear(ref.at[..., pl.ds(0, EDGE - WIDTH), :])
        clear(ref.at[..., pl.ds(ey - EDGE + WIDTH, EDGE - WIDTH), :])
    for at in (0, ey):
        ys[:, :, at:at + 2 * EDGE, :] = jnp.zeros((2, ex, 2 * EDGE, bz), jnp.float32)

    def row_ends(dy):
        if dy == 0:
            return 0, by, EDGE
        if dy > 0:
            return by - WIDTH, WIDTH, EDGE - WIDTH
        return 0, WIDTH, EDGE + by

    def remote(src, dst, phase, offset):
        pltpu.make_async_remote_copy(
            src_ref=src, dst_ref=dst, send_sem=ssem, recv_sem=rsem.at[phase],
            device_id=target(offset), device_id_type=MESH).start()

    def planes_copy(phase, offset, first, size):
        dx, dy, dz = offset
        start, rows, goes = row_ends(dy)
        if dx == 0:
            px, tx, size = WIDTH, WIDTH, bx
        elif dx > 0:
            px, tx = WIDTH + bx - first - size, WIDTH - first - size
        else:
            px, tx = WIDTH + first, WIDTH + bx + first
        src = gc0.at[:, pl.ds(px, size), pl.ds(EDGE + start, rows), :]
        dst = gc0.at[:, pl.ds(tx, size), pl.ds(goes, rows), :]
        return (src, dst, phase, offset)

    def fine_copy(offset):
        dx, dy, dz = offset
        if dz == 0:
            return planes_copy(0, offset, 0, INNER)
        start, rows, goes = row_ends(dy)
        side = 0 if dz > 0 else 1
        if dx == 0:
            src = pk.at[:, pl.ds(start, rows), :]
            dst = zr.at[side, :, pl.ds(goes, rows), :]
        else:
            end = 0 if dx > 0 else 1
            src = pkx.at[end, pl.ds(start, rows), :]
            dst = zrx.at[side, end, pl.ds(goes, rows), :]
        return (src, dst, 0, offset)

    def outer_copy(offset):
        return planes_copy(1, offset, INNER, WIDTH - INNER)

    def part(offset, depth):
        dx, dy, dz = offset
        if abs(dx) > 1 or abs(dy) > 1:
            return 0, 1
        if dz != 0:
            return 4, 1
        if dx == 0:
            return 0, 4
        if dx < 0:
            return 0, 1 + depth
        return 4 - depth, 1 + depth

    def coarse_copy(phase, offset, s, r, depth):
        dx, dy, dz = offset
        at, size = part(offset, depth)
        return (s.at[pl.ds(at, size)], r.at[kx - dx, ky - dy, 1 - dz, pl.ds(at, size)], phase, offset)

    def tiles(make, offset):
        size = 1
        for n in make(offset)[0].shape:
            size *= n
        assert size % bz == 0
        return size // bz

    def begin(make, offsets):
        for offset in offsets:
            @pl.when(valid(offset))
            def _(offset=offset):
                remote(*make(offset))

    def wait_for(sem, pairs):
        sizes = {}
        for make, offsets in pairs:
            for offset in offsets:
                key = tuple(map(abs, offset))
                sizes.setdefault(key, 0)
                if offset == key:
                    sizes[key] += tiles(make, offset)

        def amount(options):
            total = 0
            for (a, b, c), size in sizes.items():
                total = total + size * options[0][a] * options[1][b] * options[2][c]
            return total

        def number(place, count, step):
            return 1 if step == 0 else (place >= step) * 1 + (place + step < count) * 1

        def table(axis, place):
            return [number(place, counts[axis], k) for k in range(3)]

        here = []
        for axis in range(3):
            has = [1]
            for k in (1, 2):
                n = (me[axis] >= k).astype(jnp.int32) + (me[axis] + k < counts[axis]).astype(jnp.int32)
                has.append(n)
            here.append(has)
        total = amount(here)
        for value in sorted({amount(options) for options in itertools.product(
                *[[table(axis, place) for place in range(counts[axis])] for axis in range(3)])}):
            @pl.when(total == value)
            def _(value=value):
                some = units.at[pl.ds(0, value)]
                pltpu.make_async_copy(some, some, sem).wait()

    def arrive(phase, make, offsets):
        wait_for(rsem.at[phase], [(make, offsets)])

    def leave(pairs):
        wait_for(ssem, pairs)

    def mate_copy(stage, k):
        n = base[stage] + k
        return pltpu.make_async_remote_copy(
            src_ref=red_s.at[stage], dst_ref=red_r.at[n], send_sem=lssem.at[stage],
            recv_sem=lrsem.at[stage], device_id=mate(mates[stage][k]), device_id_type=MESH)

    def sum_begin(stage, value):
        red_s[stage] = value
        for k in range(len(mates[stage])):
            mate_copy(stage, k).start()

    def sum_end(stage):
        some = red_r.at[pl.ds(base[stage], len(mates[stage]))]
        pltpu.make_async_copy(some, some, lrsem.at[stage]).wait()
        return total_of([red_s[stage]] + [red_r[base[stage] + k] for k in range(len(mates[stage]))])

    strip = (lane[:by] < WIDTH) | (lane[:by] >= bz - WIDTH)
    place = lax.rem(lane + WIDTH, bz)
    low = lax.rem(place, SPAN) < WIDTH
    band = (lane < WIDTH) | (lane >= bz - WIDTH)
    first, last = lane == 0, lane == bz - 1

    def turn_to(v, shift):
        shift = shift % bz
        return v if shift == 0 else pltpu.roll(v, shift, 1)

    def pack(planes):
        pieces = [turn_to(jnp.where(strip, plane, 0.0), SPAN * i) for i, plane in enumerate(planes)]
        ends = (total_of(pieces[bx - WIDTH:]), total_of(pieces[:WIDTH]))
        return ends, total_of(pieces[WIDTH:bx - WIDTH] + list(ends))

    def lines(v, wide):
        a, b = v
        la, ra = pltpu.roll(a, 1, 1), pltpu.roll(a, bz - 1, 1)
        lb, rb = pltpu.roll(b, 1, 1), pltpu.roll(b, bz - 1, 1)
        f, l = first[:a.shape[0]], last[:a.shape[0]]
        sa = a + jnp.where(f, lb, la) + jnp.where(l, rb, ra)
        return sa, b + jnp.where(f, la, lb) + jnp.where(l, ra, rb) if wide else None

    shore = WIDTH - 1
    rows_all, rows_some = slice(0, ey), slice(EDGE - shore, EDGE + by + shore)

    def moved(rows, by_):
        return slice(rows.start + by_, rows.stop + by_)

    def boxes(value, start, stop, wide=True, rows=rows_some):
        held, pairs = {}, {}

        def at(i):
            if i not in held:
                held[i] = value(i)
            return held[i]

        def pair(i):
            if i not in pairs:
                pairs[i] = [p + q for p, q in zip(at(i), at(i + 1))]
            return pairs[i]

        def result(i):
            if (i - start) % 2 == 0:
                around = [p + q for p, q in zip(at(i - 1), pair(i))]
            else:
                around = [p + q for p, q in zip(pair(i - 1), at(i + 1))]
            total = []
            for t in range(2):
                ys[t, i, moved(rows, EDGE), :] = around[t]
                mid_row = around[t] if rows is rows_some else ys[t, i, moved(rows_some, EDGE), :]
                total.append(mid_row + ys[t, i, moved(rows_some, EDGE - 1), :] + ys[t, i, moved(rows_some, EDGE + 1), :])
            return lines(total, wide)

        return at, result

    def box(v):
        s = v + pltpu.roll(v, 1, 2) + pltpu.roll(v, v.shape[2] - 1, 2)
        s = s + pltpu.roll(s, 1, 1) + pltpu.roll(s, v.shape[1] - 1, 1)
        zero = jnp.zeros_like(s[:1])
        return s + jnp.concatenate([zero, s[:-1]], 0) + jnp.concatenate([s[1:], zero], 0)

    down = (2 * lane8) % bz
    down_c = (2 * lane8) % half
    up_a = lane8 >> 1
    up_b = (lane8 + bz) >> 1
    up_c = jnp.where(lane8 < 3 * quarter, lane8 >> 1, (lane8 >> 1) + half)

    def paired(v):
        return v + pltpu.roll(v, bz - 1, v.ndim - 1)

    lx = ox + 2

    def restricted(of):
        for m in range(lx):
            a0, b0 = of(2 * m + INNER)
            a1, b1 = of(2 * m + INNER + 1)
            xr0[moved(rows_some, m * ey), :] = a0 + a1
            xr1[moved(rows_some, m * ey), :] = b0 + b1
        n = lx * my
        a = xr0[pl.ds(0, n, stride=2), :] + xr0[pl.ds(1, n, stride=2), :]
        b = xr1[pl.ds(0, n, stride=2), :] + xr1[pl.ds(1, n, stride=2), :]
        a, b = pick(paired(0.5 * a), down), pick(paired(0.5 * b), down)
        return jnp.where(iota(a.shape, 1) < half, a, b).reshape(lx, my, bz)

    turn = lane8 // quarter

    def coarsened(v):
        for m in range(qx):
            xm[m * my:(m + 1) * my, :] = v[2 * m] + v[2 * m + 1]
        n = qx * my // 2
        a = xm[pl.ds(0, n, stride=2), :] + xm[pl.ds(1, n, stride=2), :]
        a = pick(paired(0.5 * a), down_c)
        rows = my // 2
        tile = a[:rows]
        for m in range(1, qx):
            tile = jnp.where(turn == m, a[m * rows:(m + 1) * rows], tile)
        return pltpu.roll(tile, rows - 2, 0)

    rim = (lane8 < RIM) | ((lane8 >= half - RIM) & (lane8 < half))
    edge1 = my // 2 - by // 4
    here_ends = (lane8 < RIM * ox) | ((lane8 >= half - RIM) & (lane8 < half - RIM + RIM * ox))

    def post(s, v1, tile):
        own = [v1[p][edge1:edge1 + by // 2] for p in range(ox)]
        ends = total_of([turn_to(jnp.where(rim, own[p], 0.0), RIM * p) for p in range(ox)])
        ends = jnp.where(here_ends, ends, pltpu.roll(turn_to(ends, RIM * ox), 4, 0))
        tile = jnp.where(row8 < qy, tile, ends)
        s[0] = tile
        for k in range(ox // 2):
            s[1 + k] = jnp.where(lane8 < half, own[2 * k], pltpu.roll(own[2 * k + 1], half, 1))
        s[4] = tile

    def middle(s, r, width):
        depth = RIM // 2 if width > 2 else 1

        def get(dx, dy, dz, k):
            if (dx, dy, dz) == (0, 0, 0):
                return s[k]
            if any(abs(d) >= n for d, n in zip((dx, dy, dz), counts)):
                return jnp.zeros((8, bz), jnp.float32)
            return r[kx + dx, ky + dy, 1 + dz, k]

        def rows(tiles):
            before, here, after = tiles
            return (pltpu.roll(jnp.where(row8 >= 4, before, here), 4, 0),
                    pltpu.roll(jnp.where(row8 >= 4, here, after), 4, 0))

        planes = []
        for dx in (-1, 0, 1):
            tiles = range(ox // 2 - depth, ox // 2) if dx < 0 else range(depth) if dx > 0 else range(ox // 2)
            ends = [jnp.where(lane8 < 2 * RIM * ox + RIM, get(dx, dy, 1, 4), get(dx, dy, -1, 4)) for dy in (-1, 0, 1)]
            ends = [jnp.where(row8 < 4, pltpu.roll(ends[k], 4, 0), turn_to(ends[k + 1], -RIM * ox)) for k in range(2)]
            for k in tiles:
                pair = rows([get(dx, dy, 0, 1 + k) for dy in (-1, 0, 1)])
                for odd in (0, 1):
                    p = 2 * k + odd
                    planes.append(jnp.concatenate([
                        jnp.where(lane8 < half, pltpu.roll(t, half, 1) if odd else t, turn_to(e, half - RIM * p))
                        for t, e in zip(pair, ends)], 0))
        return jnp.stack(planes)

    xs = [x for x in range(-PART, qx + PART) if -kx * qx <= x < (kx + 1) * qx]

    def gathered(s, r, far):
        zero = jnp.zeros((8, bz), jnp.float32)

        def get(dx, dy, dz):
            if (dx, dy, dz) == (0, 0, 0):
                return s[0]
            if any(abs(d) >= n for d, n in zip((dx, dy, dz), counts)) or abs(dy) > far:
                return zero
            return r[kx + dx, ky + dy, 1 + dz, part((-dx, -dy, -dz), 0)[0]]

        columns = {}
        for dx in sorted({x // qx for x in xs}):
            for dy in range(-2, 3):
                if abs(dy) > far:
                    continue
                here = get(dx, dy, 0)
                after = pltpu.roll(get(dx, dy, 1), quarter, 1)
                before = pltpu.roll(get(dx, dy, -1), 3 * quarter, 1)
                for m in range(qx):
                    tile = jnp.where(turn == (m + 1) % 4, after, here)
                    tile = jnp.where(turn == (m + 3) % 4, before, tile)
                    columns[dx * qx + m, dy] = turn_to(tile, -quarter * m)
        planes = []
        for x in xs:
            t = {dy: columns.get((x, dy), zero) for dy in range(-2, 3)}
            upper = jnp.where(row8 < qy, t[-1], pltpu.roll(t[0], 4, 0))
            if far > 1:
                lower = jnp.where(row8 < qy, t[1], pltpu.roll(jnp.where(row8 < 2, t[2], t[-2]), 4, 0))
            else:
                lower = jnp.where(row8 < qy, t[1], 0.0)
            planes.append(jnp.concatenate([upper, lower], 0))
        return jnp.stack(planes)

    def within(place, axis, size):
        place = place + me[axis] * size
        return (place >= 0) & (place < counts[axis] * size)

    for copy in copies:
        copy.wait()
    g, c = ([gc0[n, WIDTH + i, EDGE:EDGE + by, :] for i in range(bx)] for n in range(2))
    for i in range(bx):
        g_ref[i] = g[i]
    (g_last, g_first), pk[0] = pack(g)
    (c_last, c_first), pk[1] = pack(c)
    pkx[0] = g_last + turn_to(c_last, -SPAN * WIDTH)
    pkx[1] = g_first + turn_to(c_first, SPAN * WIDTH)

    for m in range(ox):
        xr0[m * ey + EDGE:m * ey + EDGE + by, :] = c[2 * m] + c[2 * m + 1]
    n = ox * my
    own1 = xr0[pl.ds(0, n, stride=2), :] + xr0[pl.ds(1, n, stride=2), :]
    own1 = pick(paired(0.5 * own1), down).reshape(ox, my, bz)
    post(s0, own1, coarsened(own1))

    def relay_copy(offset):
        dx, dy, dz = offset
        if (dy, dz) == (0, 0):
            return coarse_copy(2, offset, s0, r0, RIM // 2)
        far = abs(dx) > 1 or abs(dy) > 1
        at, size = part((-dx, 0, 0), RIM // 2)
        if far or dz != 0:
            at, size = 4 if dx == -1 else 0, 1
        src = s0.at[pl.ds(at, size)] if dx == 0 else r0.at[kx + dx, ky, 1, pl.ds(at, size)]
        goes = 0 if far else 4 if dz != 0 else at
        return src, r0.at[kx + dx, ky - dy, 1 - dz, pl.ds(goes, size)], 5, (0, dy, dz)

    along_x = [o for o in near if o[1] == o[2] == 0]
    onwards = [o for o in near if o not in along_x]
    make_b = lambda o: coarse_copy(3, o, s1, r1, RIM // 2)
    make_d = lambda o: coarse_copy(4, o, s2, r2, 1)
    pl.semaphore_wait(barrier, greeted)
    begin(relay_copy, along_x)
    begin(fine_copy, close)

    in_y = within(row - EDGE, 1, by)

    def factors(t, i, rows, c, inverse):
        d[t, i, rows], k27[t, i, rows] = inverse, 27.0 + c
        w27[t, i, rows] = 1.0 - inverse * (27.0 + c)

    def spread(i):
        if own(i):
            shifts = [SPAN * (i - WIDTH)] * 2
            packs, scale = merged, 0
        elif i < WIDTH:
            shifts = [SPAN * (bx - WIDTH + i), SPAN * (bx - WIDTH + i - WIDTH)]
            packs, scale = [ends[0]] * 2, 1
        else:
            shifts = [SPAN * (i - WIDTH - bx), SPAN * (i - bx)]
            packs, scale = [ends[1]] * 2, 2
        t1[0, i] = turn_to(packs[0], -shifts[0])
        cb = t1[1, i] = turn_to(packs[1], -shifts[1])
        factors(1, i, slice(None), cb, scales_b[scale] / (26.0 + cb))
        for at, size in ((0, EDGE), (EDGE + by, EDGE)) if own(i) else ((0, ey),):
            rows = slice(at, at + size)
            c = gc0[1, i, rows]
            factors(0, i, rows, c, scales_a[scale][rows] / (26.0 + c))

    def own(i):
        return WIDTH <= i < WIDTH + bx

    def kept_if(ok):
        return jnp.where(ok, relaxation, 0.0)

    in_x = [True, me[0] > 0, me[0] + 1 < counts[0]]
    in_z = jnp.where(lane < half, jnp.full((ey, bz), kept_if(me[2] + 1 < counts[2]), jnp.float32),
                     jnp.full((ey, bz), kept_if(me[2] > 0), jnp.float32))
    scales_a = [jnp.where(in_y, kept_if(ok), 0.0) for ok in in_x]
    scales_b = [jnp.where(in_y & band & ok, in_z, 0.0) for ok in in_x]
    for i in range(bx):
        factors(0, WIDTH + i, slice(EDGE, EDGE + by), c[i], relaxation / (26.0 + c[i]))

    arrive(2, relay_copy, along_x)
    begin(relay_copy, [o for o in onwards if abs(o[1]) <= 1])
    begin(outer_copy, sides)
    arrive(0, fine_copy, close)
    begin(relay_copy, [o for o in onwards if abs(o[1]) > 1])
    merged = [jnp.where(low, zr[0, f], zr[1, f]) for f in range(2)]
    ends = [jnp.where(low, zrx[0, e], zrx[1, e]) for e in range(2)]
    skip = WIDTH - INNER
    for i in range(skip, ex - skip):
        spread(i)

    def inside1(shape, width):
        zl = iota(shape, 2)
        zl = jnp.where(zl < 3 * quarter, zl, zl - bz)
        ok = within(iota(shape, 0) - width, 0, ox) & within(iota(shape, 1) - edge1, 1, by // 2)
        return ok & within(zl, 2, half) & (zl >= -RIM) & (zl < half + RIM)

    c1 = restricted(lambda i: (gc0[1, i, rows_some], t1[1, i, rows_some]))
    near0 = jnp.where(inside1((lx, my, bz), 1), relaxation / (26.0 + c1), 0.0)
    near1 = 27.0 + c1

    def coefficients():
        arrive(1, outer_copy, sides)
        for i in list(range(skip)) + list(range(ex - skip, ex)):
            spread(i)
        arrive(5, relay_copy, onwards)
        c1 = middle(s0, r0, RIM)
        ok = inside1(c1.shape, RIM)
        c1 = jnp.where(ok, c1, 0.0)
        mid[0] = jnp.where(ok, relaxation / (26.0 + c1), 0.0)
        mid[1] = 27.0 + c1
        c2 = gathered(s0, r0, ky)
        shape = c2.shape
        z = iota(shape, 2)
        z = jnp.where(z < 2 * quarter, z, z - bz)
        y = iota(shape, 1)
        y = jnp.where(y < my - 2, y, y - my) - qy
        ok = within(iota(shape, 0) + xs[0], 0, qx) & within(y, 1, qy)
        ok = ok & within(z, 2, quarter) & (z >= -quarter)
        c2 = jnp.where(ok, c2, 0.0)
        kept[0] = jnp.where(ok, relaxation / (26.0 + c2), 0.0)
        kept[1] = 27.0 + c2

    def cycle(phase, g_at, near0, near1, s, r, make, offsets, far, width, hook, second, finish):
        def e0(i, rows=rows_some):
            a, b = g_at(i, rows)
            return d[0, i, rows] * a, d[1, i, rows] * b

        start = WIDTH - 2
        at, result = boxes(e0, start, ex - start)

        def remainder(i):
            a, b = g_at(i, rows_some)
            sa, sb = result(i)
            return w27[0, i, rows_some] * a + sa, w27[1, i, rows_some] * b + sb

        g1 = restricted(remainder)
        f = near0 * g1
        post(s, g1[1:1 + ox], coarsened((g1 - near1 * f + box(f))[1:1 + ox]))
        begin(make, offsets)
        hook()
        arrive(phase, make, offsets)
        inv, diag = kept[0], kept[1]
        g2 = jnp.where(inv > 0.0, gathered(s, r, far), 0.0)
        reach = (width + 1) // 2
        e = inv * g2
        lowest = 0
        for sweep in range(SWEEPS - 1):
            left = reach + SWEEPS - 2 - sweep
            keep = [n for n, x in enumerate(xs) if -left <= x < qx + left]
            some = slice(keep[0], keep[-1] + 1)
            part_ = slice(keep[0] - lowest, keep[-1] + 1 - lowest)
            e = e[part_] + inv[some] * (g2[some] - diag[some] * e[part_] + box(e)[part_])
            lowest = keep[0]
        second()
        held = xs[lowest:lowest + e.shape[0]]
        nq = qx + 2 * reach
        zero = jnp.zeros_like(e[:1])
        e = jnp.concatenate([e[held.index(x)][None] if x in held else zero for x in range(-reach, qx + reach)], 0)
        e = pltpu.roll(e, my - 2, 1)[:, :my // 2].reshape(nq * my // 2, bz)
        u = pick(e, up_c)
        um[pl.ds(0, nq * my // 2, stride=2), :] = u
        um[pl.ds(1, nq * my // 2, stride=2), :] = u
        u = um[:nq * my, :].reshape(nq, my, bz)
        span = width + 1
        mx = ox + 2 * span
        u = jnp.concatenate([u[(m - span) // 2 + reach][None] for m in range(mx)], 0)
        skip1 = RIM - span
        inv, diag = mid[0, skip1:skip1 + mx], mid[1, skip1:skip1 + mx]
        g1 = jnp.where(inv > 0.0, middle(s, r, span), 0.0)
        f = inv * g1 + u
        f = f + inv * (g1 - diag * f + box(f))
        nm = mx - 2
        f = f[1:mx - 1].reshape(nm * my, bz)
        for pf, up in ((pf0, up_a), (pf1, up_b)):
            w = pick(f, up)
            pf[pl.ds(0, nm * my, stride=2), :] = w
            pf[pl.ds(1, nm * my, stride=2), :] = w

        def e1(i, rows):
            m = (i - WIDTH) // 2 + width
            a, b = e0(i, rows)
            return a + pf0[moved(rows, m * ey), :], b + pf1[moved(rows, m * ey), :]

        wide = width > 1
        past = INNER + 1 if wide else 1
        rows1 = rows_all if wide else rows_some
        at1, result1 = boxes(lambda i: e1(i, rows1), WIDTH - past, WIDTH + bx + past, rows=rows1)

        def e2(i):
            values = e1(i, rows_some) if wide else at1(i)
            return [w27[t, i, rows_some] * a + e + d[t, i, rows_some] * s_
                    for t, (a, e, s_) in enumerate(zip(values, e0(i), result1(i)))]

        at2, result2 = boxes(e2, WIDTH - past + 1, WIDTH + bx + past - 1, wide)
        for i in range(WIDTH - past + 1, WIDTH + bx + past - 1):
            a, b = at2(i)
            sa, sb = result2(i)
            finish(i, a, k27[0, i, rows_some] * a - sa, k27[1, i, rows_some] * b - sb if wide else None)

    gamma, delta = [], []

    def finish1(i, e, out, out_b):
        im0[0, i, rows_some] = out
        im0[1, i, rows_some] = out_b
        if own(i):
            e, out = e[shore:shore + by], im0[0, i, EDGE:EDGE + by]
            pre_ref[i - WIDTH] = e
            img_ref[i - WIDTH] = out
            gamma.append(g_ref[i - WIDTH] * e)
            delta.append(out * e)
        if i == WIDTH + bx - 1:
            gs = jnp.sum(total_of(gamma), axis=0, keepdims=True)
            ds = jnp.sum(total_of(delta), axis=0, keepdims=True)
            gs, ds = gs + pltpu.roll(gs, half, 1), ds + pltpu.roll(ds, half, 1)
            sum_begin(0, jnp.where(lane8[:1] < half, gs, ds))

    nothing = lambda: None
    cycle(3, lambda i, rows: (gc0[0, i, rows], t1[0, i, rows]), near0, near1, s1, r1, make_b, near, ky, RIM - 1, coefficients, nothing, finish1)

    def relay(stage):
        if len(groups) > 1:
            sum_begin(stage, sum_end(stage - 1))

    def finish2(i, e, out, out_b):
        twice_ref[i - WIDTH] = e[shore:shore + by]
        image_twice_ref[i - WIDTH] = out[shore:shore + by]

    skip1 = RIM - 1
    cycle(4, lambda i, rows: (im0[0, i, rows], im0[1, i, rows]), mid[0, skip1:skip1 + lx], mid[1, skip1:skip1 + lx], s2, r2, make_d, later, 1, 1,
          lambda: relay(1), lambda: relay(2), finish2)

    total = sum_end(len(groups) - 1)
    gs = jnp.sum(jnp.where(lane8[:1] < half, total, 0.0), axis=1, keepdims=True)
    ds = jnp.sum(jnp.where(lane8[:1] < half, 0.0, total), axis=1, keepdims=True)
    alpha_ref[...] = jnp.broadcast_to(gs / ds, (1, bz)).reshape(alpha_ref.shape)
    leave([(fine_copy, close), (outer_copy, sides), (relay_copy, near), (make_b, near), (make_d, later)])
    for stage in range(len(groups)):
        some = red_r.at[pl.ds(base[stage], len(mates[stage]))]
        pltpu.make_async_copy(some, some, lssem.at[stage]).wait()


def solution(mesh):
    counts = tuple(mesh.shape[a] for a in AXES)

    def shards(right_side, coefficient):
        bx, by, bz = block = right_side.shape
        assert SPAN <= bx and SPAN * bx <= bz and by == 16 and bx % 4 == 0
        kx = max(1, min(-(-PART // (bx // 4)), counts[0] - 1))
        ky = max(1, min(-(-PART // (by // 4)), counts[1] - 1))
        ex, ey = bx + SPAN, by + 2 * EDGE
        ox, my = bx // 2, ey // 2
        qx = bx // 4
        mx = ox + 2 * RIM
        most = (2 * kx + 1) * (2 * ky + 1) * 3
        planes = len([x for x in range(-PART, qx + PART) if -kx * qx <= x < (kx + 1) * qx])
        mates = [len(partners(counts, group)) for group in stages(counts)]
        f32 = jnp.float32
        vmem = pl.BlockSpec(memory_space=pltpu.VMEM)
        messages = [pltpu.VMEM((5, 8, bz), f32)] * 3
        messages += [pltpu.VMEM((2 * kx + 1, 2 * ky + 1, 3, 5, 8, bz), f32)] * 3
        precond, image, twice, image_twice, alpha, g = pl.pallas_call(
            functools.partial(kernel, counts, block, kx, ky),
            out_shape=[pltpu.VMEM(block, f32)] * 4 + [pltpu.VMEM((1, 1, bz), f32), pltpu.VMEM(block, f32)],
            in_specs=[pl.BlockSpec(memory_space=pltpu.HBM)] * 2,
            out_specs=[vmem] * 6,
            scratch_shapes=[
                pltpu.VMEM((2, ex, ey, bz), f32),
                pltpu.VMEM((2, ex, ey, bz), f32),
                pltpu.VMEM((2, by, bz), f32),
                pltpu.VMEM((2, by, bz), f32),
                pltpu.VMEM((2, 2, ey, bz), f32),
                pltpu.VMEM((2, 2, ey, bz), f32),
                pltpu.VMEM((2, ex, ey, bz), f32),
                *[pltpu.VMEM((2, ex, ey, bz), f32)] * 3,
                pltpu.VMEM((2, ex, ey + 2 * EDGE, bz), f32),
                pltpu.VMEM(((ox + 2) * ey, bz), f32),
                pltpu.VMEM(((ox + 2) * ey, bz), f32),
                pltpu.VMEM(((mx - 2) * ey, bz), f32),
                pltpu.VMEM(((mx - 2) * ey, bz), f32),
                pltpu.VMEM((qx * my, bz), f32),
                pltpu.VMEM(((qx + 4) * my, bz), f32),
                *messages,
                pltpu.VMEM((2, planes, my, bz), f32),
                pltpu.VMEM((2, mx, my, bz), f32),
                pltpu.VMEM((len(mates), 1, bz), f32),
                pltpu.VMEM((sum(mates), 1, bz), f32),
                pltpu.VMEM((128 * most, 1, bz), f32),
                pltpu.SemaphoreType.DMA((2,)),
                pltpu.SemaphoreType.DMA,
                pltpu.SemaphoreType.DMA((6,)),
                pltpu.SemaphoreType.DMA((len(mates),)),
                pltpu.SemaphoreType.DMA((len(mates),)),
            ],
            compiler_params=pltpu.CompilerParams(collective_id=0, has_side_effects=True),
            name="relayed",
        )(right_side, coefficient)
        return (alpha * precond, g - alpha * image,
                precond - alpha * twice, image - alpha * image_twice)

    placed = (P(*AXES), P(*AXES))
    return jax.shard_map(
        shards, mesh=mesh, in_specs=placed, out_specs=(P(*AXES),) * 4, check_vma=False
    )
```

```python
import functools
import itertools

import jax
import jax.numpy as jnp
from jax import lax
from jax.experimental import pallas as pl
from jax.experimental.pallas import tpu as pltpu
from jax.sharding import PartitionSpec as P

SWEEPS = 4
relaxation = 0.6

AXES = ("gx", "gy", "gz")
MESH = pl.DeviceIdType.MESH
WIDTH = 5
INNER = 3
EDGE = 8
SPAN = 2 * WIDTH
RIM = 4
PART = SWEEPS + 1


def pick(values, lanes):
    flat = values.reshape(-1, values.shape[-1])
    lanes = jnp.broadcast_to(lanes[:1], flat.shape)
    return jnp.take_along_axis(flat, lanes, axis=1).reshape(values.shape)


def iota(shape, dim):
    return lax.broadcasted_iota(jnp.int32, shape, dim)


def total_of(values):
    while len(values) > 1:
        values = [a + b for a, b in zip(values[::2], values[1::2])] + values[len(values) & ~1:]
    return values[0]


def stages(counts):
    if max(counts) <= RIM:
        return [(0, 1, 2)]
    return [(2,), (1,), (0,)]


def partners(counts, group):
    steps = [(0, 0, 0)]
    for axis in group:
        steps = [s[:axis] + (k,) + s[axis + 1:] for s in steps for k in range(counts[axis])]
    return [s for s in steps if s != (0, 0, 0)]


def kernel(counts, block, kx, ky, g_hbm, c_hbm, pre_ref, img_ref, twice_ref, image_twice_ref, alpha_ref, g_ref,
           gc0, im0, pk, pkx, zr, zrx, t1, d, k27, w27, ys, xr0, xr1, pf0, pf1, sf0, sf1, se, xm, um,
           s0, s1, s2, r0, r1, r2, kept, mid, red_s, red_r, units, insem, ssem, rsem, lssem, lrsem):
    bx, by, bz = block
    me = [lax.axis_index(a) for a in AXES]
    ex, ey = bx + SPAN, by + 2 * EDGE
    ox, my = bx // 2, ey // 2
    qx, qy = bx // 4, by // 4
    half, quarter = bz // 2, bz // 4
    lane = iota((ey, bz), 1)
    row = iota((ey, bz), 0)
    lane8 = iota((8, bz), 1)
    row8 = iota((8, bz), 0)

    def valid(offset):
        ok = None
        for axis, step in enumerate(offset):
            if step == 0:
                continue
            place = me[axis] + step
            term = place >= 0 if step < 0 else place < counts[axis]
            ok = term if ok is None else jnp.logical_and(ok, term)
        return ok

    def target(offset):
        return tuple(m + s for m, s in zip(me, offset))

    near = [(dx, dy, dz) for dx in range(-kx, kx + 1) for dy in range(-ky, ky + 1) for dz in (-1, 0, 1)]
    near = [o for o in near if o != (0, 0, 0) and all(counts[a] > abs(o[a]) for a in range(3))]
    near.sort(key=lambda o: -sum(map(abs, o)))
    close = [o for o in near if abs(o[0]) <= 1 and abs(o[1]) <= 1]
    sides = [o for o in close if o[0] != 0 and o[2] == 0]
    later = [o for o in near if abs(o[1]) <= 1]

    groups = stages(counts)
    mates = []
    base = [0]
    for group in groups:
        mates.append(partners(counts, group))
        base.append(base[-1] + len(mates[-1]))

    def mate(step):
        return tuple(lax.rem(m + s, n) if s else m for m, s, n in zip(me, step, counts))

    inside0 = gc0.at[:, pl.ds(WIDTH, bx), pl.ds(EDGE, by), :]
    copies = [pltpu.make_async_copy(src, inside0.at[n], insem.at[n]) for n, src in enumerate((g_hbm, c_hbm))]
    for copy in copies:
        copy.start()
    greet = [o for o in near if abs(o[1]) <= 1 and (abs(o[0]) <= 1 or o[1] == o[2] == 0)]
    barrier = pltpu.get_barrier_semaphore()
    for offset in greet:
        @pl.when(valid(offset))
        def _(offset=offset):
            pl.semaphore_signal(barrier, inc=1, device_id=target(offset), device_id_type=MESH)
    greeted = 0
    if len(groups) > 1:
        for steps in mates:
            for step in steps:
                pl.semaphore_signal(barrier, inc=1, device_id=mate(step), device_id_type=MESH)
            greeted = greeted + len(steps)

    def options(axis, step):
        if counts[axis] <= step:
            return 0
        return (me[axis] >= step).astype(jnp.int32) + (me[axis] + step < counts[axis]).astype(jnp.int32)

    around = (1 + options(0, 1)) * (1 + options(1, 1)) * (1 + options(2, 1)) - 1
    greeted = greeted + around + sum(options(0, step) for step in range(2, kx + 1))

    def clear(ref):
        ref[...] = jnp.zeros(ref.shape, jnp.float32)

    for axis, edges in enumerate((
            [[gc0.at[:, pl.ds(0, WIDTH)], zrx.at[:, 0]], [gc0.at[:, pl.ds(WIDTH + bx, WIDTH)], zrx.at[:, 1]]],
            [[ref.at[..., pl.ds(at, WIDTH), :] for ref in (gc0, zr, zrx)] for at in (EDGE - WIDTH, EDGE + by)],
            [[ref.at[side] for ref in (zr, zrx)] for side in range(2)])):
        for refs, edge in zip(edges, (0, counts[axis] - 1)):
            @pl.when(me[axis] == edge)
            def _(refs=refs):
                for ref in refs:
                    clear(ref)

    for ref in (gc0, zr, zrx):
        clear(ref.at[..., pl.ds(0, EDGE - WIDTH), :])
        clear(ref.at[..., pl.ds(ey - EDGE + WIDTH, EDGE - WIDTH), :])
    for at in (0, ey):
        ys[:, :, at:at + 2 * EDGE, :] = jnp.zeros((2, ex, 2 * EDGE, bz), jnp.float32)

    def row_ends(dy):
        if dy == 0:
            return 0, by, EDGE
        if dy > 0:
            return by - WIDTH, WIDTH, EDGE - WIDTH
        return 0, WIDTH, EDGE + by

    def remote(src, dst, phase, offset):
        pltpu.make_async_remote_copy(
            src_ref=src, dst_ref=dst, send_sem=ssem, recv_sem=rsem.at[phase],
            device_id=target(offset), device_id_type=MESH).start()

    def planes_copy(phase, offset, first, size):
        dx, dy, dz = offset
        start, rows, goes = row_ends(dy)
        if dx == 0:
            px, tx, size = WIDTH, WIDTH, bx
        elif dx > 0:
            px, tx = WIDTH + bx - first - size, WIDTH - first - size
        else:
            px, tx = WIDTH + first, WIDTH + bx + first
        src = gc0.at[:, pl.ds(px, size), pl.ds(EDGE + start, rows), :]
        dst = gc0.at[:, pl.ds(tx, size), pl.ds(goes, rows), :]
        return (src, dst, phase, offset)

    def fine_copy(offset):
        dx, dy, dz = offset
        if dz == 0:
            return planes_copy(0, offset, 0, INNER)
        start, rows, goes = row_ends(dy)
        side = 0 if dz > 0 else 1
        if dx == 0:
            src = pk.at[:, pl.ds(start, rows), :]
            dst = zr.at[side, :, pl.ds(goes, rows), :]
        else:
            end = 0 if dx > 0 else 1
            src = pkx.at[end, pl.ds(start, rows), :]
            dst = zrx.at[side, end, pl.ds(goes, rows), :]
        return (src, dst, 0, offset)

    def outer_copy(offset):
        return planes_copy(1, offset, INNER, WIDTH - INNER)

    def part(offset, depth):
        dx, dy, dz = offset
        if abs(dx) > 1 or abs(dy) > 1:
            return 0, 1
        if dz != 0:
            return 4, 1
        if dx == 0:
            return 0, 4
        if dx < 0:
            return 0, 1 + depth
        return 4 - depth, 1 + depth

    def coarse_copy(phase, offset, s, r, depth):
        dx, dy, dz = offset
        at, size = part(offset, depth)
        return (s.at[pl.ds(at, size)], r.at[kx - dx, ky - dy, 1 - dz, pl.ds(at, size)], phase, offset)

    def tiles(make, offset):
        size = 1
        for n in make(offset)[0].shape:
            size *= n
        assert size % bz == 0
        return size // bz

    def begin(make, offsets):
        for offset in offsets:
            @pl.when(valid(offset))
            def _(offset=offset):
                remote(*make(offset))

    def wait_for(sem, pairs):
        sizes = {}
        for make, offsets in pairs:
            for offset in offsets:
                key = tuple(map(abs, offset))
                sizes.setdefault(key, 0)
                if offset == key:
                    sizes[key] += tiles(make, offset)

        def amount(options):
            total = 0
            for (a, b, c), size in sizes.items():
                total = total + size * options[0][a] * options[1][b] * options[2][c]
            return total

        def number(place, count, step):
            return 1 if step == 0 else (place >= step) * 1 + (place + step < count) * 1

        def table(axis, place):
            return [number(place, counts[axis], k) for k in range(3)]

        here = []
        for axis in range(3):
            has = [1]
            for k in (1, 2):
                n = (me[axis] >= k).astype(jnp.int32) + (me[axis] + k < counts[axis]).astype(jnp.int32)
                has.append(n)
            here.append(has)
        total = amount(here)
        for value in sorted({amount(options) for options in itertools.product(
                *[[table(axis, place) for place in range(counts[axis])] for axis in range(3)])}):
            @pl.when(total == value)
            def _(value=value):
                some = units.at[pl.ds(0, value)]
                pltpu.make_async_copy(some, some, sem).wait()

    def arrive(phase, make, offsets):
        wait_for(rsem.at[phase], [(make, offsets)])

    def leave(pairs):
        wait_for(ssem, pairs)

    def mate_copy(stage, k):
        n = base[stage] + k
        return pltpu.make_async_remote_copy(
            src_ref=red_s.at[stage], dst_ref=red_r.at[n], send_sem=lssem.at[stage],
            recv_sem=lrsem.at[stage], device_id=mate(mates[stage][k]), device_id_type=MESH)

    def sum_begin(stage, value):
        red_s[stage] = value
        for k in range(len(mates[stage])):
            mate_copy(stage, k).start()

    def sum_end(stage):
        some = red_r.at[pl.ds(base[stage], len(mates[stage]))]
        pltpu.make_async_copy(some, some, lrsem.at[stage]).wait()
        return total_of([red_s[stage]] + [red_r[base[stage] + k] for k in range(len(mates[stage]))])

    strip = (lane[:by] < WIDTH) | (lane[:by] >= bz - WIDTH)
    place = lax.rem(lane + WIDTH, bz)
    low = lax.rem(place, SPAN) < WIDTH
    band = (lane < WIDTH) | (lane >= bz - WIDTH)
    first, last = lane == 0, lane == bz - 1

    def turn_to(v, shift):
        shift = shift % bz
        return v if shift == 0 else pltpu.roll(v, shift, 1)

    def pack(planes):
        pieces = [turn_to(jnp.where(strip, plane, 0.0), SPAN * i) for i, plane in enumerate(planes)]
        ends = (total_of(pieces[bx - WIDTH:]), total_of(pieces[:WIDTH]))
        return ends, total_of(pieces[WIDTH:bx - WIDTH] + list(ends))

    def lines(v, wide):
        a, b = v
        la, ra = pltpu.roll(a, 1, 1), pltpu.roll(a, bz - 1, 1)
        lb, rb = pltpu.roll(b, 1, 1), pltpu.roll(b, bz - 1, 1)
        f, l = first[:a.shape[0]], last[:a.shape[0]]
        sa = a + jnp.where(f, lb, la) + jnp.where(l, rb, ra)
        return sa, b + jnp.where(f, la, lb) + jnp.where(l, ra, rb) if wide else None

    shore = WIDTH - 1
    rows_all, rows_some = slice(0, ey), slice(EDGE - shore, EDGE + by + shore)

    def moved(rows, by_):
        return slice(rows.start + by_, rows.stop + by_)

    def boxes(value, start, stop, wide=True, rows=rows_some):
        held, pairs = {}, {}

        def at(i):
            if i not in held:
                held[i] = value(i)
            return held[i]

        def pair(i):
            if i not in pairs:
                pairs[i] = [p + q for p, q in zip(at(i), at(i + 1))]
            return pairs[i]

        def result(i):
            if (i - start) % 2 == 0:
                around = [p + q for p, q in zip(at(i - 1), pair(i))]
            else:
                around = [p + q for p, q in zip(pair(i - 1), at(i + 1))]
            total = []
            for t in range(2):
                ys[t, i, moved(rows, EDGE), :] = around[t]
                mid_row = around[t] if rows is rows_some else ys[t, i, moved(rows_some, EDGE), :]
                total.append(mid_row + ys[t, i, moved(rows_some, EDGE - 1), :] + ys[t, i, moved(rows_some, EDGE + 1), :])
            return lines(total, wide)

        return at, result

    def box(v):
        s = v + pltpu.roll(v, 1, 2) + pltpu.roll(v, v.shape[2] - 1, 2)
        s = s + pltpu.roll(s, 1, 1) + pltpu.roll(s, v.shape[1] - 1, 1)
        zero = jnp.zeros_like(s[:1])
        return s + jnp.concatenate([zero, s[:-1]], 0) + jnp.concatenate([s[1:], zero], 0)

    down = (2 * lane8) % bz
    down_c = (2 * lane8) % half
    up_a = lane8 >> 1
    up_b = (lane8 + bz) >> 1
    aside = 2 * (lane8 & 1) - 1
    up_c = jnp.where(lane8 < 3 * quarter, lane8 >> 1, (lane8 >> 1) + half)

    def paired(v):
        return v + pltpu.roll(v, bz - 1, v.ndim - 1)

    lx = ox + 2

    def restricted(of):
        for m in range(lx):
            a0, b0 = of(2 * m + INNER)
            a1, b1 = of(2 * m + INNER + 1)
            xr0[moved(rows_some, m * ey), :] = a0 + a1
            xr1[moved(rows_some, m * ey), :] = b0 + b1
        n = lx * my
        a = xr0[pl.ds(0, n, stride=2), :] + xr0[pl.ds(1, n, stride=2), :]
        b = xr1[pl.ds(0, n, stride=2), :] + xr1[pl.ds(1, n, stride=2), :]
        a, b = pick(paired(0.5 * a), down), pick(paired(0.5 * b), down)
        return jnp.where(iota(a.shape, 1) < half, a, b).reshape(lx, my, bz)

    turn = lane8 // quarter

    def coarsened(v):
        for m in range(qx):
            xm[m * my:(m + 1) * my, :] = v[2 * m] + v[2 * m + 1]
        n = qx * my // 2
        a = xm[pl.ds(0, n, stride=2), :] + xm[pl.ds(1, n, stride=2), :]
        a = pick(paired(0.5 * a), down_c)
        rows = my // 2
        tile = a[:rows]
        for m in range(1, qx):
            tile = jnp.where(turn == m, a[m * rows:(m + 1) * rows], tile)
        return pltpu.roll(tile, rows - 2, 0)

    rim = (lane8 < RIM) | ((lane8 >= half - RIM) & (lane8 < half))
    edge1 = my // 2 - by // 4
    here_ends = (lane8 < RIM * ox) | ((lane8 >= half - RIM) & (lane8 < half - RIM + RIM * ox))

    def post(s, v1, tile):
        own = [v1[p][edge1:edge1 + by // 2] for p in range(ox)]
        ends = total_of([turn_to(jnp.where(rim, own[p], 0.0), RIM * p) for p in range(ox)])
        ends = jnp.where(here_ends, ends, pltpu.roll(turn_to(ends, RIM * ox), 4, 0))
        tile = jnp.where(row8 < qy, tile, ends)
        s[0] = tile
        for k in range(ox // 2):
            s[1 + k] = jnp.where(lane8 < half, own[2 * k], pltpu.roll(own[2 * k + 1], half, 1))
        s[4] = tile

    def middle(s, r, width):
        depth = RIM // 2 if width > 2 else 1

        def get(dx, dy, dz, k):
            if (dx, dy, dz) == (0, 0, 0):
                return s[k]
            if any(abs(d) >= n for d, n in zip((dx, dy, dz), counts)):
                return jnp.zeros((8, bz), jnp.float32)
            return r[kx + dx, ky + dy, 1 + dz, k]

        def rows(tiles):
            before, here, after = tiles
            return (pltpu.roll(jnp.where(row8 >= 4, before, here), 4, 0),
                    pltpu.roll(jnp.where(row8 >= 4, here, after), 4, 0))

        planes = []
        for dx in (-1, 0, 1):
            tiles = range(ox // 2 - depth, ox // 2) if dx < 0 else range(depth) if dx > 0 else range(ox // 2)
            ends = [jnp.where(lane8 < 2 * RIM * ox + RIM, get(dx, dy, 1, 4), get(dx, dy, -1, 4)) for dy in (-1, 0, 1)]
            ends = [jnp.where(row8 < 4, pltpu.roll(ends[k], 4, 0), turn_to(ends[k + 1], -RIM * ox)) for k in range(2)]
            for k in tiles:
                pair = rows([get(dx, dy, 0, 1 + k) for dy in (-1, 0, 1)])
                for odd in (0, 1):
                    p = 2 * k + odd
                    planes.append(jnp.concatenate([
                        jnp.where(lane8 < half, pltpu.roll(t, half, 1) if odd else t, turn_to(e, half - RIM * p))
                        for t, e in zip(pair, ends)], 0))
        return jnp.stack(planes)

    xs = [x for x in range(-PART, qx + PART) if -kx * qx <= x < (kx + 1) * qx]

    def gathered(s, r, far):
        zero = jnp.zeros((8, bz), jnp.float32)

        def get(dx, dy, dz):
            if (dx, dy, dz) == (0, 0, 0):
                return s[0]
            if any(abs(d) >= n for d, n in zip((dx, dy, dz), counts)) or abs(dy) > far:
                return zero
            return r[kx + dx, ky + dy, 1 + dz, part((-dx, -dy, -dz), 0)[0]]

        columns = {}
        for dx in sorted({x // qx for x in xs}):
            for dy in range(-2, 3):
                if abs(dy) > far:
                    continue
                here = get(dx, dy, 0)
                after = pltpu.roll(get(dx, dy, 1), quarter, 1)
                before = pltpu.roll(get(dx, dy, -1), 3 * quarter, 1)
                for m in range(qx):
                    tile = jnp.where(turn == (m + 1) % 4, after, here)
                    tile = jnp.where(turn == (m + 3) % 4, before, tile)
                    columns[dx * qx + m, dy] = turn_to(tile, -quarter * m)
        planes = []
        for x in xs:
            t = {dy: columns.get((x, dy), zero) for dy in range(-2, 3)}
            upper = jnp.where(row8 < qy, t[-1], pltpu.roll(t[0], 4, 0))
            if far > 1:
                lower = jnp.where(row8 < qy, t[1], pltpu.roll(jnp.where(row8 < 2, t[2], t[-2]), 4, 0))
            else:
                lower = jnp.where(row8 < qy, t[1], 0.0)
            planes.append(jnp.concatenate([upper, lower], 0))
        return jnp.stack(planes)

    def within(place, axis, size):
        place = place + me[axis] * size
        return (place >= 0) & (place < counts[axis] * size)

    for copy in copies:
        copy.wait()
    g, c = ([gc0[n, WIDTH + i, EDGE:EDGE + by, :] for i in range(bx)] for n in range(2))
    for i in range(bx):
        g_ref[i] = g[i]
    (g_last, g_first), pk[0] = pack(g)
    (c_last, c_first), pk[1] = pack(c)
    pkx[0] = g_last + turn_to(c_last, -SPAN * WIDTH)
    pkx[1] = g_first + turn_to(c_first, SPAN * WIDTH)

    for m in range(ox):
        xr0[m * ey + EDGE:m * ey + EDGE + by, :] = c[2 * m] + c[2 * m + 1]
    n = ox * my
    own1 = xr0[pl.ds(0, n, stride=2), :] + xr0[pl.ds(1, n, stride=2), :]
    own1 = pick(paired(0.5 * own1), down).reshape(ox, my, bz)
    post(s0, own1, coarsened(own1))

    def relay_copy(offset):
        dx, dy, dz = offset
        if (dy, dz) == (0, 0):
            return coarse_copy(2, offset, s0, r0, RIM // 2)
        far = abs(dx) > 1 or abs(dy) > 1
        at, size = part((-dx, 0, 0), RIM // 2)
        if far or dz != 0:
            at, size = 4 if dx == -1 else 0, 1
        src = s0.at[pl.ds(at, size)] if dx == 0 else r0.at[kx + dx, ky, 1, pl.ds(at, size)]
        goes = 0 if far else 4 if dz != 0 else at
        return src, r0.at[kx + dx, ky - dy, 1 - dz, pl.ds(goes, size)], 5, (0, dy, dz)

    along_x = [o for o in near if o[1] == o[2] == 0]
    onwards = [o for o in near if o not in along_x]
    make_b = lambda o: coarse_copy(3, o, s1, r1, RIM // 2)
    make_d = lambda o: coarse_copy(4, o, s2, r2, 1)
    pl.semaphore_wait(barrier, greeted)
    begin(relay_copy, along_x)
    begin(fine_copy, close)

    in_y = within(row - EDGE, 1, by)

    def factors(t, i, rows, c, inverse):
        d[t, i, rows], k27[t, i, rows] = inverse, 27.0 + c
        w27[t, i, rows] = 1.0 - inverse * (27.0 + c)

    def spread(i):
        if own(i):
            shifts = [SPAN * (i - WIDTH)] * 2
            packs, scale = merged, 0
        elif i < WIDTH:
            shifts = [SPAN * (bx - WIDTH + i), SPAN * (bx - WIDTH + i - WIDTH)]
            packs, scale = [ends[0]] * 2, 1
        else:
            shifts = [SPAN * (i - WIDTH - bx), SPAN * (i - bx)]
            packs, scale = [ends[1]] * 2, 2
        t1[0, i] = turn_to(packs[0], -shifts[0])
        cb = t1[1, i] = turn_to(packs[1], -shifts[1])
        factors(1, i, slice(None), cb, scales_b[scale] / (26.0 + cb))
        for at, size in ((0, EDGE), (EDGE + by, EDGE)) if own(i) else ((0, ey),):
            rows = slice(at, at + size)
            c = gc0[1, i, rows]
            factors(0, i, rows, c, scales_a[scale][rows] / (26.0 + c))

    def own(i):
        return WIDTH <= i < WIDTH + bx

    def kept_if(ok):
        return jnp.where(ok, relaxation, 0.0)

    in_x = [True, me[0] > 0, me[0] + 1 < counts[0]]
    in_z = jnp.where(lane < half, jnp.full((ey, bz), kept_if(me[2] + 1 < counts[2]), jnp.float32),
                     jnp.full((ey, bz), kept_if(me[2] > 0), jnp.float32))
    scales_a = [jnp.where(in_y, kept_if(ok), 0.0) for ok in in_x]
    scales_b = [jnp.where(in_y & band & ok, in_z, 0.0) for ok in in_x]
    for i in range(bx):
        factors(0, WIDTH + i, slice(EDGE, EDGE + by), c[i], relaxation / (26.0 + c[i]))

    arrive(2, relay_copy, along_x)
    begin(relay_copy, [o for o in onwards if abs(o[1]) <= 1])
    begin(outer_copy, sides)
    arrive(0, fine_copy, close)
    begin(relay_copy, [o for o in onwards if abs(o[1]) > 1])
    merged = [jnp.where(low, zr[0, f], zr[1, f]) for f in range(2)]
    ends = [jnp.where(low, zrx[0, e], zrx[1, e]) for e in range(2)]
    skip = WIDTH - INNER
    for i in range(skip, ex - skip):
        spread(i)

    def inside1(shape, width):
        zl = iota(shape, 2)
        zl = jnp.where(zl < 3 * quarter, zl, zl - bz)
        ok = within(iota(shape, 0) - width, 0, ox) & within(iota(shape, 1) - edge1, 1, by // 2)
        return ok & within(zl, 2, half) & (zl >= -RIM) & (zl < half + RIM)

    c1 = restricted(lambda i: (gc0[1, i, rows_some], t1[1, i, rows_some]))
    near0 = jnp.where(inside1((lx, my, bz), 1), relaxation / (26.0 + c1), 0.0)
    near1 = 27.0 + c1

    def outer():
        arrive(1, outer_copy, sides)
        for i in list(range(skip)) + list(range(ex - skip, ex)):
            spread(i)

    def coefficients():
        arrive(5, relay_copy, onwards)
        c1 = middle(s0, r0, RIM)
        ok = inside1(c1.shape, RIM)
        c1 = jnp.where(ok, c1, 0.0)
        mid[0] = jnp.where(ok, relaxation / (26.0 + c1), 0.0)
        mid[1] = 27.0 + c1
        c2 = gathered(s0, r0, ky)
        shape = c2.shape
        z = iota(shape, 2)
        z = jnp.where(z < 2 * quarter, z, z - bz)
        y = iota(shape, 1)
        y = jnp.where(y < my - 2, y, y - my) - qy
        ok = within(iota(shape, 0) + xs[0], 0, qx) & within(y, 1, qy)
        ok = ok & within(z, 2, quarter) & (z >= -quarter)
        c2 = jnp.where(ok, c2, 0.0)
        kept[0] = jnp.where(ok, relaxation / (26.0 + c2), 0.0)
        kept[1] = 27.0 + c2

    def cycle(phase, g_at, near0, near1, s, r, make, offsets, far, width, hook, second, finish):
        def e0(i, rows=rows_some):
            a, b = g_at(i, rows)
            return d[0, i, rows] * a, d[1, i, rows] * b

        start = WIDTH - 2
        at, result = boxes(e0, start, ex - start)

        def remainder(i):
            a, b = g_at(i, rows_some)
            sa, sb = result(i)
            if phase == 4:
                se[0, i, rows_some], se[1, i, rows_some] = sa, sb
            return w27[0, i, rows_some] * a + sa, w27[1, i, rows_some] * b + sb

        g1 = restricted(remainder)
        f = near0 * g1
        post(s, g1[1:1 + ox], coarsened((g1 - near1 * f + box(f))[1:1 + ox]))
        begin(make, offsets)
        if phase == 3:
            outer()
            whole = boxes(lambda i: e0(i, rows_all), 1, ex - 1, rows=rows_all)[1]
            for i in range(1, ex - 1):
                se[0, i, rows_some], se[1, i, rows_some] = whole(i)
        hook()
        arrive(phase, make, offsets)
        inv, diag = kept[0], kept[1]
        g2 = jnp.where(inv > 0.0, gathered(s, r, far), 0.0)
        reach = (width + 1) // 2
        e = inv * g2
        lowest = 0
        for sweep in range(SWEEPS - 1):
            left = reach + SWEEPS - 2 - sweep
            keep = [n for n, x in enumerate(xs) if -left <= x < qx + left]
            some = slice(keep[0], keep[-1] + 1)
            part_ = slice(keep[0] - lowest, keep[-1] + 1 - lowest)
            e = e[part_] + inv[some] * (g2[some] - diag[some] * e[part_] + box(e)[part_])
            lowest = keep[0]
        second()
        held = xs[lowest:lowest + e.shape[0]]
        nq = qx + 2 * reach
        zero = jnp.zeros_like(e[:1])
        e = jnp.concatenate([e[held.index(x)][None] if x in held else zero for x in range(-reach, qx + reach)], 0)
        e = pltpu.roll(e, my - 2, 1)[:, :my // 2].reshape(nq * my // 2, bz)
        u = pick(e, up_c)
        um[pl.ds(0, nq * my // 2, stride=2), :] = u
        um[pl.ds(1, nq * my // 2, stride=2), :] = u
        u = um[:nq * my, :].reshape(nq, my, bz)
        span = width + 1
        mx = ox + 2 * span
        u = jnp.concatenate([u[(m - span) // 2 + reach][None] for m in range(mx)], 0)
        skip1 = RIM - span
        inv, diag = mid[0, skip1:skip1 + mx], mid[1, skip1:skip1 + mx]
        g1 = jnp.where(inv > 0.0, middle(s, r, span), 0.0)
        f = inv * g1 + u
        f = f + inv * (g1 - diag * f + box(f))
        nm = mx - 2
        f = f[1:mx - 1].reshape(nm * my, bz)
        for pf, sf, up in ((pf0, sf0, up_a), (pf1, sf1, up_b)):
            w = pick(f, up)
            z = (w + w + pick(f, (up + aside) % bz)).reshape(nm, my, bz)
            for odd in range(2):
                y = z + z + pltpu.roll(z, my - 1 if odd else 1, 1)
                sf[pl.ds(odd, nm * my, stride=2), :] = y.reshape(nm * my, bz)
            pf[pl.ds(0, nm * my, stride=2), :] = w
            pf[pl.ds(1, nm * my, stride=2), :] = w

        def e1(i, rows):
            m = (i - WIDTH) // 2 + width
            a, b = e0(i, rows)
            return a + pf0[moved(rows, m * ey), :], b + pf1[moved(rows, m * ey), :]

        wide = width > 1
        past = INNER + 1 if wide else 1
        def result1(i):
            x = i - WIDTH
            m = x // 2 + width
            n = m + 1 if x % 2 else m - 1
            total = []
            for t, sf in enumerate((sf0, sf1)):
                here = sf[moved(rows_some, m * ey), :]
                total.append(se[t, i, rows_some] + (here + here + sf[moved(rows_some, n * ey), :]))
            return total

        def e2(i):
            values = e1(i, rows_some)
            return [w27[t, i, rows_some] * a + e + d[t, i, rows_some] * s_
                    for t, (a, e, s_) in enumerate(zip(values, e0(i), result1(i)))]

        at2, result2 = boxes(e2, WIDTH - past + 1, WIDTH + bx + past - 1, wide)
        for i in range(WIDTH - past + 1, WIDTH + bx + past - 1):
            a, b = at2(i)
            sa, sb = result2(i)
            finish(i, a, k27[0, i, rows_some] * a - sa, k27[1, i, rows_some] * b - sb if wide else None)

    gamma, delta = [], []

    def finish1(i, e, out, out_b):
        im0[0, i, rows_some] = out
        im0[1, i, rows_some] = out_b
        if own(i):
            e, out = e[shore:shore + by], im0[0, i, EDGE:EDGE + by]
            pre_ref[i - WIDTH] = e
            img_ref[i - WIDTH] = out
            gamma.append(g_ref[i - WIDTH] * e)
            delta.append(out * e)
        if i == WIDTH + bx - 1:
            gs = jnp.sum(total_of(gamma), axis=0, keepdims=True)
            ds = jnp.sum(total_of(delta), axis=0, keepdims=True)
            gs, ds = gs + pltpu.roll(gs, half, 1), ds + pltpu.roll(ds, half, 1)
            sum_begin(0, jnp.where(lane8[:1] < half, gs, ds))

    nothing = lambda: None
    cycle(3, lambda i, rows: (gc0[0, i, rows], t1[0, i, rows]), near0, near1, s1, r1, make_b, near, ky, RIM - 1, coefficients, nothing, finish1)

    def relay(stage):
        if len(groups) > 1:
            sum_begin(stage, sum_end(stage - 1))

    def finish2(i, e, out, out_b):
        twice_ref[i - WIDTH] = e[shore:shore + by]
        image_twice_ref[i - WIDTH] = out[shore:shore + by]

    skip1 = RIM - 1
    cycle(4, lambda i, rows: (im0[0, i, rows], im0[1, i, rows]), mid[0, skip1:skip1 + lx], mid[1, skip1:skip1 + lx], s2, r2, make_d, later, 1, 1,
          lambda: relay(1), lambda: relay(2), finish2)

    total = sum_end(len(groups) - 1)
    gs = jnp.sum(jnp.where(lane8[:1] < half, total, 0.0), axis=1, keepdims=True)
    ds = jnp.sum(jnp.where(lane8[:1] < half, 0.0, total), axis=1, keepdims=True)
    alpha_ref[...] = jnp.broadcast_to(gs / ds, (1, bz)).reshape(alpha_ref.shape)
    leave([(fine_copy, close), (outer_copy, sides), (relay_copy, near), (make_b, near), (make_d, later)])
    for stage in range(len(groups)):
        some = red_r.at[pl.ds(base[stage], len(mates[stage]))]
        pltpu.make_async_copy(some, some, lssem.at[stage]).wait()


def solution(mesh):
    counts = tuple(mesh.shape[a] for a in AXES)

    def shards(right_side, coefficient):
        bx, by, bz = block = right_side.shape
        assert SPAN <= bx and SPAN * bx <= bz and by == 16 and bx % 4 == 0
        kx = max(1, min(-(-PART // (bx // 4)), counts[0] - 1))
        ky = max(1, min(-(-PART // (by // 4)), counts[1] - 1))
        ex, ey = bx + SPAN, by + 2 * EDGE
        ox, my = bx // 2, ey // 2
        qx = bx // 4
        mx = ox + 2 * RIM
        most = (2 * kx + 1) * (2 * ky + 1) * 3
        planes = len([x for x in range(-PART, qx + PART) if -kx * qx <= x < (kx + 1) * qx])
        mates = [len(partners(counts, group)) for group in stages(counts)]
        f32 = jnp.float32
        vmem = pl.BlockSpec(memory_space=pltpu.VMEM)
        messages = [pltpu.VMEM((5, 8, bz), f32)] * 3
        messages += [pltpu.VMEM((2 * kx + 1, 2 * ky + 1, 3, 5, 8, bz), f32)] * 3
        precond, image, twice, image_twice, alpha, g = pl.pallas_call(
            functools.partial(kernel, counts, block, kx, ky),
            out_shape=[pltpu.VMEM(block, f32)] * 4 + [pltpu.VMEM((1, 1, bz), f32), pltpu.VMEM(block, f32)],
            in_specs=[pl.BlockSpec(memory_space=pltpu.HBM)] * 2,
            out_specs=[vmem] * 6,
            scratch_shapes=[
                pltpu.VMEM((2, ex, ey, bz), f32),
                pltpu.VMEM((2, ex, ey, bz), f32),
                pltpu.VMEM((2, by, bz), f32),
                pltpu.VMEM((2, by, bz), f32),
                pltpu.VMEM((2, 2, ey, bz), f32),
                pltpu.VMEM((2, 2, ey, bz), f32),
                pltpu.VMEM((2, ex, ey, bz), f32),
                *[pltpu.VMEM((2, ex, ey, bz), f32)] * 3,
                pltpu.VMEM((2, ex, ey + 2 * EDGE, bz), f32),
                pltpu.VMEM(((ox + 2) * ey, bz), f32),
                pltpu.VMEM(((ox + 2) * ey, bz), f32),
                *[pltpu.VMEM(((mx - 2) * ey, bz), f32)] * 4,
                pltpu.VMEM((2, ex, ey, bz), f32),
                pltpu.VMEM((qx * my, bz), f32),
                pltpu.VMEM(((qx + 4) * my, bz), f32),
                *messages,
                pltpu.VMEM((2, planes, my, bz), f32),
                pltpu.VMEM((2, mx, my, bz), f32),
                pltpu.VMEM((len(mates), 1, bz), f32),
                pltpu.VMEM((sum(mates), 1, bz), f32),
                pltpu.VMEM((128 * most, 1, bz), f32),
                pltpu.SemaphoreType.DMA((2,)),
                pltpu.SemaphoreType.DMA,
                pltpu.SemaphoreType.DMA((6,)),
                pltpu.SemaphoreType.DMA((len(mates),)),
                pltpu.SemaphoreType.DMA((len(mates),)),
            ],
            compiler_params=pltpu.CompilerParams(collective_id=0, has_side_effects=True),
            name="relayed",
        )(right_side, coefficient)
        return (alpha * precond, g - alpha * image,
                precond - alpha * twice, image - alpha * image_twice)

    placed = (P(*AXES), P(*AXES))
    return jax.shard_map(
        shards, mesh=mesh, in_specs=placed, out_specs=(P(*AXES),) * 4, check_vma=False
    )
```

```python
import functools
import itertools

import jax
import jax.numpy as jnp
from jax import lax
from jax.experimental import pallas as pl
from jax.experimental.pallas import tpu as pltpu
from jax.sharding import PartitionSpec as P

SWEEPS = 4
relaxation = 0.6

AXES = ("gx", "gy", "gz")
MESH = pl.DeviceIdType.MESH
WIDTH = 5
INNER = 3
EDGE = 8
SPAN = 2 * WIDTH
RIM = 4
PART = SWEEPS + 1


def pick(values, lanes):
    flat = values.reshape(-1, values.shape[-1])
    lanes = jnp.broadcast_to(lanes[:1], flat.shape)
    return jnp.take_along_axis(flat, lanes, axis=1).reshape(values.shape)


def iota(shape, dim):
    return lax.broadcasted_iota(jnp.int32, shape, dim)


def total_of(values):
    while len(values) > 1:
        values = [a + b for a, b in zip(values[::2], values[1::2])] + values[len(values) & ~1:]
    return values[0]


def stages(counts):
    if max(counts) <= RIM:
        return [(0, 1, 2)]
    return [(2,), (1,), (0,)]


def partners(counts, group):
    steps = [(0, 0, 0)]
    for axis in group:
        steps = [s[:axis] + (k,) + s[axis + 1:] for s in steps for k in range(counts[axis])]
    return [s for s in steps if s != (0, 0, 0)]


def kernel(counts, block, kx, ky, g_hbm, c_hbm, pre_ref, img_ref, twice_ref, image_twice_ref, alpha_ref, g_ref,
           gc0, im0, pk, pkx, zr, zrx, t1, d, k27, w27, ys, xr0, xr1, pf0, pf1, sf0, sf1, se, xm, um,
           s0, s1, s2, r0, r1, r2, kept, mid, red_s, red_r, units, insem, ssem, rsem, lssem, lrsem):
    bx, by, bz = block
    me = [lax.axis_index(a) for a in AXES]
    ex, ey = bx + SPAN, by + 2 * EDGE
    ox, my = bx // 2, ey // 2
    qx, qy = bx // 4, by // 4
    half, quarter = bz // 2, bz // 4
    lane = iota((ey, bz), 1)
    row = iota((ey, bz), 0)
    lane8 = iota((8, bz), 1)
    row8 = iota((8, bz), 0)

    def valid(offset):
        ok = None
        for axis, step in enumerate(offset):
            if step == 0:
                continue
            place = me[axis] + step
            term = place >= 0 if step < 0 else place < counts[axis]
            ok = term if ok is None else jnp.logical_and(ok, term)
        return ok

    def target(offset):
        return tuple(m + s for m, s in zip(me, offset))

    near = [(dx, dy, dz) for dx in range(-kx, kx + 1) for dy in range(-ky, ky + 1) for dz in (-1, 0, 1)]
    near = [o for o in near if o != (0, 0, 0) and all(counts[a] > abs(o[a]) for a in range(3))]
    near.sort(key=lambda o: -sum(map(abs, o)))
    close = [o for o in near if abs(o[0]) <= 1 and abs(o[1]) <= 1]
    sides = [o for o in close if o[0] != 0 and o[2] == 0]
    later = [o for o in near if abs(o[1]) <= 1]

    groups = stages(counts)
    mates = []
    base = [0]
    for group in groups:
        mates.append(partners(counts, group))
        base.append(base[-1] + len(mates[-1]))

    def mate(step):
        return tuple(lax.rem(m + s, n) if s else m for m, s, n in zip(me, step, counts))

    inside0 = gc0.at[:, pl.ds(WIDTH, bx), pl.ds(EDGE, by), :]
    copies = [pltpu.make_async_copy(src, inside0.at[n], insem.at[n]) for n, src in enumerate((g_hbm, c_hbm))]
    for copy in copies:
        copy.start()
    greet = [o for o in near if abs(o[1]) <= 1 and (abs(o[0]) <= 1 or o[1] == o[2] == 0)]
    barrier = pltpu.get_barrier_semaphore()
    for offset in greet:
        @pl.when(valid(offset))
        def _(offset=offset):
            pl.semaphore_signal(barrier, inc=1, device_id=target(offset), device_id_type=MESH)
    greeted = 0
    if len(groups) > 1:
        for steps in mates:
            for step in steps:
                pl.semaphore_signal(barrier, inc=1, device_id=mate(step), device_id_type=MESH)
            greeted = greeted + len(steps)

    def options(axis, step):
        if counts[axis] <= step:
            return 0
        return (me[axis] >= step).astype(jnp.int32) + (me[axis] + step < counts[axis]).astype(jnp.int32)

    around = (1 + options(0, 1)) * (1 + options(1, 1)) * (1 + options(2, 1)) - 1
    greeted = greeted + around + sum(options(0, step) for step in range(2, kx + 1))

    def clear(ref):
        ref[...] = jnp.zeros(ref.shape, jnp.float32)

    for axis, edges in enumerate((
            [[gc0.at[:, pl.ds(0, WIDTH)], zrx.at[:, 0]], [gc0.at[:, pl.ds(WIDTH + bx, WIDTH)], zrx.at[:, 1]]],
            [[ref.at[..., pl.ds(at, WIDTH), :] for ref in (gc0, zr, zrx)] for at in (EDGE - WIDTH, EDGE + by)],
            [[ref.at[side] for ref in (zr, zrx)] for side in range(2)])):
        for refs, edge in zip(edges, (0, counts[axis] - 1)):
            @pl.when(me[axis] == edge)
            def _(refs=refs):
                for ref in refs:
                    clear(ref)

    for ref in (gc0, zr, zrx):
        clear(ref.at[..., pl.ds(0, EDGE - WIDTH), :])
        clear(ref.at[..., pl.ds(ey - EDGE + WIDTH, EDGE - WIDTH), :])
    for at in (0, ey):
        ys[:, :, at:at + 2 * EDGE, :] = jnp.zeros((2, ex, 2 * EDGE, bz), jnp.float32)

    def row_ends(dy):
        if dy == 0:
            return 0, by, EDGE
        if dy > 0:
            return by - WIDTH, WIDTH, EDGE - WIDTH
        return 0, WIDTH, EDGE + by

    def remote(src, dst, phase, offset):
        pltpu.make_async_remote_copy(
            src_ref=src, dst_ref=dst, send_sem=ssem, recv_sem=rsem.at[phase],
            device_id=target(offset), device_id_type=MESH).start()

    def planes_copy(phase, offset, first, size):
        dx, dy, dz = offset
        start, rows, goes = row_ends(dy)
        if dx == 0:
            px, tx, size = WIDTH, WIDTH, bx
        elif dx > 0:
            px, tx = WIDTH + bx - first - size, WIDTH - first - size
        else:
            px, tx = WIDTH + first, WIDTH + bx + first
        src = gc0.at[:, pl.ds(px, size), pl.ds(EDGE + start, rows), :]
        dst = gc0.at[:, pl.ds(tx, size), pl.ds(goes, rows), :]
        return (src, dst, phase, offset)

    def fine_copy(offset):
        dx, dy, dz = offset
        if dz == 0:
            return planes_copy(0, offset, 0, INNER)
        start, rows, goes = row_ends(dy)
        side = 0 if dz > 0 else 1
        if dx == 0:
            src = pk.at[:, pl.ds(start, rows), :]
            dst = zr.at[side, :, pl.ds(goes, rows), :]
        else:
            end = 0 if dx > 0 else 1
            src = pkx.at[end, pl.ds(start, rows), :]
            dst = zrx.at[side, end, pl.ds(goes, rows), :]
        return (src, dst, 0, offset)

    def outer_copy(offset):
        return planes_copy(1, offset, INNER, WIDTH - INNER)

    def part(offset, depth):
        dx, dy, dz = offset
        if abs(dx) > 1 or abs(dy) > 1:
            return 0, 1
        if dz != 0:
            return 4, 1
        if dx == 0:
            return 0, 4
        if dx < 0:
            return 0, 1 + depth
        return 4 - depth, 1 + depth

    def coarse_copy(phase, offset, s, r, depth):
        dx, dy, dz = offset
        at, size = part(offset, depth)
        return (s.at[pl.ds(at, size)], r.at[kx - dx, ky - dy, 1 - dz, pl.ds(at, size)], phase, offset)

    def tiles(make, offset):
        size = 1
        for n in make(offset)[0].shape:
            size *= n
        assert size % bz == 0
        return size // bz

    def begin(make, offsets):
        for offset in offsets:
            @pl.when(valid(offset))
            def _(offset=offset):
                remote(*make(offset))

    def wait_for(sem, pairs):
        sizes = {}
        for make, offsets in pairs:
            for offset in offsets:
                key = tuple(map(abs, offset))
                sizes.setdefault(key, 0)
                if offset == key:
                    sizes[key] += tiles(make, offset)

        def amount(options):
            total = 0
            for (a, b, c), size in sizes.items():
                total = total + size * options[0][a] * options[1][b] * options[2][c]
            return total

        def number(place, count, step):
            return 1 if step == 0 else (place >= step) * 1 + (place + step < count) * 1

        def table(axis, place):
            return [number(place, counts[axis], k) for k in range(3)]

        here = []
        for axis in range(3):
            has = [1]
            for k in (1, 2):
                n = (me[axis] >= k).astype(jnp.int32) + (me[axis] + k < counts[axis]).astype(jnp.int32)
                has.append(n)
            here.append(has)
        total = amount(here)
        for value in sorted({amount(options) for options in itertools.product(
                *[[table(axis, place) for place in range(counts[axis])] for axis in range(3)])}):
            @pl.when(total == value)
            def _(value=value):
                some = units.at[pl.ds(0, value)]
                pltpu.make_async_copy(some, some, sem).wait()

    def arrive(phase, make, offsets):
        wait_for(rsem.at[phase], [(make, offsets)])

    def leave(pairs):
        wait_for(ssem, pairs)

    def mate_copy(stage, k):
        n = base[stage] + k
        return pltpu.make_async_remote_copy(
            src_ref=red_s.at[stage], dst_ref=red_r.at[n], send_sem=lssem.at[stage],
            recv_sem=lrsem.at[stage], device_id=mate(mates[stage][k]), device_id_type=MESH)

    def sum_begin(stage, value):
        red_s[stage] = value
        for k in range(len(mates[stage])):
            mate_copy(stage, k).start()

    def sum_end(stage):
        some = red_r.at[pl.ds(base[stage], len(mates[stage]))]
        pltpu.make_async_copy(some, some, lrsem.at[stage]).wait()
        return total_of([red_s[stage]] + [red_r[base[stage] + k] for k in range(len(mates[stage]))])

    strip = (lane[:by] < WIDTH) | (lane[:by] >= bz - WIDTH)
    place = lax.rem(lane + WIDTH, bz)
    low = lax.rem(place, SPAN) < WIDTH
    band = (lane < WIDTH) | (lane >= bz - WIDTH)
    first, last = lane == 0, lane == bz - 1

    def turn_to(v, shift):
        shift = shift % bz
        return v if shift == 0 else pltpu.roll(v, shift, 1)

    def pack(planes):
        pieces = [turn_to(jnp.where(strip, plane, 0.0), SPAN * i) for i, plane in enumerate(planes)]
        ends = (total_of(pieces[bx - WIDTH:]), total_of(pieces[:WIDTH]))
        return ends, total_of(pieces[WIDTH:bx - WIDTH] + list(ends))

    def lines(v, wide):
        a, b = v
        la, ra = pltpu.roll(a, 1, 1), pltpu.roll(a, bz - 1, 1)
        lb, rb = pltpu.roll(b, 1, 1), pltpu.roll(b, bz - 1, 1)
        f, l = first[:a.shape[0]], last[:a.shape[0]]
        sa = a + jnp.where(f, lb, la) + jnp.where(l, rb, ra)
        return sa, b + jnp.where(f, la, lb) + jnp.where(l, ra, rb) if wide else None

    shore = WIDTH - 1
    rows_all, rows_some = slice(0, ey), slice(EDGE - shore, EDGE + by + shore)

    def moved(rows, by_):
        return slice(rows.start + by_, rows.stop + by_)

    def boxes(value, start, stop, wide=True, rows=rows_some):
        held, pairs = {}, {}

        def at(i):
            if i not in held:
                held[i] = value(i)
            return held[i]

        def pair(i):
            if i not in pairs:
                pairs[i] = [p + q for p, q in zip(at(i), at(i + 1))]
            return pairs[i]

        def result(i):
            if (i - start) % 2 == 0:
                around = [p + q for p, q in zip(at(i - 1), pair(i))]
            else:
                around = [p + q for p, q in zip(pair(i - 1), at(i + 1))]
            total = []
            for t in range(2):
                ys[t, i, moved(rows, EDGE), :] = around[t]
                mid_row = around[t] if rows is rows_some else ys[t, i, moved(rows_some, EDGE), :]
                total.append(mid_row + ys[t, i, moved(rows_some, EDGE - 1), :] + ys[t, i, moved(rows_some, EDGE + 1), :])
            return lines(total, wide)

        return at, result

    def box(v):
        s = v + pltpu.roll(v, 1, 2) + pltpu.roll(v, v.shape[2] - 1, 2)
        s = s + pltpu.roll(s, 1, 1) + pltpu.roll(s, v.shape[1] - 1, 1)
        zero = jnp.zeros_like(s[:1])
        return s + jnp.concatenate([zero, s[:-1]], 0) + jnp.concatenate([s[1:], zero], 0)

    down = (2 * lane8) % bz
    down_c = (2 * lane8) % half
    up_a = lane8 >> 1
    up_b = (lane8 + bz) >> 1
    aside = 2 * (lane8 & 1) - 1
    up_c = jnp.where(lane8 < 3 * quarter, lane8 >> 1, (lane8 >> 1) + half)

    def paired(v):
        return v + pltpu.roll(v, bz - 1, v.ndim - 1)

    lx = ox + 2

    def restricted(of):
        for m in range(lx):
            a0, b0 = of(2 * m + INNER)
            a1, b1 = of(2 * m + INNER + 1)
            xr0[moved(rows_some, m * ey), :] = a0 + a1
            xr1[moved(rows_some, m * ey), :] = b0 + b1
        n = lx * my
        a = xr0[pl.ds(0, n, stride=2), :] + xr0[pl.ds(1, n, stride=2), :]
        b = xr1[pl.ds(0, n, stride=2), :] + xr1[pl.ds(1, n, stride=2), :]
        a, b = pick(paired(0.5 * a), down), pick(paired(0.5 * b), down)
        return jnp.where(iota(a.shape, 1) < half, a, b).reshape(lx, my, bz)

    turn = lane8 // quarter

    def coarsened(v):
        for m in range(qx):
            xm[m * my:(m + 1) * my, :] = v[2 * m] + v[2 * m + 1]
        n = qx * my // 2
        a = xm[pl.ds(0, n, stride=2), :] + xm[pl.ds(1, n, stride=2), :]
        a = pick(paired(0.5 * a), down_c)
        rows = my // 2
        tile = a[:rows]
        for m in range(1, qx):
            tile = jnp.where(turn == m, a[m * rows:(m + 1) * rows], tile)
        return pltpu.roll(tile, rows - 2, 0)

    rim = (lane8 < RIM) | ((lane8 >= half - RIM) & (lane8 < half))
    edge1 = my // 2 - by // 4
    here_ends = (lane8 < RIM * ox) | ((lane8 >= half - RIM) & (lane8 < half - RIM + RIM * ox))

    def post(s, v1, tile):
        own = [v1[p][edge1:edge1 + by // 2] for p in range(ox)]
        ends = total_of([turn_to(jnp.where(rim, own[p], 0.0), RIM * p) for p in range(ox)])
        ends = jnp.where(here_ends, ends, pltpu.roll(turn_to(ends, RIM * ox), 4, 0))
        tile = jnp.where(row8 < qy, tile, ends)
        s[0] = tile
        for k in range(ox // 2):
            s[1 + k] = jnp.where(lane8 < half, own[2 * k], pltpu.roll(own[2 * k + 1], half, 1))
        s[4] = tile

    def middle(s, r, width):
        depth = RIM // 2 if width > 2 else 1

        def get(dx, dy, dz, k):
            if (dx, dy, dz) == (0, 0, 0):
                return s[k]
            if any(abs(d) >= n for d, n in zip((dx, dy, dz), counts)):
                return jnp.zeros((8, bz), jnp.float32)
            return r[kx + dx, ky + dy, 1 + dz, k]

        def rows(tiles):
            before, here, after = tiles
            return (pltpu.roll(jnp.where(row8 >= 4, before, here), 4, 0),
                    pltpu.roll(jnp.where(row8 >= 4, here, after), 4, 0))

        planes = []
        for dx in (-1, 0, 1):
            tiles = range(ox // 2 - depth, ox // 2) if dx < 0 else range(depth) if dx > 0 else range(ox // 2)
            ends = [jnp.where(lane8 < 2 * RIM * ox + RIM, get(dx, dy, 1, 4), get(dx, dy, -1, 4)) for dy in (-1, 0, 1)]
            ends = [jnp.where(row8 < 4, pltpu.roll(ends[k], 4, 0), turn_to(ends[k + 1], -RIM * ox)) for k in range(2)]
            for k in tiles:
                pair = rows([get(dx, dy, 0, 1 + k) for dy in (-1, 0, 1)])
                for odd in (0, 1):
                    p = 2 * k + odd
                    planes.append(jnp.concatenate([
                        jnp.where(lane8 < half, pltpu.roll(t, half, 1) if odd else t, turn_to(e, half - RIM * p))
                        for t, e in zip(pair, ends)], 0))
        return jnp.stack(planes)

    xs = [x for x in range(-PART, qx + PART) if -kx * qx <= x < (kx + 1) * qx]

    def gathered(s, r, far):
        zero = jnp.zeros((8, bz), jnp.float32)

        def get(dx, dy, dz):
            if (dx, dy, dz) == (0, 0, 0):
                return s[0]
            if any(abs(d) >= n for d, n in zip((dx, dy, dz), counts)) or abs(dy) > far:
                return zero
            return r[kx + dx, ky + dy, 1 + dz, part((-dx, -dy, -dz), 0)[0]]

        columns = {}
        for dx in sorted({x // qx for x in xs}):
            for dy in range(-2, 3):
                if abs(dy) > far:
                    continue
                here = get(dx, dy, 0)
                after = pltpu.roll(get(dx, dy, 1), quarter, 1)
                before = pltpu.roll(get(dx, dy, -1), 3 * quarter, 1)
                for m in range(qx):
                    tile = jnp.where(turn == (m + 1) % 4, after, here)
                    tile = jnp.where(turn == (m + 3) % 4, before, tile)
                    columns[dx * qx + m, dy] = turn_to(tile, -quarter * m)
        planes = []
        for x in xs:
            t = {dy: columns.get((x, dy), zero) for dy in range(-2, 3)}
            upper = jnp.where(row8 < qy, t[-1], pltpu.roll(t[0], 4, 0))
            if far > 1:
                lower = jnp.where(row8 < qy, t[1], pltpu.roll(jnp.where(row8 < 2, t[2], t[-2]), 4, 0))
            else:
                lower = jnp.where(row8 < qy, t[1], 0.0)
            planes.append(jnp.concatenate([upper, lower], 0))
        return jnp.stack(planes)

    def within(place, axis, size):
        place = place + me[axis] * size
        return (place >= 0) & (place < counts[axis] * size)

    for copy in copies:
        copy.wait()
    g, c = ([gc0[n, WIDTH + i, EDGE:EDGE + by, :] for i in range(bx)] for n in range(2))
    for i in range(bx):
        g_ref[i] = g[i]
    (g_last, g_first), pk[0] = pack(g)
    (c_last, c_first), pk[1] = pack(c)
    pkx[0] = g_last + turn_to(c_last, -SPAN * WIDTH)
    pkx[1] = g_first + turn_to(c_first, SPAN * WIDTH)

    for m in range(ox):
        xr0[m * ey + EDGE:m * ey + EDGE + by, :] = c[2 * m] + c[2 * m + 1]
    n = ox * my
    own1 = xr0[pl.ds(0, n, stride=2), :] + xr0[pl.ds(1, n, stride=2), :]
    own1 = pick(paired(0.5 * own1), down).reshape(ox, my, bz)
    post(s0, own1, coarsened(own1))

    def relay_copy(offset):
        dx, dy, dz = offset
        if (dy, dz) == (0, 0):
            return coarse_copy(2, offset, s0, r0, RIM // 2)
        far = abs(dx) > 1 or abs(dy) > 1
        at, size = part((-dx, 0, 0), RIM // 2)
        if far or dz != 0:
            at, size = 4 if dx == -1 else 0, 1
        src = s0.at[pl.ds(at, size)] if dx == 0 else r0.at[kx + dx, ky, 1, pl.ds(at, size)]
        goes = 0 if far else 4 if dz != 0 else at
        return src, r0.at[kx + dx, ky - dy, 1 - dz, pl.ds(goes, size)], 5, (0, dy, dz)

    along_x = [o for o in near if o[1] == o[2] == 0]
    onwards = [o for o in near if o not in along_x]
    make_b = lambda o: coarse_copy(3, o, s1, r1, RIM // 2)
    make_d = lambda o: coarse_copy(4, o, s2, r2, 1)
    pl.semaphore_wait(barrier, greeted)
    begin(fine_copy, [o for o in close if sum(map(abs, o)) > 1])
    begin(relay_copy, along_x)
    begin(fine_copy, [o for o in close if sum(map(abs, o)) == 1])

    in_y = within(row - EDGE, 1, by)

    def factors(t, i, rows, c, inverse):
        d[t, i, rows], k27[t, i, rows] = inverse, 27.0 + c
        w27[t, i, rows] = 1.0 - inverse * (27.0 + c)

    def spread(i):
        if own(i):
            shifts = [SPAN * (i - WIDTH)] * 2
            packs, scale = merged, 0
        elif i < WIDTH:
            shifts = [SPAN * (bx - WIDTH + i), SPAN * (bx - WIDTH + i - WIDTH)]
            packs, scale = [ends[0]] * 2, 1
        else:
            shifts = [SPAN * (i - WIDTH - bx), SPAN * (i - bx)]
            packs, scale = [ends[1]] * 2, 2
        t1[0, i] = turn_to(packs[0], -shifts[0])
        cb = t1[1, i] = turn_to(packs[1], -shifts[1])
        factors(1, i, slice(None), cb, scales_b[scale] / (26.0 + cb))
        for at, size in ((0, EDGE), (EDGE + by, EDGE)) if own(i) else ((0, ey),):
            rows = slice(at, at + size)
            c = gc0[1, i, rows]
            factors(0, i, rows, c, scales_a[scale][rows] / (26.0 + c))

    def own(i):
        return WIDTH <= i < WIDTH + bx

    def kept_if(ok):
        return jnp.where(ok, relaxation, 0.0)

    in_x = [True, me[0] > 0, me[0] + 1 < counts[0]]
    in_z = jnp.where(lane < half, jnp.full((ey, bz), kept_if(me[2] + 1 < counts[2]), jnp.float32),
                     jnp.full((ey, bz), kept_if(me[2] > 0), jnp.float32))
    scales_a = [jnp.where(in_y, kept_if(ok), 0.0) for ok in in_x]
    scales_b = [jnp.where(in_y & band & ok, in_z, 0.0) for ok in in_x]
    for i in range(bx):
        factors(0, WIDTH + i, slice(EDGE, EDGE + by), c[i], relaxation / (26.0 + c[i]))

    arrive(2, relay_copy, along_x)
    begin(relay_copy, [o for o in onwards if abs(o[1]) <= 1])
    begin(outer_copy, sides)
    arrive(0, fine_copy, close)
    begin(relay_copy, [o for o in onwards if abs(o[1]) > 1])
    merged = [jnp.where(low, zr[0, f], zr[1, f]) for f in range(2)]
    ends = [jnp.where(low, zrx[0, e], zrx[1, e]) for e in range(2)]
    skip = WIDTH - INNER
    for i in range(skip, ex - skip):
        spread(i)

    def inside1(shape, width):
        zl = iota(shape, 2)
        zl = jnp.where(zl < 3 * quarter, zl, zl - bz)
        ok = within(iota(shape, 0) - width, 0, ox) & within(iota(shape, 1) - edge1, 1, by // 2)
        return ok & within(zl, 2, half) & (zl >= -RIM) & (zl < half + RIM)

    c1 = restricted(lambda i: (gc0[1, i, rows_some], t1[1, i, rows_some]))
    near0 = jnp.where(inside1((lx, my, bz), 1), relaxation / (26.0 + c1), 0.0)
    near1 = 27.0 + c1

    def outer():
        arrive(1, outer_copy, sides)
        for i in list(range(skip)) + list(range(ex - skip, ex)):
            spread(i)

    def coefficients():
        arrive(5, relay_copy, onwards)
        c1 = middle(s0, r0, RIM)
        ok = inside1(c1.shape, RIM)
        c1 = jnp.where(ok, c1, 0.0)
        mid[0] = jnp.where(ok, relaxation / (26.0 + c1), 0.0)
        mid[1] = 27.0 + c1
        c2 = gathered(s0, r0, ky)
        shape = c2.shape
        z = iota(shape, 2)
        z = jnp.where(z < 2 * quarter, z, z - bz)
        y = iota(shape, 1)
        y = jnp.where(y < my - 2, y, y - my) - qy
        ok = within(iota(shape, 0) + xs[0], 0, qx) & within(y, 1, qy)
        ok = ok & within(z, 2, quarter) & (z >= -quarter)
        c2 = jnp.where(ok, c2, 0.0)
        kept[0] = jnp.where(ok, relaxation / (26.0 + c2), 0.0)
        kept[1] = 27.0 + c2

    def cycle(phase, g_at, near0, near1, s, r, make, offsets, far, width, hook, second, finish):
        def e0(i, rows=rows_some):
            a, b = g_at(i, rows)
            return d[0, i, rows] * a, d[1, i, rows] * b

        def settle(i, sums):
            for t, (e, s_) in enumerate(zip(e0(i), sums)):
                se[t, i, rows_some] = (w27[t, i, rows_some] + 1.0) * e + d[t, i, rows_some] * s_

        start = WIDTH - 2
        at, result = boxes(e0, start, ex - start)

        def remainder(i):
            a, b = g_at(i, rows_some)
            sa, sb = result(i)
            if phase == 4:
                se[0, i, rows_some], se[1, i, rows_some] = sa, sb
            return w27[0, i, rows_some] * a + sa, w27[1, i, rows_some] * b + sb

        g1 = restricted(remainder)
        f = near0 * g1
        post(s, g1[1:1 + ox], coarsened((g1 - near1 * f + box(f))[1:1 + ox]))
        begin(make, offsets)
        if phase == 3:
            outer()
            whole = boxes(lambda i: e0(i, rows_all), 1, ex - 1, rows=rows_all)[1]
            for i in range(1, ex - 1):
                settle(i, whole(i))
        else:
            for i in range(WIDTH - 1, WIDTH + bx + 1):
                settle(i, [se[t, i, rows_some] for t in range(2)])
        hook()
        arrive(phase, make, offsets)
        inv, diag = kept[0], kept[1]
        g2 = jnp.where(inv > 0.0, gathered(s, r, far), 0.0)
        reach = (width + 1) // 2
        e = inv * g2
        lowest = 0
        for sweep in range(SWEEPS - 1):
            left = reach + SWEEPS - 2 - sweep
            keep = [n for n, x in enumerate(xs) if -left <= x < qx + left]
            some = slice(keep[0], keep[-1] + 1)
            part_ = slice(keep[0] - lowest, keep[-1] + 1 - lowest)
            e = e[part_] + inv[some] * (g2[some] - diag[some] * e[part_] + box(e)[part_])
            lowest = keep[0]
        second()
        held = xs[lowest:lowest + e.shape[0]]
        nq = qx + 2 * reach
        zero = jnp.zeros_like(e[:1])
        e = jnp.concatenate([e[held.index(x)][None] if x in held else zero for x in range(-reach, qx + reach)], 0)
        e = pltpu.roll(e, my - 2, 1)[:, :my // 2].reshape(nq * my // 2, bz)
        u = pick(e, up_c)
        um[pl.ds(0, nq * my // 2, stride=2), :] = u
        um[pl.ds(1, nq * my // 2, stride=2), :] = u
        u = um[:nq * my, :].reshape(nq, my, bz)
        span = width + 1
        mx = ox + 2 * span
        u = jnp.concatenate([u[(m - span) // 2 + reach][None] for m in range(mx)], 0)
        skip1 = RIM - span
        inv, diag = mid[0, skip1:skip1 + mx], mid[1, skip1:skip1 + mx]
        g1 = jnp.where(inv > 0.0, middle(s, r, span), 0.0)
        f = inv * g1 + u
        f = f + inv * (g1 - diag * f + box(f))
        nm = mx - 2
        f = f[1:mx - 1].reshape(nm * my, bz)
        for pf, sf, up in ((pf0, sf0, up_a), (pf1, sf1, up_b)):
            w = pick(f, up)
            z = (w + w + pick(f, (up + aside) % bz)).reshape(nm, my, bz)
            for odd in range(2):
                y = z + z + pltpu.roll(z, my - 1 if odd else 1, 1)
                sf[pl.ds(odd, nm * my, stride=2), :] = y.reshape(nm * my, bz)
            pf[pl.ds(0, nm * my, stride=2), :] = w
            pf[pl.ds(1, nm * my, stride=2), :] = w

        wide = width > 1
        past = INNER + 1 if wide else 1
        def e2(i):
            x = i - WIDTH
            m = x // 2 + width
            n = m + 1 if x % 2 else m - 1
            values = []
            for t, (pf, sf) in enumerate(((pf0, sf0), (pf1, sf1))):
                here = sf[moved(rows_some, m * ey), :]
                around = here + here + sf[moved(rows_some, n * ey), :]
                values.append(se[t, i, rows_some] + w27[t, i, rows_some] * pf[moved(rows_some, m * ey), :]
                              + d[t, i, rows_some] * around)
            return values

        at2, result2 = boxes(e2, WIDTH - past + 1, WIDTH + bx + past - 1, wide)
        for i in range(WIDTH - past + 1, WIDTH + bx + past - 1):
            a, b = at2(i)
            sa, sb = result2(i)
            finish(i, a, k27[0, i, rows_some] * a - sa, k27[1, i, rows_some] * b - sb if wide else None)

    gamma, delta = [], []

    def finish1(i, e, out, out_b):
        im0[0, i, rows_some] = out
        im0[1, i, rows_some] = out_b
        if own(i):
            e, out = e[shore:shore + by], im0[0, i, EDGE:EDGE + by]
            pre_ref[i - WIDTH] = e
            img_ref[i - WIDTH] = out
            gamma.append(g_ref[i - WIDTH] * e)
            delta.append(out * e)
        if i == WIDTH + bx - 1:
            gs = jnp.sum(total_of(gamma), axis=0, keepdims=True)
            ds = jnp.sum(total_of(delta), axis=0, keepdims=True)
            gs, ds = gs + pltpu.roll(gs, half, 1), ds + pltpu.roll(ds, half, 1)
            sum_begin(0, jnp.where(lane8[:1] < half, gs, ds))

    nothing = lambda: None
    cycle(3, lambda i, rows: (gc0[0, i, rows], t1[0, i, rows]), near0, near1, s1, r1, make_b, near, ky, RIM - 1, coefficients, nothing, finish1)

    def relay(stage):
        if len(groups) > 1:
            sum_begin(stage, sum_end(stage - 1))

    def finish2(i, e, out, out_b):
        twice_ref[i - WIDTH] = e[shore:shore + by]
        image_twice_ref[i - WIDTH] = out[shore:shore + by]

    skip1 = RIM - 1
    cycle(4, lambda i, rows: (im0[0, i, rows], im0[1, i, rows]), mid[0, skip1:skip1 + lx], mid[1, skip1:skip1 + lx], s2, r2, make_d, later, 1, 1,
          lambda: relay(1), lambda: relay(2), finish2)

    total = sum_end(len(groups) - 1)
    gs = jnp.sum(jnp.where(lane8[:1] < half, total, 0.0), axis=1, keepdims=True)
    ds = jnp.sum(jnp.where(lane8[:1] < half, 0.0, total), axis=1, keepdims=True)
    alpha_ref[...] = jnp.broadcast_to(gs / ds, (1, bz)).reshape(alpha_ref.shape)
    leave([(fine_copy, close), (outer_copy, sides), (relay_copy, near), (make_b, near), (make_d, later)])
    for stage in range(len(groups)):
        some = red_r.at[pl.ds(base[stage], len(mates[stage]))]
        pltpu.make_async_copy(some, some, lssem.at[stage]).wait()


def solution(mesh):
    counts = tuple(mesh.shape[a] for a in AXES)

    def shards(right_side, coefficient):
        bx, by, bz = block = right_side.shape
        assert SPAN <= bx and SPAN * bx <= bz and by == 16 and bx % 4 == 0
        kx = max(1, min(-(-PART // (bx // 4)), counts[0] - 1))
        ky = max(1, min(-(-PART // (by // 4)), counts[1] - 1))
        ex, ey = bx + SPAN, by + 2 * EDGE
        ox, my = bx // 2, ey // 2
        qx = bx // 4
        mx = ox + 2 * RIM
        most = (2 * kx + 1) * (2 * ky + 1) * 3
        planes = len([x for x in range(-PART, qx + PART) if -kx * qx <= x < (kx + 1) * qx])
        mates = [len(partners(counts, group)) for group in stages(counts)]
        f32 = jnp.float32
        vmem = pl.BlockSpec(memory_space=pltpu.VMEM)
        messages = [pltpu.VMEM((5, 8, bz), f32)] * 3
        messages += [pltpu.VMEM((2 * kx + 1, 2 * ky + 1, 3, 5, 8, bz), f32)] * 3
        precond, image, twice, image_twice, alpha, g = pl.pallas_call(
            functools.partial(kernel, counts, block, kx, ky),
            out_shape=[pltpu.VMEM(block, f32)] * 4 + [pltpu.VMEM((1, 1, bz), f32), pltpu.VMEM(block, f32)],
            in_specs=[pl.BlockSpec(memory_space=pltpu.HBM)] * 2,
            out_specs=[vmem] * 6,
            scratch_shapes=[
                pltpu.VMEM((2, ex, ey, bz), f32),
                pltpu.VMEM((2, ex, ey, bz), f32),
                pltpu.VMEM((2, by, bz), f32),
                pltpu.VMEM((2, by, bz), f32),
                pltpu.VMEM((2, 2, ey, bz), f32),
                pltpu.VMEM((2, 2, ey, bz), f32),
                pltpu.VMEM((2, ex, ey, bz), f32),
                *[pltpu.VMEM((2, ex, ey, bz), f32)] * 3,
                pltpu.VMEM((2, ex, ey + 2 * EDGE, bz), f32),
                pltpu.VMEM(((ox + 2) * ey, bz), f32),
                pltpu.VMEM(((ox + 2) * ey, bz), f32),
                *[pltpu.VMEM(((mx - 2) * ey, bz), f32)] * 4,
                pltpu.VMEM((2, ex, ey, bz), f32),
                pltpu.VMEM((qx * my, bz), f32),
                pltpu.VMEM(((qx + 4) * my, bz), f32),
                *messages,
                pltpu.VMEM((2, planes, my, bz), f32),
                pltpu.VMEM((2, mx, my, bz), f32),
                pltpu.VMEM((len(mates), 1, bz), f32),
                pltpu.VMEM((sum(mates), 1, bz), f32),
                pltpu.VMEM((128 * most, 1, bz), f32),
                pltpu.SemaphoreType.DMA((2,)),
                pltpu.SemaphoreType.DMA,
                pltpu.SemaphoreType.DMA((6,)),
                pltpu.SemaphoreType.DMA((len(mates),)),
                pltpu.SemaphoreType.DMA((len(mates),)),
            ],
            compiler_params=pltpu.CompilerParams(collective_id=0, has_side_effects=True),
            name="relayed",
        )(right_side, coefficient)
        return (alpha * precond, g - alpha * image,
                precond - alpha * twice, image - alpha * image_twice)

    placed = (P(*AXES), P(*AXES))
    return jax.shard_map(
        shards, mesh=mesh, in_specs=placed, out_specs=(P(*AXES),) * 4, check_vma=False
    )
```

```python
import functools
import itertools

import jax
import jax.numpy as jnp
from jax import lax
from jax.experimental import pallas as pl
from jax.experimental.pallas import tpu as pltpu
from jax.sharding import PartitionSpec as P

SWEEPS = 4
relaxation = 0.6

AXES = ("gx", "gy", "gz")
MESH = pl.DeviceIdType.MESH
WIDTH = 5
INNER = 3
EDGE = 8
SPAN = 2 * WIDTH
RIM = 4
PART = SWEEPS + 1


def pick(values, lanes):
    flat = values.reshape(-1, values.shape[-1])
    lanes = jnp.broadcast_to(lanes[:1], flat.shape)
    return jnp.take_along_axis(flat, lanes, axis=1).reshape(values.shape)


def iota(shape, dim):
    return lax.broadcasted_iota(jnp.int32, shape, dim)


def total_of(values):
    while len(values) > 1:
        values = [a + b for a, b in zip(values[::2], values[1::2])] + values[len(values) & ~1:]
    return values[0]


def stages(counts):
    if max(counts) <= RIM:
        return [(0, 1, 2)]
    return [(2,), (1,), (0,)]


def partners(counts, group):
    steps = [(0, 0, 0)]
    for axis in group:
        steps = [s[:axis] + (k,) + s[axis + 1:] for s in steps for k in range(counts[axis])]
    return [s for s in steps if s != (0, 0, 0)]


def kernel(counts, block, kx, ky, g_hbm, c_hbm, pre_ref, img_ref, twice_ref, image_twice_ref, alpha_ref, g_ref,
           gc0, im0, pk, pkx, zr, zrx, t1, d, k27, w27, ys, xr0, xr1, pf0, pf1, sf0, sf1, se, xm, um,
           s0, s1, s2, r0, r1, r2, kept, mid, red_s, red_r, units, insem, ssem, rsem, lssem, lrsem):
    bx, by, bz = block
    me = [lax.axis_index(a) for a in AXES]
    ex, ey = bx + SPAN, by + 2 * EDGE
    ox, my = bx // 2, ey // 2
    qx, qy = bx // 4, by // 4
    half, quarter = bz // 2, bz // 4
    lane = iota((ey, bz), 1)
    row = iota((ey, bz), 0)
    lane8 = iota((8, bz), 1)
    row8 = iota((8, bz), 0)

    def valid(offset):
        ok = None
        for axis, step in enumerate(offset):
            if step == 0:
                continue
            place = me[axis] + step
            term = place >= 0 if step < 0 else place < counts[axis]
            ok = term if ok is None else jnp.logical_and(ok, term)
        return ok

    def target(offset):
        return tuple(m + s for m, s in zip(me, offset))

    near = [(dx, dy, dz) for dx in range(-kx, kx + 1) for dy in range(-ky, ky + 1) for dz in (-1, 0, 1)]
    near = [o for o in near if o != (0, 0, 0) and all(counts[a] > abs(o[a]) for a in range(3))]
    near.sort(key=lambda o: -sum(map(abs, o)))
    close = [o for o in near if abs(o[0]) <= 1 and abs(o[1]) <= 1]
    sides = [o for o in close if o[0] != 0 and o[2] == 0]
    later = [o for o in near if abs(o[1]) <= 1]

    groups = stages(counts)
    mates = []
    base = [0]
    for group in groups:
        mates.append(partners(counts, group))
        base.append(base[-1] + len(mates[-1]))

    def mate(step):
        return tuple(lax.rem(m + s, n) if s else m for m, s, n in zip(me, step, counts))

    inside0 = gc0.at[:, pl.ds(WIDTH, bx), pl.ds(EDGE, by), :]
    copies = [pltpu.make_async_copy(src, inside0.at[n], insem.at[n]) for n, src in enumerate((g_hbm, c_hbm))]
    for copy in copies:
        copy.start()
    greet = [o for o in near if abs(o[1]) <= 1 and (abs(o[0]) <= 1 or o[1] == o[2] == 0)]
    barrier = pltpu.get_barrier_semaphore()
    for offset in greet:
        @pl.when(valid(offset))
        def _(offset=offset):
            pl.semaphore_signal(barrier, inc=1, device_id=target(offset), device_id_type=MESH)
    greeted = 0
    if len(groups) > 1:
        for steps in mates:
            for step in steps:
                pl.semaphore_signal(barrier, inc=1, device_id=mate(step), device_id_type=MESH)
            greeted = greeted + len(steps)

    def options(axis, step):
        if counts[axis] <= step:
            return 0
        return (me[axis] >= step).astype(jnp.int32) + (me[axis] + step < counts[axis]).astype(jnp.int32)

    around = (1 + options(0, 1)) * (1 + options(1, 1)) * (1 + options(2, 1)) - 1
    greeted = greeted + around + sum(options(0, step) for step in range(2, kx + 1))

    def clear(ref):
        ref[...] = jnp.zeros(ref.shape, jnp.float32)

    for axis, edges in enumerate((
            [[gc0.at[:, pl.ds(0, WIDTH)], zrx.at[:, 0]], [gc0.at[:, pl.ds(WIDTH + bx, WIDTH)], zrx.at[:, 1]]],
            [[ref.at[..., pl.ds(at, WIDTH), :] for ref in (gc0, zr, zrx)] for at in (EDGE - WIDTH, EDGE + by)],
            [[ref.at[side] for ref in (zr, zrx)] for side in range(2)])):
        for refs, edge in zip(edges, (0, counts[axis] - 1)):
            @pl.when(me[axis] == edge)
            def _(refs=refs):
                for ref in refs:
                    clear(ref)

    for ref in (gc0, zr, zrx):
        clear(ref.at[..., pl.ds(0, EDGE - WIDTH), :])
        clear(ref.at[..., pl.ds(ey - EDGE + WIDTH, EDGE - WIDTH), :])
    for at in (0, ey):
        ys[:, :, at:at + 2 * EDGE, :] = jnp.zeros((2, ex, 2 * EDGE, bz), jnp.float32)

    def row_ends(dy):
        if dy == 0:
            return 0, by, EDGE
        if dy > 0:
            return by - WIDTH, WIDTH, EDGE - WIDTH
        return 0, WIDTH, EDGE + by

    def remote(src, dst, phase, offset):
        pltpu.make_async_remote_copy(
            src_ref=src, dst_ref=dst, send_sem=ssem, recv_sem=rsem.at[phase],
            device_id=target(offset), device_id_type=MESH).start()

    def planes_copy(phase, offset, first, size):
        dx, dy, dz = offset
        start, rows, goes = row_ends(dy)
        if dx == 0:
            px, tx, size = WIDTH, WIDTH, bx
        elif dx > 0:
            px, tx = WIDTH + bx - first - size, WIDTH - first - size
        else:
            px, tx = WIDTH + first, WIDTH + bx + first
        src = gc0.at[:, pl.ds(px, size), pl.ds(EDGE + start, rows), :]
        dst = gc0.at[:, pl.ds(tx, size), pl.ds(goes, rows), :]
        return (src, dst, phase, offset)

    def fine_copy(offset):
        dx, dy, dz = offset
        if dz == 0:
            return planes_copy(0, offset, 0, INNER)
        start, rows, goes = row_ends(dy)
        side = 0 if dz > 0 else 1
        if dx == 0:
            src = pk.at[:, pl.ds(start, rows), :]
            dst = zr.at[side, :, pl.ds(goes, rows), :]
        else:
            end = 0 if dx > 0 else 1
            src = pkx.at[end, pl.ds(start, rows), :]
            dst = zrx.at[side, end, pl.ds(goes, rows), :]
        return (src, dst, 0, offset)

    def outer_copy(offset):
        return planes_copy(1, offset, INNER, WIDTH - INNER)

    def part(offset, depth):
        dx, dy, dz = offset
        if abs(dx) > 1 or abs(dy) > 1:
            return 0, 1
        if dz != 0:
            return 4, 1
        if dx == 0:
            return 0, 4
        if dx < 0:
            return 0, 1 + depth
        return 4 - depth, 1 + depth

    def coarse_copy(phase, offset, s, r, depth):
        dx, dy, dz = offset
        at, size = part(offset, depth)
        return (s.at[pl.ds(at, size)], r.at[kx - dx, ky - dy, 1 - dz, pl.ds(at, size)], phase, offset)

    def tiles(make, offset):
        size = 1
        for n in make(offset)[0].shape:
            size *= n
        assert size % bz == 0
        return size // bz

    def begin(make, offsets):
        for offset in offsets:
            @pl.when(valid(offset))
            def _(offset=offset):
                remote(*make(offset))

    def wait_for(sem, pairs):
        sizes = {}
        for make, offsets in pairs:
            for offset in offsets:
                key = tuple(map(abs, offset))
                sizes.setdefault(key, 0)
                if offset == key:
                    sizes[key] += tiles(make, offset)

        def amount(options):
            total = 0
            for (a, b, c), size in sizes.items():
                total = total + size * options[0][a] * options[1][b] * options[2][c]
            return total

        def number(place, count, step):
            return 1 if step == 0 else (place >= step) * 1 + (place + step < count) * 1

        def table(axis, place):
            return [number(place, counts[axis], k) for k in range(3)]

        here = []
        for axis in range(3):
            has = [1]
            for k in (1, 2):
                n = (me[axis] >= k).astype(jnp.int32) + (me[axis] + k < counts[axis]).astype(jnp.int32)
                has.append(n)
            here.append(has)
        total = amount(here)
        for value in sorted({amount(options) for options in itertools.product(
                *[[table(axis, place) for place in range(counts[axis])] for axis in range(3)])}):
            @pl.when(total == value)
            def _(value=value):
                some = units.at[pl.ds(0, value)]
                pltpu.make_async_copy(some, some, sem).wait()

    def arrive(phase, make, offsets):
        wait_for(rsem.at[phase], [(make, offsets)])

    def leave(pairs):
        wait_for(ssem, pairs)

    def mate_copy(stage, k):
        n = base[stage] + k
        return pltpu.make_async_remote_copy(
            src_ref=red_s.at[stage], dst_ref=red_r.at[n], send_sem=lssem.at[stage],
            recv_sem=lrsem.at[stage], device_id=mate(mates[stage][k]), device_id_type=MESH)

    def sum_begin(stage, value):
        red_s[stage] = value
        for k in range(len(mates[stage])):
            mate_copy(stage, k).start()

    def sum_end(stage):
        some = red_r.at[pl.ds(base[stage], len(mates[stage]))]
        pltpu.make_async_copy(some, some, lrsem.at[stage]).wait()
        return total_of([red_s[stage]] + [red_r[base[stage] + k] for k in range(len(mates[stage]))])

    strip = (lane[:by] < WIDTH) | (lane[:by] >= bz - WIDTH)
    place = lax.rem(lane + WIDTH, bz)
    low = lax.rem(place, SPAN) < WIDTH
    band = (lane < WIDTH) | (lane >= bz - WIDTH)
    first, last = lane == 0, lane == bz - 1

    def turn_to(v, shift):
        shift = shift % bz
        return v if shift == 0 else pltpu.roll(v, shift, 1)

    def pack(planes):
        pieces = [turn_to(jnp.where(strip, plane, 0.0), SPAN * i) for i, plane in enumerate(planes)]
        ends = (total_of(pieces[bx - WIDTH:]), total_of(pieces[:WIDTH]))
        return ends, total_of(pieces[WIDTH:bx - WIDTH] + list(ends))

    def lines(v, wide):
        a, b = v
        la, ra = pltpu.roll(a, 1, 1), pltpu.roll(a, bz - 1, 1)
        lb, rb = pltpu.roll(b, 1, 1), pltpu.roll(b, bz - 1, 1)
        f, l = first[:a.shape[0]], last[:a.shape[0]]
        sa = a + jnp.where(f, lb, la) + jnp.where(l, rb, ra)
        return sa, b + jnp.where(f, la, lb) + jnp.where(l, ra, rb) if wide else None

    shore = WIDTH - 1
    rows_all, rows_some = slice(0, ey), slice(EDGE - shore, EDGE + by + shore)

    def moved(rows, by_):
        return slice(rows.start + by_, rows.stop + by_)

    def boxes(value, start, stop, wide=True, rows=rows_some):
        held, pairs = {}, {}

        def at(i):
            if i not in held:
                held[i] = value(i)
            return held[i]

        def pair(i):
            if i not in pairs:
                pairs[i] = [p + q for p, q in zip(at(i), at(i + 1))]
            return pairs[i]

        def result(i):
            if (i - start) % 2 == 0:
                around = [p + q for p, q in zip(at(i - 1), pair(i))]
            else:
                around = [p + q for p, q in zip(pair(i - 1), at(i + 1))]
            total = []
            for t in range(2):
                ys[t, i, moved(rows, EDGE), :] = around[t]
                mid_row = around[t] if rows is rows_some else ys[t, i, moved(rows_some, EDGE), :]
                total.append(mid_row + ys[t, i, moved(rows_some, EDGE - 1), :] + ys[t, i, moved(rows_some, EDGE + 1), :])
            return lines(total, wide)

        return at, result

    def box(v):
        s = v + pltpu.roll(v, 1, 2) + pltpu.roll(v, v.shape[2] - 1, 2)
        s = s + pltpu.roll(s, 1, 1) + pltpu.roll(s, v.shape[1] - 1, 1)
        zero = jnp.zeros_like(s[:1])
        return s + jnp.concatenate([zero, s[:-1]], 0) + jnp.concatenate([s[1:], zero], 0)

    down = (2 * lane8) % bz
    down_c = (2 * lane8) % half
    up_a = lane8 >> 1
    up_b = (lane8 + bz) >> 1
    aside = 2 * (lane8 & 1) - 1
    up_c = jnp.where(lane8 < 3 * quarter, lane8 >> 1, (lane8 >> 1) + half)

    def paired(v):
        return v + pltpu.roll(v, bz - 1, v.ndim - 1)

    lx = ox + 2

    def restricted(of):
        for m in range(lx):
            a0, b0 = of(2 * m + INNER)
            a1, b1 = of(2 * m + INNER + 1)
            xr0[moved(rows_some, m * ey), :] = a0 + a1
            xr1[moved(rows_some, m * ey), :] = b0 + b1
        n = lx * my
        a = xr0[pl.ds(0, n, stride=2), :] + xr0[pl.ds(1, n, stride=2), :]
        b = xr1[pl.ds(0, n, stride=2), :] + xr1[pl.ds(1, n, stride=2), :]
        a, b = pick(paired(0.5 * a), down), pick(paired(0.5 * b), down)
        return jnp.where(iota(a.shape, 1) < half, a, b).reshape(lx, my, bz)

    turn = lane8 // quarter

    def coarsened(v):
        for m in range(qx):
            xm[m * my:(m + 1) * my, :] = v[2 * m] + v[2 * m + 1]
        n = qx * my // 2
        a = xm[pl.ds(0, n, stride=2), :] + xm[pl.ds(1, n, stride=2), :]
        a = pick(paired(0.5 * a), down_c)
        rows = my // 2
        tile = a[:rows]
        for m in range(1, qx):
            tile = jnp.where(turn == m, a[m * rows:(m + 1) * rows], tile)
        return pltpu.roll(tile, rows - 2, 0)

    rim = (lane8 < RIM) | ((lane8 >= half - RIM) & (lane8 < half))
    edge1 = my // 2 - by // 4
    here_ends = (lane8 < RIM * ox) | ((lane8 >= half - RIM) & (lane8 < half - RIM + RIM * ox))

    def post(s, v1, tile):
        own = [v1[p][edge1:edge1 + by // 2] for p in range(ox)]
        ends = total_of([turn_to(jnp.where(rim, own[p], 0.0), RIM * p) for p in range(ox)])
        ends = jnp.where(here_ends, ends, pltpu.roll(turn_to(ends, RIM * ox), 4, 0))
        tile = jnp.where(row8 < qy, tile, ends)
        s[0] = tile
        for k in range(ox // 2):
            s[1 + k] = jnp.where(lane8 < half, own[2 * k], pltpu.roll(own[2 * k + 1], half, 1))
        s[4] = tile

    def middle(s, r, width):
        depth = RIM // 2 if width > 2 else 1

        def get(dx, dy, dz, k):
            if (dx, dy, dz) == (0, 0, 0):
                return s[k]
            if any(abs(d) >= n for d, n in zip((dx, dy, dz), counts)):
                return jnp.zeros((8, bz), jnp.float32)
            return r[kx + dx, ky + dy, 1 + dz, k]

        def rows(tiles):
            before, here, after = tiles
            return (pltpu.roll(jnp.where(row8 >= 4, before, here), 4, 0),
                    pltpu.roll(jnp.where(row8 >= 4, here, after), 4, 0))

        planes = []
        for dx in (-1, 0, 1):
            tiles = range(ox // 2 - depth, ox // 2) if dx < 0 else range(depth) if dx > 0 else range(ox // 2)
            ends = [jnp.where(lane8 < 2 * RIM * ox + RIM, get(dx, dy, 1, 4), get(dx, dy, -1, 4)) for dy in (-1, 0, 1)]
            ends = [jnp.where(row8 < 4, pltpu.roll(ends[k], 4, 0), turn_to(ends[k + 1], -RIM * ox)) for k in range(2)]
            for k in tiles:
                pair = rows([get(dx, dy, 0, 1 + k) for dy in (-1, 0, 1)])
                for odd in (0, 1):
                    p = 2 * k + odd
                    planes.append(jnp.concatenate([
                        jnp.where(lane8 < half, pltpu.roll(t, half, 1) if odd else t, turn_to(e, half - RIM * p))
                        for t, e in zip(pair, ends)], 0))
        return jnp.stack(planes)

    xs = [x for x in range(-PART, qx + PART) if -kx * qx <= x < (kx + 1) * qx]

    def gathered(s, r, far):
        zero = jnp.zeros((8, bz), jnp.float32)

        def get(dx, dy, dz):
            if (dx, dy, dz) == (0, 0, 0):
                return s[0]
            if any(abs(d) >= n for d, n in zip((dx, dy, dz), counts)) or abs(dy) > far:
                return zero
            return r[kx + dx, ky + dy, 1 + dz, part((-dx, -dy, -dz), 0)[0]]

        columns = {}
        for dx in sorted({x // qx for x in xs}):
            for dy in range(-2, 3):
                if abs(dy) > far:
                    continue
                here = get(dx, dy, 0)
                after = pltpu.roll(get(dx, dy, 1), quarter, 1)
                before = pltpu.roll(get(dx, dy, -1), 3 * quarter, 1)
                for m in range(qx):
                    tile = jnp.where(turn == (m + 1) % 4, after, here)
                    tile = jnp.where(turn == (m + 3) % 4, before, tile)
                    columns[dx * qx + m, dy] = turn_to(tile, -quarter * m)
        planes = []
        for x in xs:
            t = {dy: columns.get((x, dy), zero) for dy in range(-2, 3)}
            upper = jnp.where(row8 < qy, t[-1], pltpu.roll(t[0], 4, 0))
            if far > 1:
                lower = jnp.where(row8 < qy, t[1], pltpu.roll(jnp.where(row8 < 2, t[2], t[-2]), 4, 0))
            else:
                lower = jnp.where(row8 < qy, t[1], 0.0)
            planes.append(jnp.concatenate([upper, lower], 0))
        return jnp.stack(planes)

    def within(place, axis, size):
        place = place + me[axis] * size
        return (place >= 0) & (place < counts[axis] * size)

    for copy in copies:
        copy.wait()
    g, c = ([gc0[n, WIDTH + i, EDGE:EDGE + by, :] for i in range(bx)] for n in range(2))
    for i in range(bx):
        g_ref[i] = g[i]
    (g_last, g_first), pk[0] = pack(g)
    (c_last, c_first), pk[1] = pack(c)
    pkx[0] = g_last + turn_to(c_last, -SPAN * WIDTH)
    pkx[1] = g_first + turn_to(c_first, SPAN * WIDTH)

    for m in range(ox):
        xr0[m * ey + EDGE:m * ey + EDGE + by, :] = c[2 * m] + c[2 * m + 1]
    n = ox * my
    own1 = xr0[pl.ds(0, n, stride=2), :] + xr0[pl.ds(1, n, stride=2), :]
    own1 = pick(paired(0.5 * own1), down).reshape(ox, my, bz)
    post(s0, own1, coarsened(own1))

    def relay_copy(offset):
        dx, dy, dz = offset
        if (dy, dz) == (0, 0):
            return coarse_copy(2, offset, s0, r0, RIM // 2)
        far = abs(dx) > 1 or abs(dy) > 1
        at, size = part((-dx, 0, 0), RIM // 2)
        if far or dz != 0:
            at, size = 4 if dx == -1 else 0, 1
        src = s0.at[pl.ds(at, size)] if dx == 0 else r0.at[kx + dx, ky, 1, pl.ds(at, size)]
        goes = 0 if far else 4 if dz != 0 else at
        return src, r0.at[kx + dx, ky - dy, 1 - dz, pl.ds(goes, size)], 5, (0, dy, dz)

    along_x = [o for o in near if o[1] == o[2] == 0]
    onwards = [o for o in near if o not in along_x]
    make_b = lambda o: coarse_copy(3, o, s1, r1, RIM // 2)
    make_d = lambda o: coarse_copy(4, o, s2, r2, 1)
    pl.semaphore_wait(barrier, greeted)
    begin(fine_copy, [o for o in close if sum(map(abs, o)) > 1])
    begin(relay_copy, along_x)
    begin(fine_copy, [o for o in close if sum(map(abs, o)) == 1])

    in_y = within(row - EDGE, 1, by)

    def factors(t, i, rows, c, inverse):
        d[t, i, rows], k27[t, i, rows] = inverse, 27.0 + c
        w27[t, i, rows] = 1.0 - inverse * (27.0 + c)

    def spread(i):
        if own(i):
            shifts = [SPAN * (i - WIDTH)] * 2
            packs, scale = merged, 0
        elif i < WIDTH:
            shifts = [SPAN * (bx - WIDTH + i), SPAN * (bx - WIDTH + i - WIDTH)]
            packs, scale = [ends[0]] * 2, 1
        else:
            shifts = [SPAN * (i - WIDTH - bx), SPAN * (i - bx)]
            packs, scale = [ends[1]] * 2, 2
        t1[0, i] = turn_to(packs[0], -shifts[0])
        cb = t1[1, i] = turn_to(packs[1], -shifts[1])
        factors(1, i, slice(None), cb, scales_b[scale] / (26.0 + cb))
        for at, size in ((0, EDGE), (EDGE + by, EDGE)) if own(i) else ((0, ey),):
            rows = slice(at, at + size)
            c = gc0[1, i, rows]
            factors(0, i, rows, c, scales_a[scale][rows] / (26.0 + c))

    def own(i):
        return WIDTH <= i < WIDTH + bx

    def kept_if(ok):
        return jnp.where(ok, relaxation, 0.0)

    in_x = [True, me[0] > 0, me[0] + 1 < counts[0]]
    in_z = jnp.where(lane < half, jnp.full((ey, bz), kept_if(me[2] + 1 < counts[2]), jnp.float32),
                     jnp.full((ey, bz), kept_if(me[2] > 0), jnp.float32))
    scales_a = [jnp.where(in_y, kept_if(ok), 0.0) for ok in in_x]
    scales_b = [jnp.where(in_y & band & ok, in_z, 0.0) for ok in in_x]
    for i in range(bx):
        factors(0, WIDTH + i, slice(EDGE, EDGE + by), c[i], relaxation / (26.0 + c[i]))

    arrive(2, relay_copy, along_x)
    begin(relay_copy, [o for o in onwards if abs(o[1]) <= 1])
    arrive(0, fine_copy, close)
    begin(relay_copy, [o for o in onwards if abs(o[1]) > 1])
    begin(outer_copy, sides)
    merged = [jnp.where(low, zr[0, f], zr[1, f]) for f in range(2)]
    ends = [jnp.where(low, zrx[0, e], zrx[1, e]) for e in range(2)]
    skip = WIDTH - INNER
    for i in range(skip, ex - skip):
        spread(i)

    def inside1(shape, width):
        zl = iota(shape, 2)
        zl = jnp.where(zl < 3 * quarter, zl, zl - bz)
        ok = within(iota(shape, 0) - width, 0, ox) & within(iota(shape, 1) - edge1, 1, by // 2)
        return ok & within(zl, 2, half) & (zl >= -RIM) & (zl < half + RIM)

    c1 = restricted(lambda i: (gc0[1, i, rows_some], t1[1, i, rows_some]))
    near0 = jnp.where(inside1((lx, my, bz), 1), relaxation / (26.0 + c1), 0.0)
    near1 = 27.0 + c1

    def outer():
        arrive(1, outer_copy, sides)
        for i in list(range(skip)) + list(range(ex - skip, ex)):
            spread(i)

    def coefficients():
        arrive(5, relay_copy, onwards)
        c1 = middle(s0, r0, RIM)
        ok = inside1(c1.shape, RIM)
        c1 = jnp.where(ok, c1, 0.0)
        mid[0] = jnp.where(ok, relaxation / (26.0 + c1), 0.0)
        mid[1] = 27.0 + c1
        c2 = gathered(s0, r0, ky)
        shape = c2.shape
        z = iota(shape, 2)
        z = jnp.where(z < 2 * quarter, z, z - bz)
        y = iota(shape, 1)
        y = jnp.where(y < my - 2, y, y - my) - qy
        ok = within(iota(shape, 0) + xs[0], 0, qx) & within(y, 1, qy)
        ok = ok & within(z, 2, quarter) & (z >= -quarter)
        c2 = jnp.where(ok, c2, 0.0)
        kept[0] = jnp.where(ok, relaxation / (26.0 + c2), 0.0)
        kept[1] = 27.0 + c2

    def cycle(phase, g_at, near0, near1, s, r, make, offsets, far, width, hook, second, finish):
        def e0(i, rows=rows_some):
            a, b = g_at(i, rows)
            return d[0, i, rows] * a, d[1, i, rows] * b

        def settle(i, sums):
            for t, (e, s_) in enumerate(zip(e0(i), sums)):
                se[t, i, rows_some] = (w27[t, i, rows_some] + 1.0) * e + d[t, i, rows_some] * s_

        start = WIDTH - 2
        at, result = boxes(e0, start, ex - start)

        def remainder(i):
            a, b = g_at(i, rows_some)
            sa, sb = result(i)
            if phase == 4:
                se[0, i, rows_some], se[1, i, rows_some] = sa, sb
            return w27[0, i, rows_some] * a + sa, w27[1, i, rows_some] * b + sb

        g1 = restricted(remainder)
        f = near0 * g1
        post(s, g1[1:1 + ox], coarsened((g1 - near1 * f + box(f))[1:1 + ox]))
        begin(make, offsets)
        if phase == 3:
            outer()
            whole = boxes(lambda i: e0(i, rows_all), 1, ex - 1, rows=rows_all)[1]
            for i in range(1, ex - 1):
                settle(i, whole(i))
        else:
            for i in range(WIDTH - 1, WIDTH + bx + 1):
                settle(i, [se[t, i, rows_some] for t in range(2)])
        hook()
        arrive(phase, make, offsets)
        inv, diag = kept[0], kept[1]
        g2 = jnp.where(inv > 0.0, gathered(s, r, far), 0.0)
        reach = (width + 1) // 2
        e = inv * g2
        lowest = 0
        for sweep in range(SWEEPS - 1):
            left = reach + SWEEPS - 2 - sweep
            keep = [n for n, x in enumerate(xs) if -left <= x < qx + left]
            some = slice(keep[0], keep[-1] + 1)
            part_ = slice(keep[0] - lowest, keep[-1] + 1 - lowest)
            e = e[part_] + inv[some] * (g2[some] - diag[some] * e[part_] + box(e)[part_])
            lowest = keep[0]
        second()
        held = xs[lowest:lowest + e.shape[0]]
        nq = qx + 2 * reach
        zero = jnp.zeros_like(e[:1])
        e = jnp.concatenate([e[held.index(x)][None] if x in held else zero for x in range(-reach, qx + reach)], 0)
        e = pltpu.roll(e, my - 2, 1)[:, :my // 2].reshape(nq * my // 2, bz)
        u = pick(e, up_c)
        um[pl.ds(0, nq * my // 2, stride=2), :] = u
        um[pl.ds(1, nq * my // 2, stride=2), :] = u
        u = um[:nq * my, :].reshape(nq, my, bz)
        span = width + 1
        mx = ox + 2 * span
        u = jnp.concatenate([u[(m - span) // 2 + reach][None] for m in range(mx)], 0)
        skip1 = RIM - span
        inv, diag = mid[0, skip1:skip1 + mx], mid[1, skip1:skip1 + mx]
        g1 = jnp.where(inv > 0.0, middle(s, r, span), 0.0)
        f = inv * g1 + u
        f = f + inv * (g1 - diag * f + box(f))
        nm = mx - 2
        f = f[1:mx - 1].reshape(nm * my, bz)
        for pf, sf, up in ((pf0, sf0, up_a), (pf1, sf1, up_b)):
            w = pick(f, up)
            z = (w + w + pick(f, (up + aside) % bz)).reshape(nm, my, bz)
            for odd in range(2):
                y = z + z + pltpu.roll(z, my - 1 if odd else 1, 1)
                sf[pl.ds(odd, nm * my, stride=2), :] = y.reshape(nm * my, bz)
            pf[pl.ds(0, nm * my, stride=2), :] = w
            pf[pl.ds(1, nm * my, stride=2), :] = w

        wide = width > 1
        past = INNER + 1 if wide else 1
        def e2(i):
            x = i - WIDTH
            m = x // 2 + width
            n = m + 1 if x % 2 else m - 1
            values = []
            for t, (pf, sf) in enumerate(((pf0, sf0), (pf1, sf1))):
                here = sf[moved(rows_some, m * ey), :]
                around = here + here + sf[moved(rows_some, n * ey), :]
                values.append(se[t, i, rows_some] + w27[t, i, rows_some] * pf[moved(rows_some, m * ey), :]
                              + d[t, i, rows_some] * around)
            return values

        at2, result2 = boxes(e2, WIDTH - past + 1, WIDTH + bx + past - 1, wide)
        for i in range(WIDTH - past + 1, WIDTH + bx + past - 1):
            a, b = at2(i)
            sa, sb = result2(i)
            finish(i, a, k27[0, i, rows_some] * a - sa, k27[1, i, rows_some] * b - sb if wide else None)

    gamma, delta = [], []

    def finish1(i, e, out, out_b):
        im0[0, i, rows_some] = out
        im0[1, i, rows_some] = out_b
        if own(i):
            e, out = e[shore:shore + by], im0[0, i, EDGE:EDGE + by]
            pre_ref[i - WIDTH] = e
            img_ref[i - WIDTH] = out
            gamma.append(g_ref[i - WIDTH] * e)
            delta.append(out * e)
        if i == WIDTH + bx - 1:
            gs = jnp.sum(total_of(gamma), axis=0, keepdims=True)
            ds = jnp.sum(total_of(delta), axis=0, keepdims=True)
            gs, ds = gs + pltpu.roll(gs, half, 1), ds + pltpu.roll(ds, half, 1)
            sum_begin(0, jnp.where(lane8[:1] < half, gs, ds))

    nothing = lambda: None
    cycle(3, lambda i, rows: (gc0[0, i, rows], t1[0, i, rows]), near0, near1, s1, r1, make_b, near, ky, RIM - 1, coefficients, nothing, finish1)

    def relay(stage):
        if len(groups) > 1:
            sum_begin(stage, sum_end(stage - 1))

    def finish2(i, e, out, out_b):
        twice_ref[i - WIDTH] = e[shore:shore + by]
        image_twice_ref[i - WIDTH] = out[shore:shore + by]

    skip1 = RIM - 1
    cycle(4, lambda i, rows: (im0[0, i, rows], im0[1, i, rows]), mid[0, skip1:skip1 + lx], mid[1, skip1:skip1 + lx], s2, r2, make_d, later, 1, 1,
          lambda: relay(1), lambda: relay(2), finish2)

    total = sum_end(len(groups) - 1)
    gs = jnp.sum(jnp.where(lane8[:1] < half, total, 0.0), axis=1, keepdims=True)
    ds = jnp.sum(jnp.where(lane8[:1] < half, 0.0, total), axis=1, keepdims=True)
    alpha_ref[...] = jnp.broadcast_to(gs / ds, (1, bz)).reshape(alpha_ref.shape)
    leave([(fine_copy, close), (outer_copy, sides), (relay_copy, near), (make_b, near), (make_d, later)])
    for stage in range(len(groups)):
        some = red_r.at[pl.ds(base[stage], len(mates[stage]))]
        pltpu.make_async_copy(some, some, lssem.at[stage]).wait()


def solution(mesh):
    counts = tuple(mesh.shape[a] for a in AXES)

    def shards(right_side, coefficient):
        bx, by, bz = block = right_side.shape
        assert SPAN <= bx and SPAN * bx <= bz and by == 16 and bx % 4 == 0
        kx = max(1, min(-(-PART // (bx // 4)), counts[0] - 1))
        ky = max(1, min(-(-PART // (by // 4)), counts[1] - 1))
        ex, ey = bx + SPAN, by + 2 * EDGE
        ox, my = bx // 2, ey // 2
        qx = bx // 4
        mx = ox + 2 * RIM
        most = (2 * kx + 1) * (2 * ky + 1) * 3
        planes = len([x for x in range(-PART, qx + PART) if -kx * qx <= x < (kx + 1) * qx])
        mates = [len(partners(counts, group)) for group in stages(counts)]
        f32 = jnp.float32
        vmem = pl.BlockSpec(memory_space=pltpu.VMEM)
        messages = [pltpu.VMEM((5, 8, bz), f32)] * 3
        messages += [pltpu.VMEM((2 * kx + 1, 2 * ky + 1, 3, 5, 8, bz), f32)] * 3
        precond, image, twice, image_twice, alpha, g = pl.pallas_call(
            functools.partial(kernel, counts, block, kx, ky),
            out_shape=[pltpu.VMEM(block, f32)] * 4 + [pltpu.VMEM((1, 1, bz), f32), pltpu.VMEM(block, f32)],
            in_specs=[pl.BlockSpec(memory_space=pltpu.HBM)] * 2,
            out_specs=[vmem] * 6,
            scratch_shapes=[
                pltpu.VMEM((2, ex, ey, bz), f32),
                pltpu.VMEM((2, ex, ey, bz), f32),
                pltpu.VMEM((2, by, bz), f32),
                pltpu.VMEM((2, by, bz), f32),
                pltpu.VMEM((2, 2, ey, bz), f32),
                pltpu.VMEM((2, 2, ey, bz), f32),
                pltpu.VMEM((2, ex, ey, bz), f32),
                *[pltpu.VMEM((2, ex, ey, bz), f32)] * 3,
                pltpu.VMEM((2, ex, ey + 2 * EDGE, bz), f32),
                pltpu.VMEM(((ox + 2) * ey, bz), f32),
                pltpu.VMEM(((ox + 2) * ey, bz), f32),
                *[pltpu.VMEM(((mx - 2) * ey, bz), f32)] * 4,
                pltpu.VMEM((2, ex, ey, bz), f32),
                pltpu.VMEM((qx * my, bz), f32),
                pltpu.VMEM(((qx + 4) * my, bz), f32),
                *messages,
                pltpu.VMEM((2, planes, my, bz), f32),
                pltpu.VMEM((2, mx, my, bz), f32),
                pltpu.VMEM((len(mates), 1, bz), f32),
                pltpu.VMEM((sum(mates), 1, bz), f32),
                pltpu.VMEM((128 * most, 1, bz), f32),
                pltpu.SemaphoreType.DMA((2,)),
                pltpu.SemaphoreType.DMA,
                pltpu.SemaphoreType.DMA((6,)),
                pltpu.SemaphoreType.DMA((len(mates),)),
                pltpu.SemaphoreType.DMA((len(mates),)),
            ],
            compiler_params=pltpu.CompilerParams(collective_id=0, has_side_effects=True),
            name="relayed",
        )(right_side, coefficient)
        return (alpha * precond, g - alpha * image,
                precond - alpha * twice, image - alpha * image_twice)

    placed = (P(*AXES), P(*AXES))
    return jax.shard_map(
        shards, mesh=mesh, in_specs=placed, out_specs=(P(*AXES),) * 4, check_vma=False
    )
```
